128 devices in a mesh: dp: 1, tp: 16 (over z, y), sp: 8 (over x, core).
Axes of the slice: x: 4, y: 4, z: 4, core: 2. Of those that a mesh axis runs over, the one named last changes fastest.
Arguments:
- x_seq: bfloat16 [16384, 4608], P(('dp', 'sp', 'tp'))
- w_query: bfloat16 [4608, 32, 128], P(None, 'tp')
- w_key: bfloat16 [4608, 16, 128], P(None, 'tp')
- w_value: bfloat16 [4608, 16, 128], P(None, 'tp')
- w_out: bfloat16 [32, 128, 4608], P('tp')
Outputs:
- output: bfloat16 [16384, 4608], P(('dp', 'sp', 'tp'))
All inputs are finite; a program needn't handle non-finite values.
Results may differ from the reference program's by a relative error of at most 0.00875352.
Values are sent between devices in bfloat16 or wider.
A program may use at most 1 GiB of HBM per device.

```python
import jax
import jax.numpy as jnp
from jax import lax

D = 4608
HEADS = 32
KV_HEADS = 16
HEAD = 128
WINDOW = 4096
CHUNK = 1024
SP = 8
QBLOCK = 128

SEQ = 2 * SP * CHUNK
GROUP = HEADS // KV_HEADS
SPAN = WINDOW + QBLOCK
NEG_BIG = -1e30


def setup_inputs(seed: int = 0, part: int = 0) -> dict:
    base_key = jax.random.key(seed)
    part_key = jax.random.fold_in(base_key, part)
    weight_keys = jax.random.split(base_key, 4)
    x_rows = jax.random.normal(part_key, (SEQ, D), jnp.float32)
    w_query = jax.random.normal(weight_keys[0], (D, HEADS, HEAD), jnp.float32) * (1.5 * D ** -0.5)
    w_key = jax.random.normal(weight_keys[1], (D, KV_HEADS, HEAD), jnp.float32) * D ** -0.5
    w_value = jax.random.normal(weight_keys[2], (D, KV_HEADS, HEAD), jnp.float32) * D ** -0.5
    w_out = jax.random.normal(weight_keys[3], (HEADS, HEAD, D), jnp.float32) * (HEADS * HEAD) ** -0.5
    return {"x_seq": x_rows.astype(jnp.bfloat16), "w_query": w_query.astype(jnp.bfloat16), "w_key": w_key.astype(jnp.bfloat16), "w_value": w_value.astype(jnp.bfloat16), "w_out": w_out.astype(jnp.bfloat16)}


def to_natural(rows_in):
    blocks = rows_in.reshape((SP, 2, CHUNK) + rows_in.shape[1:])
    return jnp.concatenate([blocks[:, 0], blocks[::-1, 1]], axis=0).reshape(rows_in.shape)


def to_stored(rows_in):
    blocks = rows_in.reshape((2 * SP, CHUNK) + rows_in.shape[1:])
    return jnp.stack([blocks[:SP], blocks[SP:][::-1]], axis=1).reshape(rows_in.shape)


def reference(x_seq, w_query, w_key, w_value, w_out):
    x_nat = to_natural(x_seq)
    q_all = jnp.dot(x_nat, w_query.reshape(D, HEADS * HEAD), preferred_element_type=jnp.float32).astype(jnp.bfloat16).reshape(SEQ, KV_HEADS, GROUP, HEAD)
    k_all = jnp.dot(x_nat, w_key.reshape(D, KV_HEADS * HEAD), preferred_element_type=jnp.float32).astype(jnp.bfloat16).reshape(SEQ, KV_HEADS, HEAD)
    v_all = jnp.dot(x_nat, w_value.reshape(D, KV_HEADS * HEAD), preferred_element_type=jnp.float32).astype(jnp.bfloat16).reshape(SEQ, KV_HEADS, HEAD)
    zero_front = jnp.zeros((WINDOW, KV_HEADS, HEAD), jnp.bfloat16)
    k_pad = jnp.concatenate([zero_front, k_all], axis=0)
    v_pad = jnp.concatenate([zero_front, v_all], axis=0)
    score_scale = HEAD ** -0.5
    row_ids = jnp.arange(QBLOCK)[:, None]
    col_ids = jnp.arange(SPAN)[None, :]

    def one_block(start):
        q_blk = lax.dynamic_slice_in_dim(q_all, start, QBLOCK, 0).astype(jnp.float32)
        k_blk = lax.dynamic_slice_in_dim(k_pad, start, SPAN, 0).astype(jnp.float32)
        v_blk = lax.dynamic_slice_in_dim(v_pad, start, SPAN, 0).astype(jnp.float32)
        scores = jnp.einsum("qhgd,khd->hgqk", q_blk, k_blk) * score_scale
        pos_gap = WINDOW + row_ids - col_ids
        visible = (pos_gap >= 0) & (pos_gap < WINDOW) & (start - WINDOW + col_ids >= 0)
        scores = jnp.where(visible, scores, NEG_BIG)
        row_max = jnp.max(scores, axis=-1, keepdims=True)
        prob_blk = jnp.where(visible, jnp.exp(scores - row_max), 0.0)
        row_denom = jnp.sum(prob_blk, axis=-1)
        weighted = jnp.einsum("hgqk,khd->hgqd", prob_blk.astype(jnp.bfloat16).astype(jnp.float32), v_blk)
        normed = (weighted / row_denom[..., None]).astype(jnp.bfloat16)
        return jnp.transpose(normed, (2, 0, 1, 3)).reshape(QBLOCK, HEADS * HEAD)

    starts = jnp.arange(SEQ // QBLOCK) * QBLOCK
    o_nat = lax.map(one_block, starts).reshape(SEQ, HEADS * HEAD)
    y_nat = jnp.dot(o_nat, w_out.reshape(HEADS * HEAD, D), preferred_element_type=jnp.float32).astype(jnp.bfloat16)
    return to_stored(y_nat)
```

```python
import functools

import jax
import jax.numpy as jnp
from jax import lax
from jax.experimental import pallas as pl
from jax.experimental.pallas import tpu as pltpu
from jax.sharding import PartitionSpec as P

WINDOW = 4096
NEG_BIG = -1e30
LOG2E = 1.4426950408889634
MESH = pl.DeviceIdType.MESH
NY = 4
TQ = 256
WIDE = 768
N_WIDE = (WINDOW - TQ) // WIDE


def dot_nt(lhs, rhs):
    return lax.dot_general(lhs, rhs, (((1,), (1,)), ((), ())), preferred_element_type=jnp.float32)


def attn_out_kernel(q_hbm, kv_hbm, wo_hbm, y_hbm, q_v, kv_v, wo_v, s_v, mx_v, mb_v, l_v, acc_v, o_st, og, yst, yv,
                    ld_sem, kv_sem, wo_sem, o_send, o_recv, y_send, y_recv, y_sem):
    sp = lax.axis_index("sp")
    tp = lax.axis_index("tp")
    my_z, my_y = tp // NY, tp % NY
    n_tp = NY * NY
    n_sp = 8
    chunk = kv_v.shape[0] // (2 * n_sp)
    head = kv_v.shape[1] // 2
    cols = yst.shape[2]
    coef = head ** -0.5 * LOG2E
    n_back = WINDOW // chunk

    q_copy = pltpu.make_async_copy(q_hbm, q_v, ld_sem)
    q_copy.start()

    def kv_copy(blk):
        src = kv_hbm.at[blk, 0] if blk < n_sp else kv_hbm.at[2 * n_sp - 1 - blk, 1]
        return pltpu.make_async_copy(src, kv_v.at[pl.ds(blk * chunk, chunk)], kv_sem.at[blk])

    def kv_needed(blk):
        low = (blk <= sp) & (blk >= sp - n_back)
        high = (blk <= 2 * n_sp - 1 - sp) & (blk >= 2 * n_sp - 1 - sp - n_back)
        return low | high

    for blk in range(2 * n_sp):
        @pl.when(kv_needed(blk))
        def _(blk=blk):
            kv_copy(blk).start()

    def wo_copy(idx):
        z_src, y_src = idx // NY, idx % NY
        return pltpu.make_async_copy(wo_hbm.at[:, y_src, (my_z - z_src + NY) % NY], wo_v.at[idx], wo_sem.at[idx])

    for idx in range(n_tp):
        wo_copy(idx).start()

    barrier = pltpu.get_barrier_semaphore()
    for step in range(1, n_tp):
        pl.semaphore_signal(barrier, inc=1, device_id={"tp": (tp + step) % n_tp}, device_id_type=MESH)
    pl.semaphore_wait(barrier, n_tp - 1)

    q_copy.wait()
    for blk in range(2 * n_sp):
        @pl.when(kv_needed(blk))
        def _(blk=blk):
            kv_copy(blk).wait()

    row_i = lax.broadcasted_iota(jnp.int32, (2 * TQ, TQ), 0) % TQ
    col_i = lax.broadcasted_iota(jnp.int32, (2 * TQ, TQ), 1)

    def lane_max(scores):
        best = scores[:, 0:head]
        for idx in range(1, scores.shape[1] // head):
            best = jnp.maximum(best, scores[:, idx * head:(idx + 1) * head])
        return best

    def o_copy(tile, z_dst):
        y_dst, z_row = tile % NY, tile // NY
        rows = chunk // (2 * NY)
        src = o_st.at[pl.ds(pl.multiple_of(tile * rows, rows), rows)]
        dst = og.at[z_row, :, pl.ds(pl.multiple_of(tp * 2 * head, 2 * head), 2 * head)]
        return pltpu.make_async_remote_copy(src_ref=src, dst_ref=dst, send_sem=o_send.at[tile, z_dst], recv_sem=o_recv.at[z_row, tp],
                                            device_id={"tp": NY * z_dst + y_dst}, device_id_type=MESH)

    def attend(q_idx, gidx, wide, start_tile, n_steps, with_first):
        q_blk = q_v[pl.ds(pl.multiple_of(q_idx * TQ, TQ), TQ), :]
        q_two = jnp.concatenate([q_blk[:, :head], q_blk[:, head:]], axis=0)

        def keys(tile, width):
            return kv_v[pl.ds(pl.multiple_of(tile * TQ, TQ), width), 0:head]

        def values(tile, width):
            return kv_v[pl.ds(pl.multiple_of(tile * TQ, TQ), width), head:2 * head]

        per = wide // TQ
        scores = jnp.where(col_i <= row_i, dot_nt(q_two, keys(gidx, TQ)), NEG_BIG)
        s_v[:, 0:TQ] = scores
        best = lane_max(scores)
        if with_first:
            scores = jnp.where(col_i > row_i, dot_nt(q_two, keys(gidx - WINDOW // TQ, TQ)), NEG_BIG)
            s_v[:, TQ:2 * TQ] = scores
            best = jnp.maximum(best, lane_max(scores))
        mx_v[...] = best

        def score_step(idx, carry):
            part = dot_nt(q_two, keys(start_tile + per * idx, wide))
            s_v[:, pl.ds(pl.multiple_of(2 * TQ + idx * wide, TQ), wide)] = part
            mx_v[...] = jnp.maximum(mx_v[...], lane_max(part))
            return carry

        lax.fori_loop(0, n_steps, score_step, 0)
        row_best = jnp.max(mx_v[...], axis=1, keepdims=True) * coef
        mb_v[...] = jnp.broadcast_to(row_best, mb_v.shape)

        def probs(col, width):
            base = mb_v[...]
            total = None
            parts = []
            for idx in range(width // head):
                part = jnp.exp2(s_v[:, pl.ds(pl.multiple_of(col + idx * head, head), head)] * coef - base)
                total = part if total is None else total + part
                parts.append(part.astype(jnp.bfloat16))
            return jnp.concatenate(parts, axis=1), total

        prob, total = probs(0, TQ)
        acc = jnp.dot(prob, values(gidx, TQ), preferred_element_type=jnp.float32)
        if with_first:
            prob, total_b = probs(TQ, TQ)
            total = total + total_b
            acc = acc + jnp.dot(prob, values(gidx - WINDOW // TQ, TQ), preferred_element_type=jnp.float32)
        l_v[...] = total
        acc_v[...] = acc

        def value_step(idx, carry):
            prob, total = probs(2 * TQ + idx * wide, wide)
            l_v[...] += total
            acc_v[...] += jnp.dot(prob, values(start_tile + per * idx, wide), preferred_element_type=jnp.float32)
            return carry

        lax.fori_loop(0, n_steps, value_step, 0)
        denom = jnp.sum(l_v[...], axis=1, keepdims=True)
        out = (acc_v[...] / denom).astype(jnp.bfloat16)
        out = jnp.concatenate([out[:TQ], out[TQ:]], axis=1)
        o_st[pl.ds(pl.multiple_of(q_idx * TQ, TQ), TQ), :] = out

    def q_step(q_idx, carry):
        tiles = chunk // TQ
        blk = jnp.where(q_idx < tiles, sp, 2 * n_sp - 1 - sp)
        gidx = blk * tiles + q_idx % tiles

        @pl.when(gidx >= WINDOW // TQ)
        def _():
            attend(q_idx, gidx, WIDE, gidx - WINDOW // TQ + 1, N_WIDE, True)

        @pl.when(gidx < WINDOW // TQ)
        def _():
            attend(q_idx, gidx, TQ, 0, gidx, False)

        for sub in range(2):
            tile = 2 * q_idx + sub
            for z_dst in range(NY):
                mine = (tile % NY == my_y) & (my_z == z_dst)

                @pl.when(jnp.logical_not(mine))
                def _(tile=tile, z_dst=z_dst):
                    o_copy(tile, z_dst).start()

            @pl.when(tile % NY == my_y)
            def _(tile=tile):
                rows = chunk // (2 * NY)
                og[tile // NY, :, pl.ds(pl.multiple_of(tp * 2 * head, 2 * head), 2 * head)] = \
                    o_st[pl.ds(pl.multiple_of(tile * rows, rows), rows), :]
        return carry

    lax.fori_loop(0, 2 * chunk // TQ, q_step, 0)

    rows = yst.shape[1]

    def o_arrival(z_row, src):
        dst = og.at[z_row, :, pl.ds(src * 2 * head, 2 * head)]
        return pltpu.make_async_remote_copy(src_ref=o_st.at[pl.ds(0, rows)], dst_ref=dst, send_sem=o_send.at[0, 0],
                                            recv_sem=o_recv.at[z_row, src], device_id={"tp": 0}, device_id_type=MESH)

    def y_copy(z_dst, z_src):
        return pltpu.make_async_remote_copy(
            src_ref=yst.at[z_dst], dst_ref=yv.at[:, pl.ds(pl.multiple_of(z_src * cols, 128), cols)],
            send_sem=y_send.at[z_dst], recv_sem=y_recv.at[z_src], device_id={"tp": NY * z_dst + my_y}, device_id_type=MESH)

    for idx in range(n_tp):
        wo_copy(idx).wait()
    for half in range(2):
        for z_row in (2 * half, 2 * half + 1):
            for src in range(n_tp):
                @pl.when(tp != src)
                def _(z_row=z_row, src=src):
                    o_arrival(z_row, src).wait_recv()
        lhs = og[2 * half:2 * half + 2].reshape(2 * rows, n_tp * 2 * head)
        for col in range(0, cols, 384):
            w_cols = wo_v[:, :, :, col:col + 384].reshape(n_tp * 2 * head, 384)
            res = jnp.dot(lhs, w_cols, preferred_element_type=jnp.float32).astype(jnp.bfloat16)
            yst[2 * half:2 * half + 2, :, col:col + 384] = res.reshape(2, rows, 384)
        for z_dst in (2 * half, 2 * half + 1):
            @pl.when(my_z != z_dst)
            def _(z_dst=z_dst):
                y_copy(z_dst, my_z).start()

            @pl.when(my_z == z_dst)
            def _(z_dst=z_dst):
                yv[:, pl.ds(pl.multiple_of(my_z * cols, 128), cols)] = yst[z_dst]

    for z_src in range(NY):
        @pl.when(my_z != z_src)
        def _(z_src=z_src):
            y_copy(z_src, z_src).wait_recv()
    y_out = pltpu.make_async_copy(yv, y_hbm, y_sem)
    y_out.start()
    for tile in range(2 * n_tp // 2):
        for z_dst in range(NY):
            mine = (tile % NY == my_y) & (my_z == z_dst)

            @pl.when(jnp.logical_not(mine))
            def _(tile=tile, z_dst=z_dst):
                o_copy(tile, z_dst).wait_send()
    for z_dst in range(NY):
        @pl.when(my_z != z_dst)
        def _(z_dst=z_dst):
            y_copy(z_dst, my_z).wait_send()
    y_out.wait()


def attn_out(q_loc, kv_all, wo_rel):
    n_e, _, _, w_rows, cols = wo_rel.shape
    rows, two_head = q_loc.shape
    n_tp = NY * NY
    any_spec = pl.BlockSpec(memory_space=pl.ANY)
    n_keys = kv_all.shape[0] * rows
    dma = pltpu.SemaphoreType.DMA
    return pl.pallas_call(
        attn_out_kernel,
        out_shape=jax.ShapeDtypeStruct((rows // n_tp, NY * cols), jnp.bfloat16),
        in_specs=[any_spec] * 3,
        out_specs=any_spec,
        scratch_shapes=[
            pltpu.VMEM((rows, two_head), jnp.bfloat16),
            pltpu.VMEM((n_keys, two_head), jnp.bfloat16),
            pltpu.VMEM((n_tp, n_e, w_rows, cols), jnp.bfloat16),
            pltpu.VMEM((2 * TQ, WINDOW + TQ), jnp.float32),
            pltpu.VMEM((2 * TQ, two_head // 2), jnp.float32),
            pltpu.VMEM((2 * TQ, two_head // 2), jnp.float32),
            pltpu.VMEM((2 * TQ, two_head // 2), jnp.float32),
            pltpu.VMEM((2 * TQ, two_head // 2), jnp.float32),
            pltpu.VMEM((rows, two_head), jnp.bfloat16),
            pltpu.VMEM((NY, rows // n_tp, n_tp * two_head), jnp.bfloat16),
            pltpu.VMEM((NY, rows // n_tp, cols), jnp.bfloat16),
            pltpu.VMEM((rows // n_tp, NY * cols), jnp.bfloat16),
            dma, dma((16,)), dma((n_tp,)), dma((n_tp, NY)), dma((NY, n_tp)), dma((NY,)), dma((NY,)), dma,
        ],
        compiler_params=pltpu.CompilerParams(collective_id=1, has_side_effects=True, vmem_limit_bytes=62 * 1024 * 1024),
        cost_estimate=pl.CostEstimate(flops=20_000_000_000, bytes_accessed=30_000_000, transcendentals=16_000_000),
        name="attn_out",
    )(q_loc, kv_all, wo_rel)


def gather_w_out(w_out):
    heads_loc, head_dim, d_model = w_out.shape
    sp_rank, tp_rank = lax.axis_index("sp"), lax.axis_index("tp")
    n_sp = lax.axis_size("sp")
    rows = heads_loc * head_dim // n_sp
    flat = w_out.reshape(heads_loc * head_dim, d_model)
    mine = lax.dynamic_slice_in_dim(flat, sp_rank * rows, rows, 0)
    my_z = tp_rank // NY
    pieces = []
    for k in range(NY):
        piece = lax.dynamic_slice_in_dim(mine, ((my_z + k) % NY) * (d_model // NY), d_model // NY, 1)
        if k:
            piece = lax.ppermute(piece, "tp", [(t, ((t // NY + k) % NY) * NY + t % NY) for t in range(NY * NY)])
        pieces.append(piece)
    part = jnp.stack(pieces)
    part = lax.all_gather(part, "tp", axis=0, axis_index_groups=[[NY * z + y for y in range(NY)] for z in range(NY)])
    return lax.all_gather(part, "sp", axis=0)


def solution(mesh):
    def local_attn(x_part, w_query, w_key, w_value, w_out):
        d_model = x_part.shape[1]
        wo_rel = gather_w_out(w_out)
        x_block = lax.all_gather(x_part, "tp", axis=0, tiled=True)
        rows = x_block.shape[0]

        def project(weight):
            return jnp.dot(x_block, weight.reshape(d_model, -1), preferred_element_type=jnp.float32).astype(jnp.bfloat16)

        q_loc = project(w_query)
        kv_loc = jnp.concatenate([project(w_key), project(w_value)], axis=1)
        kv_all = lax.all_gather(kv_loc.reshape(2, rows // 2, -1), "sp", axis=0)
        return attn_out(q_loc, kv_all, wo_rel)

    return jax.shard_map(local_attn, mesh=mesh, in_specs=(P(("dp", "sp", "tp"), None), P(None, "tp", None), P(None, "tp", None), P(None, "tp", None), P("tp", None, None)), out_specs=P(("dp", "sp", "tp"), None), check_vma=False)
```

```python
import functools

import jax
import jax.numpy as jnp
from jax import lax
from jax.experimental import pallas as pl
from jax.experimental.pallas import tpu as pltpu
from jax.sharding import PartitionSpec as P

WINDOW = 4096
NEG_BIG = -1e30
LOG2E = 1.4426950408889634
MESH = pl.DeviceIdType.MESH
NY = 4
TQ = 256
WIDE = 768
N_WIDE = (WINDOW - TQ) // WIDE


def dot_nt(lhs, rhs):
    return lax.dot_general(lhs, rhs, (((1,), (1,)), ((), ())), preferred_element_type=jnp.float32)


def layer_kernel(x_hbm, wq_hbm, wk_hbm, wv_hbm, wo_hbm, y_hbm, xg, w_v, q_v, kv_v, wo_v, s_v, mx_v, mb_v, l_v, acc_v, o_st, og, yst, yv,
                 x_sem, w_sem, x_send, x_recv, kv_send, kv_recv, wo_sem, wo_send, wo_recv, sl_send, sl_recv, o_send, o_recv, y_send, y_recv, y_sem):
    sp = lax.axis_index("sp")
    tp = lax.axis_index("tp")
    my_z, my_y = tp // NY, tp % NY
    my_x, my_c = sp // 2, sp % 2
    n_tp = NY * NY
    n_sp = 8
    chunk = kv_v.shape[0] // (2 * n_sp)
    head = kv_v.shape[1] // 2
    cols = yst.shape[2]
    rows = yst.shape[1]
    coef = head ** -0.5 * LOG2E
    n_back = WINDOW // chunk
    part = rows // 4

    x_load = pltpu.make_async_copy(x_hbm, xg.at[tp], x_sem)
    x_load.start()
    w_loads = (pltpu.make_async_copy(wq_hbm, w_v.at[:, 0:2 * head], w_sem.at[0]),
               pltpu.make_async_copy(wk_hbm, w_v.at[:, 2 * head:3 * head], w_sem.at[1]),
               pltpu.make_async_copy(wv_hbm, w_v.at[:, 3 * head:4 * head], w_sem.at[2]))
    for load in w_loads:
        load.start()

    barrier = pltpu.get_barrier_semaphore()
    for step in range(1, n_tp):
        pl.semaphore_signal(barrier, inc=1, device_id={"tp": (tp + step) % n_tp}, device_id_type=MESH)
    for step in range(1, n_sp):
        pl.semaphore_signal(barrier, inc=1, device_id={"sp": (sp + step) % n_sp}, device_id_type=MESH)
    pl.semaphore_wait(barrier, n_tp + n_sp - 2)

    zm, zp, zo = (my_z + 3) % NY, (my_z + 1) % NY, (my_z + 2) % NY
    ym, yp, yo = (my_y + 3) % NY, (my_y + 1) % NY, (my_y + 2) % NY
    sends = []

    def x_copy(src_tp, first, count, dst_tp, slot):
        ref = xg.at[src_tp, pl.ds(first * part, count * part)]
        return pltpu.make_async_remote_copy(src_ref=ref, dst_ref=ref, send_sem=x_send.at[slot], recv_sem=x_recv.at[src_tp, first],
                                            device_id={"tp": dst_tp}, device_id_type=MESH)

    def x_put(z_src, y_src, first, count, z_dst, y_dst):
        copy = x_copy(NY * z_src + y_src, first, count, NY * z_dst + y_dst, len(sends))
        sends.append(copy)
        copy.start()

    def x_wait(z_src, y_src, first, count):
        x_copy(NY * z_src + y_src, first, count, 0, 0).wait_recv()

    def kv_copy(src_blk, first, count, half, back, dst_sp):
        ref = kv_v.at[pl.ds(pl.multiple_of(src_blk * chunk + first, rows), count)]
        return pltpu.make_async_remote_copy(src_ref=ref, dst_ref=ref, send_sem=kv_send.at[half, back - 1], recv_sem=kv_recv.at[src_blk],
                                            device_id={"sp": dst_sp}, device_id_type=MESH)

    def kv_target(blk, back):
        tgt = blk + back
        low = tgt < n_sp
        dst = jnp.where(low, tgt, 2 * n_sp - 1 - tgt)
        return dst, (tgt < 2 * n_sp) & (low | (blk >= n_sp) | (dst < sp))

    def project(tiles):
        def body(idx, carry):
            tile = tiles[0]
            for other in range(1, len(tiles)):
                tile = jnp.where(idx == other, tiles[other], tile)
            prod = jnp.dot(xg[tile], w_v[...], preferred_element_type=jnp.float32).astype(jnp.bfloat16)
            half = tile // (n_tp // 2)
            blk = jnp.where(half == 0, sp, 2 * n_sp - 1 - sp)
            first = (tile % (n_tp // 2)) * rows
            q_v[pl.ds(pl.multiple_of(tile * rows, rows), rows), :] = prod[:, :2 * head]
            kv_v[pl.ds(pl.multiple_of(blk * chunk + first, rows), rows), :] = prod[:, 2 * head:]
            for back in range(1, n_back + 1):
                dst, wanted = kv_target(blk, back)

                @pl.when(wanted)
                def _(back=back, dst=dst):
                    kv_copy(blk, first, rows, half, back, dst).start()
            return carry

        lax.fori_loop(0, len(tiles), body, 0)

    def tile_of(z_idx, y_idx):
        return NY * z_idx + y_idx

    x_load.wait()
    for z_dst, y_dst, first in ((zp, my_y, 0), (zm, my_y, 0), (my_z, yp, 2), (my_z, ym, 2), (my_z, yp, 0), (my_z, ym, 0), (zp, my_y, 2), (zm, my_y, 2)):
        x_put(my_z, my_y, first, 2, z_dst, y_dst)
    for load in w_loads:
        load.wait()
    project([tp])

    def take_items(z_item, y_item):
        for y_src, first, y_dst in ((ym, 0, yp), (yp, 1, ym)):
            x_wait(z_item, y_src, 0, 2)
            x_put(z_item, y_src, first, 1, my_z, y_dst)
        for z_src, first, z_dst in ((zm, 2, zp), (zp, 3, zm)):
            x_wait(z_src, y_item, 2, 2)
            x_put(z_src, y_item, first, 1, z_dst, my_y)

    def send_items(z_item, y_item):
        for y_dst in (yp, ym):
            x_put(z_item, my_y, 0, 2, my_z, y_dst)
        for z_dst in (zp, zm):
            x_put(my_z, y_item, 2, 2, z_dst, my_y)

    def take_far(z_item, y_item):
        for first in range(2):
            x_wait(z_item, yo, first, 1)
            x_wait(zo, y_item, 2 + first, 1)

    for z_src, first, z_dst in ((zm, 0, zp), (zp, 1, zm)):
        x_wait(z_src, my_y, 0, 2)
        x_put(z_src, my_y, first, 1, z_dst, my_y)
    for y_src, first, y_dst in ((ym, 2, yp), (yp, 3, ym)):
        x_wait(my_z, y_src, 2, 2)
        x_put(my_z, y_src, first, 1, my_z, y_dst)
    send_items(zm, ym)
    send_items(zp, yp)
    take_items(my_z, my_y)
    project([tile_of(zm, my_y), tile_of(zp, my_y), tile_of(my_z, ym), tile_of(my_z, yp)])
    for first in range(2):
        x_wait(zo, my_y, first, 1)
        x_wait(my_z, yo, 2 + first, 1)
    send_items(zo, yo)
    take_items(zm, ym)
    project([tile_of(zm, ym)])
    take_items(zp, yp)
    project([tile_of(zm, yp), tile_of(zp, ym), tile_of(zp, yp)])
    take_far(my_z, my_y)
    project([tile_of(my_z, yo), tile_of(zo, my_y)])
    take_items(zo, yo)

    def wo_copy(step):
        dst = (tp + step) % n_tp
        src_ref = wo_hbm.at[sp, :, pl.ds(pl.multiple_of((dst // NY) * cols, 128), cols)]
        return pltpu.make_async_remote_copy(src_ref=src_ref, dst_ref=wo_v.at[tp, sp], send_sem=wo_send.at[step], recv_sem=wo_recv.at[tp],
                                            device_id={"tp": dst}, device_id_type=MESH)

    wo_own = pltpu.make_async_copy(wo_hbm.at[sp, :, pl.ds(pl.multiple_of(my_z * cols, 128), cols)], wo_v.at[tp, sp], wo_sem)
    wo_own.start()
    for step in range(1, n_tp):
        wo_copy(step).start()

    take_far(zm, ym)
    project([tile_of(zm, yo), tile_of(zo, ym)])
    take_far(zp, yp)
    project([tile_of(zp, yo), tile_of(zo, yp)])
    take_far(zo, yo)
    project([tile_of(zo, yo)])

    x_left, x_right, x_far = (my_x + 3) % NY, (my_x + 1) % NY, (my_x + 2) % NY
    slabs = []

    def slab_copy(x_src, c_src, first, count, x_dst, c_dst, slot):
        ref = wo_v.at[pl.ds(first * (n_tp // 2), count * (n_tp // 2)), 2 * x_src + c_src]
        return pltpu.make_async_remote_copy(src_ref=ref, dst_ref=ref, send_sem=sl_send.at[slot], recv_sem=sl_recv.at[2 * x_src + c_src, first],
                                            device_id={"sp": 2 * x_dst + c_dst}, device_id_type=MESH)

    def slab_put(x_src, first, count, x_dst, c_dst):
        copy = slab_copy(x_src, my_c, first, count, x_dst, c_dst, len(slabs))
        slabs.append(copy)
        copy.start()

    def slab_wait(x_src, c_src, first, count):
        slab_copy(x_src, c_src, first, count, 0, 0, 0).wait_recv()

    def wo_first():
        wo_own.wait()
        for step in range(1, n_tp):
            src = (tp + step) % n_tp
            pltpu.make_async_remote_copy(src_ref=wo_v.at[src, sp], dst_ref=wo_v.at[src, sp], send_sem=wo_send.at[step], recv_sem=wo_recv.at[src],
                                         device_id={"tp": src}, device_id_type=MESH).wait_recv()
        for x_dst in (x_right, x_left):
            slab_put(my_x, 0, 2, x_dst, my_c)
        slab_put(my_x, 0, 2, my_x, 1 - my_c)

    def wo_second():
        for x_src, first, x_dst in ((x_left, 0, x_right), (x_right, 1, x_left)):
            slab_wait(x_src, my_c, 0, 2)
            slab_put(x_src, first, 1, x_dst, my_c)
        for x_src in (x_left, x_right):
            slab_put(x_src, 0, 2, my_x, 1 - my_c)

    def wo_third():
        for first in range(2):
            slab_wait(x_far, my_c, first, 1)
            slab_put(x_far, first, 1, my_x, 1 - my_c)

    def wo_last():
        for x_src in (my_x, x_left, x_right):
            slab_wait(x_src, 1 - my_c, 0, 2)
        for first in range(2):
            slab_wait(x_far, 1 - my_c, first, 1)

    def low_needs(blk):
        return (blk < sp) & (blk >= sp - n_back)

    def high_needs(blk):
        return (blk < 2 * n_sp - 1 - sp) & (blk >= 2 * n_sp - 1 - sp - n_back) & (blk != sp) & jnp.logical_not(low_needs(blk))

    def kv_wait(needs):
        for blk in range(2 * n_sp - 1):
            @pl.when(needs(blk))
            def _(blk=blk):
                kv_copy(blk, 0, chunk, 0, 1, 0).wait_recv()

    row_i = lax.broadcasted_iota(jnp.int32, (2 * TQ, TQ), 0) % TQ
    col_i = lax.broadcasted_iota(jnp.int32, (2 * TQ, TQ), 1)

    def lane_max(scores):
        best = scores[:, 0:head]
        for idx in range(1, scores.shape[1] // head):
            best = jnp.maximum(best, scores[:, idx * head:(idx + 1) * head])
        return best

    def o_copy(tile, z_dst):
        y_dst, z_row = tile % NY, tile // NY
        src = o_st.at[pl.ds(pl.multiple_of(tile * rows, rows), rows)]
        dst = og.at[z_row, :, pl.ds(pl.multiple_of(tp * 2 * head, 2 * head), 2 * head)]
        return pltpu.make_async_remote_copy(src_ref=src, dst_ref=dst, send_sem=o_send.at[tile, z_dst], recv_sem=o_recv.at[z_row, tp],
                                            device_id={"tp": NY * z_dst + y_dst}, device_id_type=MESH)

    def attend(q_idx, gidx, wide, start_tile, n_steps, with_first):
        q_blk = q_v[pl.ds(pl.multiple_of(q_idx * TQ, TQ), TQ), :]
        q_two = jnp.concatenate([q_blk[:, :head], q_blk[:, head:]], axis=0)

        def keys(tile, width):
            return kv_v[pl.ds(pl.multiple_of(tile * TQ, TQ), width), 0:head]

        def values(tile, width):
            return kv_v[pl.ds(pl.multiple_of(tile * TQ, TQ), width), head:2 * head]

        per = wide // TQ
        scores = jnp.where(col_i <= row_i, dot_nt(q_two, keys(gidx, TQ)), NEG_BIG)
        s_v[:, 0:TQ] = scores
        best = lane_max(scores)
        if with_first:
            scores = jnp.where(col_i > row_i, dot_nt(q_two, keys(gidx - WINDOW // TQ, TQ)), NEG_BIG)
            s_v[:, TQ:2 * TQ] = scores
            best = jnp.maximum(best, lane_max(scores))
        mx_v[...] = best

        def score_step(idx, carry):
            part = dot_nt(q_two, keys(start_tile + per * idx, wide))
            s_v[:, pl.ds(pl.multiple_of(2 * TQ + idx * wide, TQ), wide)] = part
            mx_v[...] = jnp.maximum(mx_v[...], lane_max(part))
            return carry

        lax.fori_loop(0, n_steps, score_step, 0)
        row_best = jnp.max(mx_v[...], axis=1, keepdims=True) * coef
        mb_v[...] = jnp.broadcast_to(row_best, mb_v.shape)

        def probs(col, width):
            base = mb_v[...]
            total = None
            parts = []
            for idx in range(width // head):
                part = jnp.exp2(s_v[:, pl.ds(pl.multiple_of(col + idx * head, head), head)] * coef - base)
                total = part if total is None else total + part
                parts.append(part.astype(jnp.bfloat16))
            return jnp.concatenate(parts, axis=1), total

        prob, total = probs(0, TQ)
        acc = jnp.dot(prob, values(gidx, TQ), preferred_element_type=jnp.float32)
        if with_first:
            prob, total_b = probs(TQ, TQ)
            total = total + total_b
            acc = acc + jnp.dot(prob, values(gidx - WINDOW // TQ, TQ), preferred_element_type=jnp.float32)
        l_v[...] = total
        acc_v[...] = acc

        def value_step(idx, carry):
            prob, total = probs(2 * TQ + idx * wide, wide)
            l_v[...] += total
            acc_v[...] += jnp.dot(prob, values(start_tile + per * idx, wide), preferred_element_type=jnp.float32)
            return carry

        lax.fori_loop(0, n_steps, value_step, 0)
        denom = jnp.sum(l_v[...], axis=1, keepdims=True)
        out = (acc_v[...] / denom).astype(jnp.bfloat16)
        out = jnp.concatenate([out[:TQ], out[TQ:]], axis=1)
        o_st[pl.ds(pl.multiple_of(q_idx * TQ, TQ), TQ), :] = out

    def q_step(q_idx, carry):
        tiles = chunk // TQ
        blk = jnp.where(q_idx < tiles, sp, 2 * n_sp - 1 - sp)
        gidx = blk * tiles + q_idx % tiles

        @pl.when(gidx >= WINDOW // TQ)
        def _():
            attend(q_idx, gidx, WIDE, gidx - WINDOW // TQ + 1, N_WIDE, True)

        @pl.when(gidx < WINDOW // TQ)
        def _():
            attend(q_idx, gidx, TQ, 0, gidx, False)

        for sub in range(2):
            tile = 2 * q_idx + sub
            for z_dst in range(NY):
                mine = (tile % NY == my_y) & (my_z == z_dst)

                @pl.when(jnp.logical_not(mine))
                def _(tile=tile, z_dst=z_dst):
                    o_copy(tile, z_dst).start()

            @pl.when(tile % NY == my_y)
            def _(tile=tile):
                og[tile // NY, :, pl.ds(pl.multiple_of(tp * 2 * head, 2 * head), 2 * head)] = \
                    o_st[pl.ds(pl.multiple_of(tile * rows, rows), rows), :]
        return carry

    kv_wait(low_needs)
    lax.fori_loop(0, 3, q_step, 0)
    wo_first()
    lax.fori_loop(3, 4, q_step, 0)
    kv_wait(high_needs)
    lax.fori_loop(4, 7, q_step, 0)
    wo_second()
    lax.fori_loop(7, 8, q_step, 0)
    wo_third()

    def o_arrival(z_row, src):
        dst = og.at[z_row, :, pl.ds(src * 2 * head, 2 * head)]
        return pltpu.make_async_remote_copy(src_ref=o_st.at[pl.ds(0, rows)], dst_ref=dst, send_sem=o_send.at[0, 0],
                                            recv_sem=o_recv.at[z_row, src], device_id={"tp": 0}, device_id_type=MESH)

    def y_copy(z_dst, z_src):
        return pltpu.make_async_remote_copy(
            src_ref=yst.at[z_dst], dst_ref=yv.at[:, pl.ds(pl.multiple_of(z_src * cols, 128), cols)],
            send_sem=y_send.at[z_dst], recv_sem=y_recv.at[z_src], device_id={"tp": NY * z_dst + my_y}, device_id_type=MESH)

    wo_last()
    for half in range(2):
        for z_row in (2 * half, 2 * half + 1):
            for src in range(n_tp):
                @pl.when(tp != src)
                def _(z_row=z_row, src=src):
                    o_arrival(z_row, src).wait_recv()
        lhs = og[2 * half:2 * half + 2].reshape(2 * rows, n_tp * 2 * head)
        for col in range(0, cols, 384):
            w_cols = wo_v[:, :, :, col:col + 384].reshape(n_tp * 2 * head, 384)
            res = jnp.dot(lhs, w_cols, preferred_element_type=jnp.float32).astype(jnp.bfloat16)
            yst[2 * half:2 * half + 2, :, col:col + 384] = res.reshape(2, rows, 384)
        for z_dst in (2 * half, 2 * half + 1):
            @pl.when(my_z != z_dst)
            def _(z_dst=z_dst):
                y_copy(z_dst, my_z).start()

            @pl.when(my_z == z_dst)
            def _(z_dst=z_dst):
                yv[:, pl.ds(pl.multiple_of(my_z * cols, 128), cols)] = yst[z_dst]

    for z_src in range(NY):
        @pl.when(my_z != z_src)
        def _(z_src=z_src):
            y_copy(z_src, z_src).wait_recv()
    y_out = pltpu.make_async_copy(yv, y_hbm, y_sem)
    y_out.start()
    for tile in range(2 * n_tp // 2):
        for z_dst in range(NY):
            mine = (tile % NY == my_y) & (my_z == z_dst)

            @pl.when(jnp.logical_not(mine))
            def _(tile=tile, z_dst=z_dst):
                o_copy(tile, z_dst).wait_send()
    for z_dst in range(NY):
        @pl.when(my_z != z_dst)
        def _(z_dst=z_dst):
            y_copy(z_dst, my_z).wait_send()
    for copy in sends + slabs:
        copy.wait_send()
    for step in range(1, n_tp):
        wo_copy(step).wait_send()
    for half in range(2):
        blk = (sp, 2 * n_sp - 1 - sp)[half]
        for back in range(1, n_back + 1):
            dst, wanted = kv_target(blk, back)

            @pl.when(wanted)
            def _(half=half, blk=blk, back=back, dst=dst):
                kv_copy(blk, 0, chunk, half, back, dst).wait_send()
    y_out.wait()


def solution(mesh):
    n_sp, n_tp = mesh.shape["sp"], mesh.shape["tp"]

    def local_attn(x_part, w_query, w_key, w_value, w_out):
        rows, d_model = x_part.shape
        heads_loc, head = w_query.shape[1], w_query.shape[2]
        two_head = heads_loc * head
        seq_loc = rows * n_tp
        cols = d_model // NY
        any_spec = pl.BlockSpec(memory_space=pl.ANY)
        dma = pltpu.SemaphoreType.DMA
        bf16, f32 = jnp.bfloat16, jnp.float32
        wo_rows = w_out.shape[0] * w_out.shape[1] // n_sp
        return pl.pallas_call(
            layer_kernel,
            out_shape=jax.ShapeDtypeStruct((rows, d_model), bf16),
            in_specs=[any_spec] * 5,
            out_specs=any_spec,
            scratch_shapes=[
                pltpu.VMEM((n_tp, rows, d_model), bf16),
                pltpu.VMEM((d_model, 2 * two_head), bf16),
                pltpu.VMEM((seq_loc, two_head), bf16),
                pltpu.VMEM((n_sp * seq_loc, two_head), bf16),
                pltpu.VMEM((n_tp, n_sp, wo_rows, cols), bf16),
                pltpu.VMEM((2 * TQ, WINDOW + TQ), f32),
                pltpu.VMEM((2 * TQ, head), f32),
                pltpu.VMEM((2 * TQ, head), f32),
                pltpu.VMEM((2 * TQ, head), f32),
                pltpu.VMEM((2 * TQ, head), f32),
                pltpu.VMEM((seq_loc, two_head), bf16),
                pltpu.VMEM((NY, rows, n_tp * two_head), bf16),
                pltpu.VMEM((NY, rows, cols), bf16),
                pltpu.VMEM((rows, d_model), bf16),
                dma, dma((3,)), dma((48,)), dma((n_tp, 4)), dma((2, 4)), dma((2 * n_sp,)), dma, dma((n_tp,)), dma((n_tp,)),
                dma((16,)), dma((n_sp, 2)), dma((n_tp, NY)), dma((NY, n_tp)), dma((NY,)), dma((NY,)), dma,
            ],
            compiler_params=pltpu.CompilerParams(collective_id=1, has_side_effects=True, vmem_limit_bytes=67043328),
            name="layer",
        )(x_part, w_query.reshape(d_model, two_head), w_key.reshape(d_model, head), w_value.reshape(d_model, head),
          w_out.reshape(n_sp, wo_rows, d_model))

    return jax.shard_map(local_attn, mesh=mesh, in_specs=(P(("dp", "sp", "tp"), None), P(None, "tp", None), P(None, "tp", None), P(None, "tp", None), P("tp", None, None)), out_specs=P(("dp", "sp", "tp"), None), check_vma=False)
```

```python
import functools

import jax
import jax.numpy as jnp
from jax import lax
from jax.experimental import pallas as pl
from jax.experimental.pallas import tpu as pltpu
from jax.sharding import PartitionSpec as P

WINDOW = 4096
NEG_BIG = -1e30
LOG2E = 1.4426950408889634
MESH = pl.DeviceIdType.MESH
NY = 4
TQ = 256
WIDE = 768
N_WIDE = (WINDOW - TQ) // WIDE


def dot_nt(lhs, rhs):
    return lax.dot_general(lhs, rhs, (((1,), (1,)), ((), ())), preferred_element_type=jnp.float32)


def layer_kernel(x_hbm, wq_hbm, wk_hbm, wv_hbm, wo_hbm, y_hbm, xg, w_v, q_v, kv_v, q_st, kv_st, wo_v, s_v, mx_v, mb_v, l_v, acc_v, o_st, og,
                 yst, yv, x_sem, wl_sem, x_send, x_recv, w_send, w_recv, share_send, share_recv, a_send, a_recv, kv_send, kv_recv, wo_sem,
                 wo_send, wo_recv, sl_send, sl_recv, o_send, o_recv, y_send, y_recv, y_sem):
    sp = lax.axis_index("sp")
    tp = lax.axis_index("tp")
    my_z, my_y = tp // NY, tp % NY
    my_x, my_c = sp // 2, sp % 2
    n_tp = NY * NY
    n_sp = 8
    chunk = kv_v.shape[0] // (2 * n_sp)
    head = kv_v.shape[1] // 2
    cols = yst.shape[2]
    rows = yst.shape[1]
    part = NY * rows
    coef = head ** -0.5 * LOG2E
    d_half = w_v.shape[1] // 2
    s_rows = d_half // 6
    d_rows = 2 * s_rows

    x_load = pltpu.make_async_copy(x_hbm, xg.at[my_y], x_sem)
    x_load.start()
    w_loads = (pltpu.make_async_copy(wq_hbm, w_v.at[my_z, :, 0:2 * head], wl_sem.at[0]),
               pltpu.make_async_copy(wk_hbm, w_v.at[my_z, :, 2 * head:3 * head], wl_sem.at[1]),
               pltpu.make_async_copy(wv_hbm, w_v.at[my_z, :, 3 * head:4 * head], wl_sem.at[2]))
    for load in w_loads:
        load.start()

    barrier = pltpu.get_barrier_semaphore()
    for step in range(1, n_tp):
        pl.semaphore_signal(barrier, inc=1, device_id={"tp": (tp + step) % n_tp}, device_id_type=MESH)
    for step in range(1, n_sp):
        pl.semaphore_signal(barrier, inc=1, device_id={"sp": (sp + step) % n_sp}, device_id_type=MESH)
    pl.semaphore_wait(barrier, n_tp + n_sp - 2)

    zm, zp, zo = (my_z + 3) % NY, (my_z + 1) % NY, (my_z + 2) % NY
    ym, yp, yo = (my_y + 3) % NY, (my_y + 1) % NY, (my_y + 2) % NY
    x_left, x_right, x_far = (my_x + 3) % NY, (my_x + 1) % NY, (my_x + 2) % NY
    sends = []
    n_sends = [0, 0]

    def x_copy(y_src, first, count, y_dst, slot):
        ref = xg.at[y_src, pl.ds(first * (rows // 2), count * (rows // 2))]
        return pltpu.make_async_remote_copy(src_ref=ref, dst_ref=ref, send_sem=x_send.at[slot], recv_sem=x_recv.at[y_src, first],
                                            device_id={"tp": NY * my_z + y_dst}, device_id_type=MESH)

    def x_put(y_src, first, count, y_dst):
        copy = x_copy(y_src, first, count, y_dst, n_sends[0])
        n_sends[0] += 1
        sends.append(copy)
        copy.start()

    def x_wait(y_src, first, count):
        x_copy(y_src, first, count, 0, 0).wait_recv()

    def w_copy(z_src, x_src, first, count, dst, slot):
        size = d_rows if x_src is None else s_rows
        base = my_c * d_half + (0 if x_src is None else d_rows + x_src * s_rows)
        ref = w_v.at[z_src, pl.ds(pl.multiple_of(base + first * (size // 2), 64), count * (size // 2))]
        return pltpu.make_async_remote_copy(src_ref=ref, dst_ref=ref, send_sem=w_send.at[slot],
                                            recv_sem=w_recv.at[z_src, NY if x_src is None else x_src, first], device_id=dst, device_id_type=MESH)

    def w_put(z_src, x_src, first, count, dst):
        copy = w_copy(z_src, x_src, first, count, dst, n_sends[1])
        n_sends[1] += 1
        sends.append(copy)
        copy.start()

    def w_wait(z_src, x_src, first, count):
        w_copy(z_src, x_src, first, count, {"tp": 0}, 0).wait_recv()

    def to_z(z_dst):
        return {"tp": NY * z_dst + my_y}

    def to_x(x_dst):
        return {"sp": 2 * x_dst + my_c}

    def share_copy(z_src, core, slot):
        ref = w_v.at[z_src, pl.ds(pl.multiple_of(core * d_half, 64), d_half)]
        return pltpu.make_async_remote_copy(src_ref=ref, dst_ref=ref, send_sem=share_send.at[slot], recv_sem=share_recv.at[z_src],
                                            device_id={"sp": 2 * my_x + 1 - my_c}, device_id_type=MESH)

    def blk_of(z_idx):
        return jnp.where(z_idx < NY // 2, sp, 2 * n_sp - 1 - sp)

    def kv_rows(z_idx):
        return pl.multiple_of(blk_of(z_idx) * chunk + (z_idx % 2) * part, part)

    def own_products(y_list):
        def body(idx, carry):
            y_idx = y_list[0]
            for other in range(1, len(y_list)):
                y_idx = jnp.where(idx == other, y_list[other], y_idx)
            prod = jnp.dot(xg[y_idx], w_v[my_z], preferred_element_type=jnp.float32).astype(jnp.bfloat16)
            q_v[pl.ds(pl.multiple_of(my_z * part + y_idx * rows, rows), rows), :] = prod[:, :2 * head]
            kv_v[pl.ds(pl.multiple_of(kv_rows(my_z) + y_idx * rows, rows), rows), :] = prod[:, 2 * head:]
            return carry

        lax.fori_loop(0, len(y_list), body, 0)

    def a_copy(kind, z_src, z_dst, slot):
        if kind:
            src, dst = q_st.at[slot], q_v.at[pl.ds(pl.multiple_of(z_src * part, part), part)]
        else:
            src, dst = kv_st.at[slot], kv_v.at[pl.ds(kv_rows(z_src), part)]
        return pltpu.make_async_remote_copy(src_ref=src, dst_ref=dst, send_sem=a_send.at[kind, slot], recv_sem=a_recv.at[kind, z_src],
                                            device_id=to_z(z_dst), device_id_type=MESH)

    def products(z_dst, slot):
        def body(idx, carry):
            lhs = xg[pl.ds(2 * idx, 2)].reshape(2 * rows, xg.shape[2])
            prod = jnp.dot(lhs, w_v[z_dst], preferred_element_type=jnp.float32).astype(jnp.bfloat16)
            at = pl.ds(pl.multiple_of(idx * 2 * rows, 2 * rows), 2 * rows)
            q_st[slot, at, :] = prod[:, :2 * head]
            kv_st[slot, at, :] = prod[:, 2 * head:]
            return carry

        lax.fori_loop(0, 2, body, 0)
        for kind in range(2):
            a_copy(kind, my_z, z_dst, slot).start()

    def a_wait(kind, z_src):
        a_copy(kind, z_src, 0, 0).wait_recv()

    def kv_part(pair, core, z_idx, kind, dst):
        blk = jnp.where(pair < NY, 2 * pair + core, 2 * pair + 1 - core)
        ref = kv_v.at[pl.ds(pl.multiple_of(blk * chunk + (z_idx % 2) * part, part), part)]
        return pltpu.make_async_remote_copy(src_ref=ref, dst_ref=ref, send_sem=kv_send.at[z_idx, kind], recv_sem=kv_recv.at[blk, z_idx % 2],
                                            device_id=dst, device_id_type=MESH)

    partner = {"sp": 2 * my_x + 1 - my_c}

    def own_pair(z_idx):
        return jnp.where(z_idx < NY // 2, my_x, 2 * NY - 1 - my_x)

    def own_next(z_idx):
        low = z_idx < NY // 2
        return jnp.where(low, jnp.where(my_x < NY - 1, my_x + 1, NY - 2), my_x - 1), low | (my_x >= 1)

    def direct_in(z_idx):
        low = z_idx < NY // 2
        return jnp.where(low, my_x - 1, 2 * NY - 2 - my_x), (low & (my_x >= 1)) | (jnp.logical_not(low) & (my_x < NY - 1))

    def direct_next(z_idx):
        return jnp.where(z_idx < NY // 2, my_x + 1, my_x - 1), (my_x >= 1) & (my_x < NY - 1)

    def relay_in(z_idx):
        low = z_idx < NY // 2
        return jnp.where(low, my_x - 2, 2 * NY - 3 - my_x), (low & (my_x >= 2)) | (jnp.logical_not(low) & (my_x < NY - 2))

    def turn_in(z_idx):
        return NY - 1, (z_idx < NY // 2) & (my_x == NY - 2)

    def kv_own(z_idx, act):
        dst, wanted = own_next(z_idx)

        @pl.when(wanted)
        def _():
            act(kv_part(own_pair(z_idx), my_c, z_idx, 1, to_x(dst)))

        act(kv_part(own_pair(z_idx), my_c, z_idx, 0, partner))

    def kv_direct(z_idx, act, arrive):
        pair, wanted = direct_in(z_idx)

        @pl.when(wanted)
        def _():
            if arrive:
                kv_part(pair, my_c, z_idx, 2, partner).wait_recv()
            dst, more = direct_next(z_idx)

            @pl.when(more)
            def _():
                act(kv_part(pair, my_c, z_idx, 3, to_x(dst)))

            act(kv_part(pair, my_c, z_idx, 2, partner))

    def kv_relay(z_idx, act, arrive):
        for kind, (pair, wanted) in ((4, relay_in(z_idx)), (5, turn_in(z_idx))):
            @pl.when(wanted)
            def _(kind=kind, pair=pair):
                copy = kv_part(pair, my_c, z_idx, kind, partner)
                if arrive:
                    copy.wait_recv()
                act(copy)

    def kv_from_partner(z_idx):
        kv_part(own_pair(z_idx), 1 - my_c, z_idx, 0, partner).wait_recv()
        for pair, wanted in (direct_in(z_idx), relay_in(z_idx), turn_in(z_idx)):
            @pl.when(wanted)
            def _(pair=pair):
                kv_part(pair, 1 - my_c, z_idx, 0, partner).wait_recv()

    def start(copy):
        copy.start()

    def done(copy):
        copy.wait_send()

    def wo_copy(step):
        dst = (tp + step) % n_tp
        src_ref = wo_hbm.at[sp, :, pl.ds(pl.multiple_of((dst // NY) * cols, 128), cols)]
        return pltpu.make_async_remote_copy(src_ref=src_ref, dst_ref=wo_v.at[tp, sp], send_sem=wo_send.at[step], recv_sem=wo_recv.at[tp],
                                            device_id={"tp": dst}, device_id_type=MESH)

    slabs = []

    def slab_copy(x_src, c_src, first, count, x_dst, c_dst, slot):
        ref = wo_v.at[pl.ds(first * (n_tp // 2), count * (n_tp // 2)), 2 * x_src + c_src]
        return pltpu.make_async_remote_copy(src_ref=ref, dst_ref=ref, send_sem=sl_send.at[slot], recv_sem=sl_recv.at[2 * x_src + c_src, first],
                                            device_id={"sp": 2 * x_dst + c_dst}, device_id_type=MESH)

    def slab_put(x_src, first, count, x_dst, c_dst):
        copy = slab_copy(x_src, my_c, first, count, x_dst, c_dst, len(slabs))
        slabs.append(copy)
        copy.start()

    def slab_wait(x_src, c_src, first, count):
        slab_copy(x_src, c_src, first, count, 0, 0, 0).wait_recv()

    def wo_first():
        wo_own.wait()
        for step in range(1, n_tp):
            src = (tp + step) % n_tp
            pltpu.make_async_remote_copy(src_ref=wo_v.at[src, sp], dst_ref=wo_v.at[src, sp], send_sem=wo_send.at[step], recv_sem=wo_recv.at[src],
                                         device_id={"tp": src}, device_id_type=MESH).wait_recv()
        for x_dst in (x_right, x_left):
            slab_put(my_x, 0, 2, x_dst, my_c)
        slab_put(my_x, 0, 2, my_x, 1 - my_c)

    def wo_second():
        for x_src, first, x_dst in ((x_left, 0, x_right), (x_right, 1, x_left)):
            slab_wait(x_src, my_c, 0, 2)
            slab_put(x_src, first, 1, x_dst, my_c)
        for x_src in (x_left, x_right):
            slab_put(x_src, 0, 2, my_x, 1 - my_c)

    def wo_third():
        for first in range(2):
            slab_wait(x_far, my_c, first, 1)
            slab_put(x_far, first, 1, my_x, 1 - my_c)

    def wo_last():
        for x_src in (my_x, x_left, x_right):
            slab_wait(x_src, 1 - my_c, 0, 2)
        for first in range(2):
            slab_wait(x_far, 1 - my_c, first, 1)

    x_load.wait()
    x_put(my_y, 0, 2, yp)
    x_put(my_y, 0, 2, ym)
    for load in w_loads:
        load.wait()
    for z_dst in (zp, zm):
        w_put(my_z, my_x, 0, 2, to_z(z_dst))
    for z_src, first, z_dst in ((zm, 0, zp), (zp, 1, zm)):
        w_wait(z_src, my_x, 0, 2)
        w_put(z_src, my_x, first, 1, to_z(z_dst))
        for x_dst in (x_right, x_left):
            w_put(z_src, my_x, 0, 2, to_x(x_dst))
    for z_dst in (zp, zm):
        w_put(my_z, None, 0, 2, to_z(z_dst))
    own_products([my_y])
    for z_src in (zm, zp):
        for x_src, first, x_dst in ((x_left, 0, x_right), (x_right, 1, x_left)):
            w_wait(z_src, x_src, 0, 2)
            w_put(z_src, x_src, first, 1, to_x(x_dst))
    for first in range(2):
        w_wait(zo, my_x, first, 1)
    for x_dst in (x_right, x_left):
        w_put(zo, my_x, 0, 2, to_x(x_dst))
    for y_src, first, y_dst in ((ym, 0, yp), (yp, 1, ym)):
        x_wait(y_src, 0, 2)
        x_put(y_src, first, 1, y_dst)
    for z_src, first, z_dst in ((zm, 0, zp), (zp, 1, zm)):
        w_wait(z_src, None, 0, 2)
        w_put(z_src, None, first, 1, to_z(z_dst))
    own_products([ym, yp])
    for slot, z_src in enumerate((zm, zp)):
        for first in range(2):
            w_wait(z_src, x_far, first, 1)
        share_copy(z_src, my_c, slot).start()
    for x_src, first, x_dst in ((x_left, 0, x_right), (x_right, 1, x_left)):
        w_wait(zo, x_src, 0, 2)
        w_put(zo, x_src, first, 1, to_x(x_dst))
    for first in range(2):
        x_wait(yo, first, 1)
    own_products([yo])
    kv_own(my_z, start)
    for slot, z_dst in enumerate((zm, zp)):
        share_copy(z_dst, 1 - my_c, slot).wait_recv()
        products(z_dst, slot)
    for first in range(2):
        w_wait(zo, None, first, 1)
        w_wait(zo, x_far, first, 1)
    share_copy(zo, my_c, 2).start()
    share_copy(zo, 1 - my_c, 2).wait_recv()
    products(zo, 2)
    kv_direct(my_z, start, True)
    for z_src in (zm, zp):
        a_wait(0, z_src)
        kv_own(z_src, start)
    kv_relay(my_z, start, True)
    wo_own = pltpu.make_async_copy(wo_hbm.at[sp, :, pl.ds(pl.multiple_of(my_z * cols, 128), cols)], wo_v.at[tp, sp], wo_sem)
    wo_own.start()
    for step in range(1, n_tp):
        wo_copy(step).start()

    for z_src in (zm, zp):
        kv_direct(z_src, start, True)
    a_wait(0, zo)
    kv_own(zo, start)
    for z_src in (zm, zp):
        kv_relay(z_src, start, True)
    kv_direct(zo, start, True)
    kv_relay(zo, start, True)
    wo_first()
    for z_src in (zm, zp, zo):
        a_wait(1, z_src)
    for z_idx in range(NY):
        kv_from_partner(z_idx)

    row_i = lax.broadcasted_iota(jnp.int32, (2 * TQ, TQ), 0) % TQ
    col_i = lax.broadcasted_iota(jnp.int32, (2 * TQ, TQ), 1)

    def lane_max(scores):
        best = scores[:, 0:head]
        for idx in range(1, scores.shape[1] // head):
            best = jnp.maximum(best, scores[:, idx * head:(idx + 1) * head])
        return best

    def o_copy(tile, z_dst):
        y_dst, z_row = tile % NY, tile // NY
        src = o_st.at[pl.ds(pl.multiple_of(tile * rows, rows), rows)]
        dst = og.at[z_row, :, pl.ds(pl.multiple_of(tp * 2 * head, 2 * head), 2 * head)]
        return pltpu.make_async_remote_copy(src_ref=src, dst_ref=dst, send_sem=o_send.at[tile, z_dst], recv_sem=o_recv.at[z_row, tp],
                                            device_id={"tp": NY * z_dst + y_dst}, device_id_type=MESH)

    def attend(q_idx, gidx, wide, start_tile, n_steps, with_first):
        q_blk = q_v[pl.ds(pl.multiple_of(q_idx * TQ, TQ), TQ), :]
        q_two = jnp.concatenate([q_blk[:, :head], q_blk[:, head:]], axis=0)

        def keys(tile, width):
            return kv_v[pl.ds(pl.multiple_of(tile * TQ, TQ), width), 0:head]

        def values(tile, width):
            return kv_v[pl.ds(pl.multiple_of(tile * TQ, TQ), width), head:2 * head]

        per = wide // TQ
        scores = jnp.where(col_i <= row_i, dot_nt(q_two, keys(gidx, TQ)), NEG_BIG)
        s_v[:, 0:TQ] = scores
        best = lane_max(scores)
        if with_first:
            scores = jnp.where(col_i > row_i, dot_nt(q_two, keys(gidx - WINDOW // TQ, TQ)), NEG_BIG)
            s_v[:, TQ:2 * TQ] = scores
            best = jnp.maximum(best, lane_max(scores))
        mx_v[...] = best

        def score_step(idx, carry):
            part = dot_nt(q_two, keys(start_tile + per * idx, wide))
            s_v[:, pl.ds(pl.multiple_of(2 * TQ + idx * wide, TQ), wide)] = part
            mx_v[...] = jnp.maximum(mx_v[...], lane_max(part))
            return carry

        lax.fori_loop(0, n_steps, score_step, 0)
        row_best = jnp.max(mx_v[...], axis=1, keepdims=True) * coef
        mb_v[...] = jnp.broadcast_to(row_best, mb_v.shape)

        def probs(col, width):
            base = mb_v[...]
            total = None
            parts = []
            for idx in range(width // head):
                part = jnp.exp2(s_v[:, pl.ds(pl.multiple_of(col + idx * head, head), head)] * coef - base)
                total = part if total is None else total + part
                parts.append(part.astype(jnp.bfloat16))
            return jnp.concatenate(parts, axis=1), total

        prob, total = probs(0, TQ)
        acc = jnp.dot(prob, values(gidx, TQ), preferred_element_type=jnp.float32)
        if with_first:
            prob, total_b = probs(TQ, TQ)
            total = total + total_b
            acc = acc + jnp.dot(prob, values(gidx - WINDOW // TQ, TQ), preferred_element_type=jnp.float32)
        l_v[...] = total
        acc_v[...] = acc

        def value_step(idx, carry):
            prob, total = probs(2 * TQ + idx * wide, wide)
            l_v[...] += total
            acc_v[...] += jnp.dot(prob, values(start_tile + per * idx, wide), preferred_element_type=jnp.float32)
            return carry

        lax.fori_loop(0, n_steps, value_step, 0)
        denom = jnp.sum(l_v[...], axis=1, keepdims=True)
        out = (acc_v[...] / denom).astype(jnp.bfloat16)
        out = jnp.concatenate([out[:TQ], out[TQ:]], axis=1)
        o_st[pl.ds(pl.multiple_of(q_idx * TQ, TQ), TQ), :] = out

    def q_step(q_idx, carry):
        tiles = chunk // TQ
        blk = jnp.where(q_idx < tiles, sp, 2 * n_sp - 1 - sp)
        gidx = blk * tiles + q_idx % tiles

        @pl.when(gidx >= WINDOW // TQ)
        def _():
            attend(q_idx, gidx, WIDE, gidx - WINDOW // TQ + 1, N_WIDE, True)

        @pl.when(gidx < WINDOW // TQ)
        def _():
            attend(q_idx, gidx, TQ, 0, gidx, False)

        for sub in range(2):
            tile = 2 * q_idx + sub
            for z_dst in range(NY):
                mine = (tile % NY == my_y) & (my_z == z_dst)

                @pl.when(jnp.logical_not(mine))
                def _(tile=tile, z_dst=z_dst):
                    o_copy(tile, z_dst).start()

            @pl.when(tile % NY == my_y)
            def _(tile=tile):
                og[tile // NY, :, pl.ds(pl.multiple_of(tp * 2 * head, 2 * head), 2 * head)] = \
                    o_st[pl.ds(pl.multiple_of(tile * rows, rows), rows), :]
        return carry

    lax.fori_loop(0, 5, q_step, 0)
    wo_second()
    lax.fori_loop(5, 2 * chunk // TQ, q_step, 0)
    wo_third()

    def o_arrival(z_row, src):
        dst = og.at[z_row, :, pl.ds(src * 2 * head, 2 * head)]
        return pltpu.make_async_remote_copy(src_ref=o_st.at[pl.ds(0, rows)], dst_ref=dst, send_sem=o_send.at[0, 0],
                                            recv_sem=o_recv.at[z_row, src], device_id={"tp": 0}, device_id_type=MESH)

    def y_copy(z_dst, z_src):
        return pltpu.make_async_remote_copy(
            src_ref=yst.at[z_dst], dst_ref=yv.at[:, pl.ds(pl.multiple_of(z_src * cols, 128), cols)],
            send_sem=y_send.at[z_dst], recv_sem=y_recv.at[z_src], device_id={"tp": NY * z_dst + my_y}, device_id_type=MESH)

    wo_last()
    for half in range(2):
        for z_row in (2 * half, 2 * half + 1):
            for src in range(n_tp):
                @pl.when(tp != src)
                def _(z_row=z_row, src=src):
                    o_arrival(z_row, src).wait_recv()
        lhs = og[2 * half:2 * half + 2].reshape(2 * rows, n_tp * 2 * head)
        for col in range(0, cols, 384):
            w_cols = wo_v[:, :, :, col:col + 384].reshape(n_tp * 2 * head, 384)
            res = jnp.dot(lhs, w_cols, preferred_element_type=jnp.float32).astype(jnp.bfloat16)
            yst[2 * half:2 * half + 2, :, col:col + 384] = res.reshape(2, rows, 384)
        for z_dst in (2 * half, 2 * half + 1):
            @pl.when(my_z != z_dst)
            def _(z_dst=z_dst):
                y_copy(z_dst, my_z).start()

            @pl.when(my_z == z_dst)
            def _(z_dst=z_dst):
                yv[:, pl.ds(pl.multiple_of(my_z * cols, 128), cols)] = yst[z_dst]

    for z_src in range(NY):
        @pl.when(my_z != z_src)
        def _(z_src=z_src):
            y_copy(z_src, z_src).wait_recv()
    y_out = pltpu.make_async_copy(yv, y_hbm, y_sem)
    y_out.start()
    for tile in range(2 * n_tp // 2):
        for z_dst in range(NY):
            mine = (tile % NY == my_y) & (my_z == z_dst)

            @pl.when(jnp.logical_not(mine))
            def _(tile=tile, z_dst=z_dst):
                o_copy(tile, z_dst).wait_send()
    for z_dst in range(NY):
        @pl.when(my_z != z_dst)
        def _(z_dst=z_dst):
            y_copy(z_dst, my_z).wait_send()
    for copy in sends + slabs:
        copy.wait_send()
    for step in range(1, n_tp):
        wo_copy(step).wait_send()
    for slot in range(3):
        share_copy(my_z, my_c, slot).wait_send()
        for kind in range(2):
            a_copy(kind, my_z, 0, slot).wait_send()
    for z_idx in range(NY):
        kv_own(z_idx, done)
        kv_direct(z_idx, done, False)
        kv_relay(z_idx, done, False)
    y_out.wait()


def solution(mesh):
    n_sp, n_tp = mesh.shape["sp"], mesh.shape["tp"]

    def local_attn(x_part, w_query, w_key, w_value, w_out):
        rows, d_model = x_part.shape
        heads_loc, head = w_query.shape[1], w_query.shape[2]
        two_head = heads_loc * head
        seq_loc = rows * n_tp
        cols = d_model // NY
        any_spec = pl.BlockSpec(memory_space=pl.ANY)
        dma = pltpu.SemaphoreType.DMA
        bf16, f32 = jnp.bfloat16, jnp.float32
        wo_rows = w_out.shape[0] * w_out.shape[1] // n_sp
        return pl.pallas_call(
            layer_kernel,
            out_shape=jax.ShapeDtypeStruct((rows, d_model), bf16),
            in_specs=[any_spec] * 5,
            out_specs=any_spec,
            scratch_shapes=[
                pltpu.VMEM((NY, rows, d_model), bf16),
                pltpu.VMEM((NY, d_model, 2 * two_head), bf16),
                pltpu.VMEM((seq_loc, two_head), bf16),
                pltpu.VMEM((n_sp * seq_loc, two_head), bf16),
                pltpu.VMEM((NY - 1, seq_loc // NY, two_head), bf16),
                pltpu.VMEM((NY - 1, seq_loc // NY, two_head), bf16),
                pltpu.VMEM((n_tp, n_sp, wo_rows, cols), bf16),
                pltpu.VMEM((2 * TQ, WINDOW + TQ), f32),
                pltpu.VMEM((2 * TQ, head), f32),
                pltpu.VMEM((2 * TQ, head), f32),
                pltpu.VMEM((2 * TQ, head), f32),
                pltpu.VMEM((2 * TQ, head), f32),
                pltpu.VMEM((seq_loc, two_head), bf16),
                pltpu.VMEM((NY, rows, n_tp * two_head), bf16),
                pltpu.VMEM((NY, rows, cols), bf16),
                pltpu.VMEM((rows, d_model), bf16),
                dma, dma((3,)), dma((4,)), dma((NY, 2)), dma((24,)), dma((NY, NY + 1, 2)), dma((3,)), dma((NY,)), dma((2, 3)), dma((2, NY)),
                dma((NY, 6)), dma((2 * n_sp, 2)), dma, dma((n_tp,)), dma((n_tp,)),
                dma((16,)), dma((n_sp, 2)), dma((n_tp, NY)), dma((NY, n_tp)), dma((NY,)), dma((NY,)), dma,
            ],
            compiler_params=pltpu.CompilerParams(collective_id=1, has_side_effects=True, vmem_limit_bytes=67043328),
            name="layer",
        )(x_part, w_query.reshape(d_model, two_head), w_key.reshape(d_model, head), w_value.reshape(d_model, head),
          w_out.reshape(n_sp, wo_rows, d_model))

    return jax.shard_map(local_attn, mesh=mesh, in_specs=(P(("dp", "sp", "tp"), None), P(None, "tp", None), P(None, "tp", None), P(None, "tp", None), P("tp", None, None)), out_specs=P(("dp", "sp", "tp"), None), check_vma=False)
```

```python
import functools

import jax
import jax.numpy as jnp
from jax import lax
from jax.experimental import pallas as pl
from jax.experimental.pallas import tpu as pltpu
from jax.sharding import PartitionSpec as P

WINDOW = 4096
NEG_BIG = -1e30
LOG2E = 1.4426950408889634
MESH = pl.DeviceIdType.MESH
NY = 4
TQ = 256
WIDE = 768
N_WIDE = (WINDOW - TQ) // WIDE


def dot_nt(lhs, rhs):
    return lax.dot_general(lhs, rhs, (((1,), (1,)), ((), ())), preferred_element_type=jnp.float32)


def layer_kernel(x_hbm, wq_hbm, wk_hbm, wv_hbm, wo_hbm, y_hbm, xg, w_v, q_v, kv_v, kv_st, far_st, wo_v, s_v, mx_v, mb_v, l_v, acc_v, o_st,
                 og, yst, yv, x_sem, wl_sem, x_send, x_recv, w_send, w_recv, share_send, share_recv, a_send, a_recv, far_send, far_recv,
                 pass_send, pass_recv, kv_send, kv_recv, wo_sem, wo_send, wo_recv, wy_send, wy_recv, sl_send, sl_recv, oy_send, oy_recv,
                 oz_send, oz_recv, of_send, of_recv, y_send, y_recv, y_sem):
    sp = lax.axis_index("sp")
    tp = lax.axis_index("tp")
    my_z, my_y = tp // NY, tp % NY
    my_x, my_c = sp // 2, sp % 2
    n_tp = NY * NY
    n_sp = 8
    chunk = kv_v.shape[0] // (2 * n_sp)
    head = kv_v.shape[1] // 2
    cols = yst.shape[2]
    rows = yst.shape[1]
    part = NY * rows
    coef = head ** -0.5 * LOG2E
    d_half = w_v.shape[1] // 2
    s_rows = d_half // 6
    d_rows = 2 * s_rows

    x_load = pltpu.make_async_copy(x_hbm, xg.at[my_y], x_sem)
    x_load.start()
    w_loads = (pltpu.make_async_copy(wq_hbm, w_v.at[my_z, :, 0:2 * head], wl_sem.at[0]),
               pltpu.make_async_copy(wk_hbm, w_v.at[my_z, :, 2 * head:3 * head], wl_sem.at[1]),
               pltpu.make_async_copy(wv_hbm, w_v.at[my_z, :, 3 * head:4 * head], wl_sem.at[2]))
    for load in w_loads:
        load.start()

    barrier = pltpu.get_barrier_semaphore()
    for step in range(1, n_tp):
        pl.semaphore_signal(barrier, inc=1, device_id={"tp": (tp + step) % n_tp}, device_id_type=MESH)
    for step in range(1, n_sp):
        pl.semaphore_signal(barrier, inc=1, device_id={"sp": (sp + step) % n_sp}, device_id_type=MESH)
    pl.semaphore_wait(barrier, n_tp + n_sp - 2)

    zm, zp, zo = (my_z + 3) % NY, (my_z + 1) % NY, (my_z + 2) % NY
    ym, yp, yo = (my_y + 3) % NY, (my_y + 1) % NY, (my_y + 2) % NY
    x_left, x_right, x_far = (my_x + 3) % NY, (my_x + 1) % NY, (my_x + 2) % NY
    sends = []
    n_sends = [0, 0]

    def x_copy(y_src, first, count, y_dst, slot):
        ref = xg.at[y_src, pl.ds(first * (rows // 2), count * (rows // 2))]
        return pltpu.make_async_remote_copy(src_ref=ref, dst_ref=ref, send_sem=x_send.at[slot], recv_sem=x_recv.at[y_src, first],
                                            device_id={"tp": NY * my_z + y_dst}, device_id_type=MESH)

    def x_put(y_src, first, count, y_dst):
        copy = x_copy(y_src, first, count, y_dst, n_sends[0])
        n_sends[0] += 1
        sends.append(copy)
        copy.start()

    def x_wait(y_src, first, count):
        x_copy(y_src, first, count, 0, 0).wait_recv()

    def w_copy(z_src, x_src, first, count, dst, slot):
        size = d_rows if x_src is None else s_rows
        base = my_c * d_half + (0 if x_src is None else d_rows + x_src * s_rows)
        ref = w_v.at[z_src, pl.ds(pl.multiple_of(base + first * (size // 2), 64), count * (size // 2))]
        return pltpu.make_async_remote_copy(src_ref=ref, dst_ref=ref, send_sem=w_send.at[slot],
                                            recv_sem=w_recv.at[z_src, NY if x_src is None else x_src, first], device_id=dst, device_id_type=MESH)

    def w_put(z_src, x_src, first, count, dst):
        copy = w_copy(z_src, x_src, first, count, dst, n_sends[1])
        n_sends[1] += 1
        sends.append(copy)
        copy.start()

    def w_wait(z_src, x_src, first, count):
        w_copy(z_src, x_src, first, count, {"tp": 0}, 0).wait_recv()

    def to_z(z_dst):
        return {"tp": NY * z_dst + my_y}

    def to_x(x_dst):
        return {"sp": 2 * x_dst + my_c}

    def share_copy(z_src, core, slot):
        ref = w_v.at[z_src, pl.ds(pl.multiple_of(core * d_half, 64), d_half)]
        return pltpu.make_async_remote_copy(src_ref=ref, dst_ref=ref, send_sem=share_send.at[slot], recv_sem=share_recv.at[z_src],
                                            device_id={"sp": 2 * my_x + 1 - my_c}, device_id_type=MESH)

    def blk_of(z_idx):
        return jnp.where(z_idx < NY // 2, sp, 2 * n_sp - 1 - sp)

    def kv_rows(z_idx):
        return pl.multiple_of(blk_of(z_idx) * chunk + (z_idx % 2) * part, part)

    def own_products(y_list):
        def body(idx, carry):
            y_idx = y_list[0]
            for other in range(1, len(y_list)):
                y_idx = jnp.where(idx == other, y_list[other], y_idx)
            prod = jnp.dot(xg[y_idx], w_v[my_z], preferred_element_type=jnp.float32).astype(jnp.bfloat16)
            q_v[pl.ds(pl.multiple_of(my_z * part + y_idx * rows, rows), rows), :] = prod[:, :2 * head]
            kv_v[pl.ds(pl.multiple_of(kv_rows(my_z) + y_idx * rows, rows), rows), :] = prod[:, 2 * head:]
            return carry

        lax.fori_loop(0, len(y_list), body, 0)

    def a_copy(kind, z_src, z_dst, slot):
        if kind:
            src, dst = o_st.at[pl.ds(slot * part, part)], q_v.at[pl.ds(pl.multiple_of(z_src * part, part), part)]
        else:
            src, dst = kv_st.at[slot], kv_v.at[pl.ds(kv_rows(z_src), part)]
        return pltpu.make_async_remote_copy(src_ref=src, dst_ref=dst, send_sem=a_send.at[kind, slot], recv_sem=a_recv.at[kind, z_src],
                                            device_id=to_z(z_dst), device_id_type=MESH)

    def products(z_dst, slot):
        def body(idx, carry):
            lhs = xg[pl.ds(2 * idx, 2)].reshape(2 * rows, xg.shape[2])
            prod = jnp.dot(lhs, w_v[z_dst], preferred_element_type=jnp.float32).astype(jnp.bfloat16)
            o_st[pl.ds(pl.multiple_of(slot * part + idx * 2 * rows, 2 * rows), 2 * rows), :] = prod[:, :2 * head]
            kv_st[slot, pl.ds(pl.multiple_of(idx * 2 * rows, 2 * rows), 2 * rows), :] = prod[:, 2 * head:]
            return carry

        lax.fori_loop(0, 2, body, 0)

    def a_start(z_dst, slot):
        for kind in range(2):
            a_copy(kind, my_z, z_dst, slot).start()

    def a_wait(kind, z_src):
        a_copy(kind, z_src, 0, 0).wait_recv()

    half_rows = part // 2

    def far_copy(kind, half):
        src = o_st.at[pl.ds(2 * part + half * half_rows, half_rows)] if kind else kv_st.at[2, pl.ds(half * half_rows, half_rows)]
        return pltpu.make_async_remote_copy(src_ref=src, dst_ref=far_st.at[kind, half], send_sem=far_send.at[kind, half],
                                            recv_sem=far_recv.at[kind, half], device_id=to_z(zm if half else zp), device_id_type=MESH)

    def pass_copy(kind, half, z_src):
        at = (z_src * part if kind else kv_rows(z_src)) + half * half_rows
        dst = (q_v if kind else kv_v).at[pl.ds(pl.multiple_of(at, half_rows), half_rows)]
        return pltpu.make_async_remote_copy(src_ref=far_st.at[kind, half], dst_ref=dst, send_sem=pass_send.at[kind, half],
                                            recv_sem=pass_recv.at[kind, half], device_id=to_z(zm if half else zp), device_id_type=MESH)

    def far_pass(kind):
        for half in range(2):
            far_copy(kind, half).wait_recv()
            pass_copy(kind, half, zp if half else zm).start()

    def far_wait(kind):
        for half in range(2):
            pass_copy(kind, half, zo).wait_recv()

    def kv_part(pair, core, z_idx, kind, dst):
        blk = jnp.where(pair < NY, 2 * pair + core, 2 * pair + 1 - core)
        ref = kv_v.at[pl.ds(pl.multiple_of(blk * chunk + (z_idx % 2) * part, part), part)]
        return pltpu.make_async_remote_copy(src_ref=ref, dst_ref=ref, send_sem=kv_send.at[z_idx, kind], recv_sem=kv_recv.at[blk, z_idx % 2],
                                            device_id=dst, device_id_type=MESH)

    partner = {"sp": 2 * my_x + 1 - my_c}

    def own_pair(z_idx):
        return jnp.where(z_idx < NY // 2, my_x, 2 * NY - 1 - my_x)

    def own_next(z_idx):
        low = z_idx < NY // 2
        return jnp.where(low, jnp.where(my_x < NY - 1, my_x + 1, NY - 2), my_x - 1), low | (my_x >= 1)

    def direct_in(z_idx):
        low = z_idx < NY // 2
        return jnp.where(low, my_x - 1, 2 * NY - 2 - my_x), (low & (my_x >= 1)) | (jnp.logical_not(low) & (my_x < NY - 1))

    def direct_next(z_idx):
        return jnp.where(z_idx < NY // 2, my_x + 1, my_x - 1), (my_x >= 1) & (my_x < NY - 1)

    def relay_in(z_idx):
        low = z_idx < NY // 2
        return jnp.where(low, my_x - 2, 2 * NY - 3 - my_x), (low & (my_x >= 2)) | (jnp.logical_not(low) & (my_x < NY - 2))

    def turn_in(z_idx):
        return NY - 1, (z_idx < NY // 2) & (my_x == NY - 2)

    def kv_own(z_idx, act):
        dst, wanted = own_next(z_idx)

        @pl.when(wanted)
        def _():
            act(kv_part(own_pair(z_idx), my_c, z_idx, 1, to_x(dst)))

        act(kv_part(own_pair(z_idx), my_c, z_idx, 0, partner))

    def kv_direct(z_idx, act, arrive):
        pair, wanted = direct_in(z_idx)

        @pl.when(wanted)
        def _():
            if arrive:
                kv_part(pair, my_c, z_idx, 2, partner).wait_recv()
            dst, more = direct_next(z_idx)

            @pl.when(more)
            def _():
                act(kv_part(pair, my_c, z_idx, 3, to_x(dst)))

            act(kv_part(pair, my_c, z_idx, 2, partner))

    def kv_relay(z_idx, act, arrive):
        for kind, (pair, wanted) in ((4, relay_in(z_idx)), (5, turn_in(z_idx))):
            @pl.when(wanted)
            def _(kind=kind, pair=pair):
                copy = kv_part(pair, my_c, z_idx, kind, partner)
                if arrive:
                    copy.wait_recv()
                act(copy)

    def kv_from_partner(z_idx):
        kv_part(own_pair(z_idx), 1 - my_c, z_idx, 0, partner).wait_recv()
        for pair, wanted in (direct_in(z_idx), relay_in(z_idx), turn_in(z_idx)):
            @pl.when(wanted)
            def _(pair=pair):
                kv_part(pair, 1 - my_c, z_idx, 0, partner).wait_recv()

    def start(copy):
        copy.start()

    def done(copy):
        copy.wait_send()

    def wo_copy(step):
        dst = (my_z + step) % NY
        src_ref = wo_hbm.at[sp, :, pl.ds(pl.multiple_of(dst * cols, 128), cols)]
        return pltpu.make_async_remote_copy(src_ref=src_ref, dst_ref=wo_v.at[NY * my_y + my_z, sp], send_sem=wo_send.at[step],
                                            recv_sem=wo_recv.at[my_z], device_id=to_z(dst), device_id_type=MESH)

    wo_own = pltpu.make_async_copy(wo_hbm.at[sp, :, pl.ds(pl.multiple_of(my_z * cols, 128), cols)], wo_v.at[NY * my_y + my_z, sp], wo_sem)

    def wo_z_start():
        wo_own.start()
        for step in range(1, NY):
            wo_copy(step).start()

    def wy_copy(y_src, first, count, y_dst, slot):
        ref = wo_v.at[pl.ds(NY * y_src + 2 * first, 2 * count), sp]
        return pltpu.make_async_remote_copy(src_ref=ref, dst_ref=ref, send_sem=wy_send.at[slot], recv_sem=wy_recv.at[y_src, first],
                                            device_id={"tp": NY * my_z + y_dst}, device_id_type=MESH)

    wy_sends = (wy_copy(my_y, 0, 2, yp, 0), wy_copy(my_y, 0, 2, ym, 1), wy_copy(ym, 0, 1, yp, 2), wy_copy(yp, 1, 1, ym, 3))

    def wo_y_start():
        wo_own.wait()
        for z_src in (zm, zp, zo):
            ref = wo_v.at[NY * my_y + z_src, sp]
            pltpu.make_async_remote_copy(src_ref=ref, dst_ref=ref, send_sem=wo_send.at[1], recv_sem=wo_recv.at[z_src],
                                         device_id=to_z(z_src), device_id_type=MESH).wait_recv()
        for copy in wy_sends[:2]:
            copy.start()

    def wo_y_pass():
        for y_src, copy in ((ym, wy_sends[2]), (yp, wy_sends[3])):
            wy_copy(y_src, 0, 2, 0, 0).wait_recv()
            copy.start()

    slabs = []
    other_c = 1 - my_c

    def slab_copy(x_src, c_src, first, count, x_dst, c_dst, slot):
        ref = wo_v.at[pl.ds(first * (n_tp // 2), count * (n_tp // 2)), 2 * x_src + c_src]
        return pltpu.make_async_remote_copy(src_ref=ref, dst_ref=ref, send_sem=sl_send.at[slot], recv_sem=sl_recv.at[2 * x_src + c_src, first],
                                            device_id={"sp": 2 * x_dst + c_dst}, device_id_type=MESH)

    def slab_put(x_src, first, count, x_dst, c_dst):
        slabs.append((x_src, my_c, first, count, x_dst, c_dst, len(slabs)))
        slab_copy(*slabs[-1]).start()

    def slab_wait(x_src, c_src, first, count):
        slab_copy(x_src, c_src, first, count, 0, 0, 0).wait_recv()

    def wo_first():
        for first in range(2):
            wy_copy(yo, first, 1, 0, 0).wait_recv()
        for x_dst in (x_right, x_left):
            slab_put(my_x, 0, 2, x_dst, my_c)
        slab_put(my_x, 0, 2, my_x, other_c)

    def wo_second():
        for x_src, first, x_dst in ((x_left, 0, x_right), (x_right, 1, x_left)):
            slab_wait(x_src, my_c, 0, 2)
            slab_put(x_src, first, 1, x_dst, my_c)
        for x_src in (x_left, x_right):
            slab_put(x_src, 0, 2, my_x, other_c)

    def wo_third():
        for first in range(2):
            slab_wait(x_far, my_c, first, 1)
            slab_put(x_far, first, 1, my_x, other_c)

    def wo_last():
        for x_src in (my_x, x_left, x_right):
            slab_wait(x_src, other_c, 0, 2)
        for first in range(2):
            slab_wait(x_far, other_c, first, 1)

    x_load.wait()
    x_put(my_y, 0, 2, yp)
    x_put(my_y, 0, 2, ym)
    for load in w_loads:
        load.wait()
    for z_dst in (zp, zm):
        w_put(my_z, my_x, 0, 2, to_z(z_dst))
    for z_src, first, z_dst in ((zm, 0, zp), (zp, 1, zm)):
        w_wait(z_src, my_x, 0, 2)
        w_put(z_src, my_x, first, 1, to_z(z_dst))
        for x_dst in (x_right, x_left):
            w_put(z_src, my_x, 0, 2, to_x(x_dst))
    for z_dst in (zp, zm):
        w_put(my_z, None, 0, 2, to_z(z_dst))
    wo_z_start()
    own_products([my_y])
    for z_src in (zm, zp):
        for x_src, first, x_dst in ((x_left, 0, x_right), (x_right, 1, x_left)):
            w_wait(z_src, x_src, 0, 2)
            w_put(z_src, x_src, first, 1, to_x(x_dst))
    for first in range(2):
        w_wait(zo, my_x, first, 1)
    for x_dst in (x_right, x_left):
        w_put(zo, my_x, 0, 2, to_x(x_dst))
    for y_src, first, y_dst in ((ym, 0, yp), (yp, 1, ym)):
        x_wait(y_src, 0, 2)
        x_put(y_src, first, 1, y_dst)
    for z_src, first, z_dst in ((zm, 0, zp), (zp, 1, zm)):
        w_wait(z_src, None, 0, 2)
        w_put(z_src, None, first, 1, to_z(z_dst))
    own_products([ym, yp])
    for slot, z_src in enumerate((zm, zp)):
        for first in range(2):
            w_wait(z_src, x_far, first, 1)
        share_copy(z_src, my_c, slot).start()
    for x_src, first, x_dst in ((x_left, 0, x_right), (x_right, 1, x_left)):
        w_wait(zo, x_src, 0, 2)
        w_put(zo, x_src, first, 1, to_x(x_dst))
    for first in range(2):
        x_wait(yo, first, 1)
    wo_y_start()
    own_products([yo])
    kv_own(my_z, start)
    for slot, z_dst in enumerate((zm, zp)):
        share_copy(z_dst, 1 - my_c, slot).wait_recv()
        products(z_dst, slot)
        a_start(z_dst, slot)
    for first in range(2):
        w_wait(zo, None, first, 1)
        w_wait(zo, x_far, first, 1)
    share_copy(zo, my_c, 2).start()
    share_copy(zo, 1 - my_c, 2).wait_recv()
    products(zo, 2)
    for kind in range(2):
        for half in range(2):
            far_copy(kind, half).start()
    kv_direct(my_z, start, True)
    for z_src in (zm, zp):
        a_wait(0, z_src)
        kv_own(z_src, start)
    far_pass(0)
    kv_relay(my_z, start, True)
    wo_y_pass()
    for z_src in (zm, zp):
        kv_direct(z_src, start, True)
    far_wait(0)
    kv_own(zo, start)
    far_pass(1)
    for z_src in (zm, zp):
        kv_relay(z_src, start, True)
    kv_direct(zo, start, True)
    kv_relay(zo, start, True)
    wo_first()
    for z_src in (zm, zp):
        a_wait(1, z_src)
    far_wait(1)
    for slot in range(2):
        a_copy(1, my_z, 0, slot).wait_send()
        far_copy(1, slot).wait_send()
    for z_idx in range(NY):
        kv_from_partner(z_idx)

    row_i = lax.broadcasted_iota(jnp.int32, (2 * TQ, TQ), 0) % TQ
    col_i = lax.broadcasted_iota(jnp.int32, (2 * TQ, TQ), 1)

    def lane_max(scores):
        best = scores[:, 0:head]
        for idx in range(1, scores.shape[1] // head):
            best = jnp.maximum(best, scores[:, idx * head:(idx + 1) * head])
        return best

    wide_o = NY * 2 * head

    def oy_copy(tile, src_tp):
        return pltpu.make_async_remote_copy(
            src_ref=o_st.at[pl.ds(pl.multiple_of(tile * rows, rows), rows)],
            dst_ref=og.at[tile // NY, :, pl.ds(pl.multiple_of(src_tp * 2 * head, 2 * head), 2 * head)],
            send_sem=oy_send.at[tile], recv_sem=oy_recv.at[tile // NY, src_tp % NY], device_id={"tp": NY * my_z + tile % NY}, device_id_type=MESH)

    def oz_copy(row, z_src, side):
        ref = og.at[row, :, pl.ds(pl.multiple_of(z_src * wide_o, wide_o), wide_o)]
        return pltpu.make_async_remote_copy(src_ref=ref, dst_ref=ref, send_sem=oz_send.at[row, side], recv_sem=oz_recv.at[row, z_src],
                                            device_id=to_z(zm if side else zp), device_id_type=MESH)

    def of_copy(row, z_src, side):
        ref = og.at[row, pl.ds(side * (rows // 2), rows // 2), pl.ds(pl.multiple_of(z_src * wide_o, wide_o), wide_o)]
        return pltpu.make_async_remote_copy(src_ref=ref, dst_ref=ref, send_sem=of_send.at[row, side], recv_sem=of_recv.at[row, side],
                                            device_id=to_z(zm if side else zp), device_id_type=MESH)

    def o_round(row):
        for y_src in (ym, yp, yo):
            oy_copy(NY * row + my_y, NY * my_z + y_src).wait_recv()
        for side in range(2):
            oz_copy(row, my_z, side).start()

    def o_pass(row):
        for side, z_src in ((0, zm), (1, zp)):
            oz_copy(row, z_src, side).wait_recv()
            of_copy(row, z_src, side).start()

    def o_far(row):
        for side in range(2):
            of_copy(row, zo, side).wait_recv()

    def attend(q_idx, gidx, wide, start_tile, n_steps, with_first):
        q_blk = q_v[pl.ds(pl.multiple_of(q_idx * TQ, TQ), TQ), :]
        q_two = jnp.concatenate([q_blk[:, :head], q_blk[:, head:]], axis=0)

        def keys(tile, width):
            return kv_v[pl.ds(pl.multiple_of(tile * TQ, TQ), width), 0:head]

        def values(tile, width):
            return kv_v[pl.ds(pl.multiple_of(tile * TQ, TQ), width), head:2 * head]

        per = wide // TQ
        scores = jnp.where(col_i <= row_i, dot_nt(q_two, keys(gidx, TQ)), NEG_BIG)
        s_v[:, 0:TQ] = scores
        best = lane_max(scores)
        if with_first:
            scores = jnp.where(col_i > row_i, dot_nt(q_two, keys(gidx - WINDOW // TQ, TQ)), NEG_BIG)
            s_v[:, TQ:2 * TQ] = scores
            best = jnp.maximum(best, lane_max(scores))
        mx_v[...] = best

        def score_step(idx, carry):
            part = dot_nt(q_two, keys(start_tile + per * idx, wide))
            s_v[:, pl.ds(pl.multiple_of(2 * TQ + idx * wide, TQ), wide)] = part
            mx_v[...] = jnp.maximum(mx_v[...], lane_max(part))
            return carry

        lax.fori_loop(0, n_steps, score_step, 0)
        row_best = jnp.max(mx_v[...], axis=1, keepdims=True) * coef
        mb_v[...] = jnp.broadcast_to(row_best, mb_v.shape)

        def probs(col, width):
            base = mb_v[...]
            total = None
            parts = []
            for idx in range(width // head):
                part = jnp.exp2(s_v[:, pl.ds(pl.multiple_of(col + idx * head, head), head)] * coef - base)
                total = part if total is None else total + part
                parts.append(part.astype(jnp.bfloat16))
            return jnp.concatenate(parts, axis=1), total

        prob, total = probs(0, TQ)
        acc = jnp.dot(prob, values(gidx, TQ), preferred_element_type=jnp.float32)
        if with_first:
            prob, total_b = probs(TQ, TQ)
            total = total + total_b
            acc = acc + jnp.dot(prob, values(gidx - WINDOW // TQ, TQ), preferred_element_type=jnp.float32)
        l_v[...] = total
        acc_v[...] = acc

        def value_step(idx, carry):
            prob, total = probs(2 * TQ + idx * wide, wide)
            l_v[...] += total
            acc_v[...] += jnp.dot(prob, values(start_tile + per * idx, wide), preferred_element_type=jnp.float32)
            return carry

        lax.fori_loop(0, n_steps, value_step, 0)
        denom = jnp.sum(l_v[...], axis=1, keepdims=True)
        out = (acc_v[...] / denom).astype(jnp.bfloat16)
        out = jnp.concatenate([out[:TQ], out[TQ:]], axis=1)
        o_st[pl.ds(pl.multiple_of(q_idx * TQ, TQ), TQ), :] = out

    def q_step(q_idx, carry):
        tiles = chunk // TQ
        blk = jnp.where(q_idx < tiles, sp, 2 * n_sp - 1 - sp)
        gidx = blk * tiles + q_idx % tiles

        @pl.when(gidx >= WINDOW // TQ)
        def _():
            attend(q_idx, gidx, WIDE, gidx - WINDOW // TQ + 1, N_WIDE, True)

        @pl.when(gidx < WINDOW // TQ)
        def _():
            attend(q_idx, gidx, TQ, 0, gidx, False)

        for sub in range(2):
            tile = 2 * q_idx + sub

            @pl.when(tile % NY != my_y)
            def _(tile=tile):
                oy_copy(tile, tp).start()

            @pl.when(tile % NY == my_y)
            def _(tile=tile):
                og[tile // NY, :, pl.ds(pl.multiple_of(tp * 2 * head, 2 * head), 2 * head)] = \
                    o_st[pl.ds(pl.multiple_of(tile * rows, rows), rows), :]

        @pl.when((q_idx >= 2) & (q_idx % 2 == 0))
        def _():
            o_round(q_idx // 2 - 1)

        @pl.when((q_idx >= 3) & (q_idx % 2 == 1))
        def _():
            o_pass((q_idx - 3) // 2)

        @pl.when(q_idx == 5)
        def _():
            wo_second()

        return carry

    lax.fori_loop(0, 2 * chunk // TQ, q_step, 0)

    def y_copy(z_dst, z_src):
        return pltpu.make_async_remote_copy(
            src_ref=yst.at[z_dst], dst_ref=yv.at[:, pl.ds(pl.multiple_of(z_src * cols, 128), cols)],
            send_sem=y_send.at[z_dst], recv_sem=y_recv.at[z_src], device_id={"tp": NY * z_dst + my_y}, device_id_type=MESH)

    def out_product(first, count):
        for row in range(first, first + count):
            o_far(row)
        lhs = og[first:first + count].reshape(count * rows, n_tp * 2 * head)
        for col in range(0, cols, 384):
            w_cols = jnp.concatenate([wo_v[NY * y_idx + z_idx, :, :, col:col + 384].reshape(2 * head, 384)
                                      for z_idx in range(NY) for y_idx in range(NY)], axis=0)
            res = jnp.dot(lhs, w_cols, preferred_element_type=jnp.float32).astype(jnp.bfloat16)
            yst[first:first + count, :, col:col + 384] = res.reshape(count, rows, 384)
        for z_dst in range(first, first + count):
            @pl.when(my_z != z_dst)
            def _(z_dst=z_dst):
                y_copy(z_dst, my_z).start()

            @pl.when(my_z == z_dst)
            def _(z_dst=z_dst):
                yv[:, pl.ds(pl.multiple_of(my_z * cols, 128), cols)] = yst[z_dst]

    o_round(NY - 1)
    wo_third()
    o_pass(NY - 1)
    wo_last()
    out_product(0, 2)
    out_product(2, 1)
    out_product(3, 1)
    for z_src in range(NY):
        @pl.when(my_z != z_src)
        def _(z_src=z_src):
            y_copy(z_src, z_src).wait_recv()
    y_out = pltpu.make_async_copy(yv, y_hbm, y_sem)
    y_out.start()
    for tile in range(n_tp):
        @pl.when(tile % NY != my_y)
        def _(tile=tile):
            oy_copy(tile, tp).wait_send()
    for row in range(NY):
        for side, z_src in ((0, zm), (1, zp)):
            oz_copy(row, my_z, side).wait_send()
            of_copy(row, z_src, side).wait_send()
    for z_dst in range(NY):
        @pl.when(my_z != z_dst)
        def _(z_dst=z_dst):
            y_copy(z_dst, my_z).wait_send()
    for copy in sends + [slab_copy(*slab) for slab in slabs]:
        copy.wait_send()
    for step in range(1, NY):
        wo_copy(step).wait_send()
    for copy in wy_sends:
        copy.wait_send()
    for slot in range(3):
        share_copy(my_z, my_c, slot).wait_send()
    for slot in range(2):
        a_copy(0, my_z, 0, slot).wait_send()
        far_copy(0, slot).wait_send()
        for kind in range(2):
            pass_copy(kind, slot, my_z).wait_send()
    for z_idx in range(NY):
        kv_own(z_idx, done)
        kv_direct(z_idx, done, False)
        kv_relay(z_idx, done, False)
    y_out.wait()


def solution(mesh):
    n_sp, n_tp = mesh.shape["sp"], mesh.shape["tp"]

    def local_attn(x_part, w_query, w_key, w_value, w_out):
        rows, d_model = x_part.shape
        heads_loc, head = w_query.shape[1], w_query.shape[2]
        two_head = heads_loc * head
        seq_loc = rows * n_tp
        cols = d_model // NY
        any_spec = pl.BlockSpec(memory_space=pl.ANY)
        dma = pltpu.SemaphoreType.DMA
        bf16, f32 = jnp.bfloat16, jnp.float32
        wo_rows = w_out.shape[0] * w_out.shape[1] // n_sp
        return pl.pallas_call(
            layer_kernel,
            out_shape=jax.ShapeDtypeStruct((rows, d_model), bf16),
            in_specs=[any_spec] * 5,
            out_specs=any_spec,
            scratch_shapes=[
                pltpu.VMEM((NY, rows, d_model), bf16),
                pltpu.VMEM((NY, d_model, 2 * two_head), bf16),
                pltpu.VMEM((seq_loc, two_head), bf16),
                pltpu.VMEM((n_sp * seq_loc, two_head), bf16),
                pltpu.VMEM((NY - 1, seq_loc // NY, two_head), bf16),
                pltpu.VMEM((2, 2, seq_loc // (2 * NY), two_head), bf16),
                pltpu.VMEM((n_tp, n_sp, wo_rows, cols), bf16),
                pltpu.VMEM((2 * TQ, WINDOW + TQ), f32),
                pltpu.VMEM((2 * TQ, head), f32),
                pltpu.VMEM((2 * TQ, head), f32),
                pltpu.VMEM((2 * TQ, head), f32),
                pltpu.VMEM((2 * TQ, head), f32),
                pltpu.VMEM((seq_loc, two_head), bf16),
                pltpu.VMEM((NY, rows, n_tp * two_head), bf16),
                pltpu.VMEM((NY, rows, cols), bf16),
                pltpu.VMEM((rows, d_model), bf16),
                dma, dma((3,)), dma((4,)), dma((NY, 2)), dma((24,)), dma((NY, NY + 1, 2)), dma((3,)), dma((NY,)), dma((2, 2)), dma((2, NY)),
                dma((2, 2)), dma((2, 2)), dma((2, 2)), dma((2, 2)), dma((NY, 6)), dma((2 * n_sp, 2)), dma, dma((NY,)), dma((NY,)), dma((4,)),
                dma((NY, 2)), dma((16,)), dma((n_sp, 2)), dma((n_tp,)), dma((NY, NY)), dma((NY, 2)), dma((NY, NY)), dma((NY, 2)), dma((NY, 2)),
                dma((NY,)), dma((NY,)), dma,
            ],
            compiler_params=pltpu.CompilerParams(collective_id=1, has_side_effects=True, vmem_limit_bytes=67043328),
            name="layer",
        )(x_part, w_query.reshape(d_model, two_head), w_key.reshape(d_model, head), w_value.reshape(d_model, head),
          w_out.reshape(n_sp, wo_rows, d_model))

    return jax.shard_map(local_attn, mesh=mesh, in_specs=(P(("dp", "sp", "tp"), None), P(None, "tp", None), P(None, "tp", None), P(None, "tp", None), P("tp", None, None)), out_specs=P(("dp", "sp", "tp"), None), check_vma=False)
```

```python
import functools

import jax
import jax.numpy as jnp
from jax import lax
from jax.experimental import pallas as pl
from jax.experimental.pallas import tpu as pltpu
from jax.sharding import PartitionSpec as P

WINDOW = 4096
NEG_BIG = -1e30
LOG2E = 1.4426950408889634
MESH = pl.DeviceIdType.MESH
NY = 4
TQ = 256
WIDE = 768
N_WIDE = (WINDOW - TQ) // WIDE


def dot_nt(lhs, rhs):
    return lax.dot_general(lhs, rhs, (((1,), (1,)), ((), ())), preferred_element_type=jnp.float32)


def layer_kernel(x_hbm, wq_hbm, wk_hbm, wv_hbm, wo_hbm, y_hbm, xg, w_v, q_v, kv_v, kv_st, far_st, wo_v, s_v, mx_v, mb_v, l_v, acc_v, o_st,
                 og, yst, yv, x_sem, wl_sem, x_send, x_recv, w_send, w_recv, share_send, share_recv, a_send, a_recv, far_send, far_recv,
                 pass_send, pass_recv, kv_send, kv_recv, wo_sem, wo_send, wo_recv, wy_send, wy_recv, sl_send, sl_recv, oy_send, oy_recv,
                 oz_send, oz_recv, of_send, of_recv, y_send, y_recv, y_sem):
    sp = lax.axis_index("sp")
    tp = lax.axis_index("tp")
    my_z, my_y = tp // NY, tp % NY
    my_x, my_c = sp // 2, sp % 2
    n_tp = NY * NY
    n_sp = 8
    chunk = kv_v.shape[0] // (2 * n_sp)
    head = kv_v.shape[1] // 2
    cols = yst.shape[2]
    rows = yst.shape[1]
    part = NY * rows
    coef = head ** -0.5 * LOG2E
    d_half = w_v.shape[1] // 2
    s_rows = d_half // (6 * 32) * 32 - 32
    d_rows = d_half - NY * s_rows

    x_load = pltpu.make_async_copy(x_hbm, xg.at[my_y], x_sem)
    x_load.start()
    w_loads = (pltpu.make_async_copy(wq_hbm, w_v.at[my_z, :, 0:2 * head], wl_sem.at[0]),
               pltpu.make_async_copy(wk_hbm, w_v.at[my_z, :, 2 * head:3 * head], wl_sem.at[1]),
               pltpu.make_async_copy(wv_hbm, w_v.at[my_z, :, 3 * head:4 * head], wl_sem.at[2]))
    for load in w_loads:
        load.start()

    barrier = pltpu.get_barrier_semaphore()
    for step in range(1, n_tp):
        pl.semaphore_signal(barrier, inc=1, device_id={"tp": (tp + step) % n_tp}, device_id_type=MESH)
    for step in range(1, n_sp):
        pl.semaphore_signal(barrier, inc=1, device_id={"sp": (sp + step) % n_sp}, device_id_type=MESH)
    pl.semaphore_wait(barrier, n_tp + n_sp - 2)

    zm, zp, zo = (my_z + 3) % NY, (my_z + 1) % NY, (my_z + 2) % NY
    ym, yp, yo = (my_y + 3) % NY, (my_y + 1) % NY, (my_y + 2) % NY
    x_left, x_right, x_far = (my_x + 3) % NY, (my_x + 1) % NY, (my_x + 2) % NY
    partner = {"sp": 2 * my_x + 1 - my_c}
    sends = []
    n_sends = [0, 0]

    def x_copy(y_src, first, count, y_dst, slot):
        ref = xg.at[y_src, pl.ds(first * (rows // 2), count * (rows // 2))]
        return pltpu.make_async_remote_copy(src_ref=ref, dst_ref=ref, send_sem=x_send.at[slot], recv_sem=x_recv.at[y_src, first],
                                            device_id={"tp": NY * my_z + y_dst}, device_id_type=MESH)

    def x_put(y_src, first, count, y_dst):
        copy = x_copy(y_src, first, count, y_dst, n_sends[0])
        n_sends[0] += 1
        sends.append(copy)
        copy.start()

    def x_wait(y_src, first, count):
        x_copy(y_src, first, count, 0, 0).wait_recv()

    def w_copy(z_src, x_src, first, count, dst, slot):
        size = d_rows if x_src is None else s_rows
        base = my_c * d_half + (0 if x_src is None else d_rows + x_src * s_rows)
        ref = w_v.at[z_src, pl.ds(pl.multiple_of(base + first * (size // 2), 16), count * (size // 2))]
        return pltpu.make_async_remote_copy(src_ref=ref, dst_ref=ref, send_sem=w_send.at[slot],
                                            recv_sem=w_recv.at[z_src, NY if x_src is None else x_src, first], device_id=dst, device_id_type=MESH)

    def w_put(z_src, x_src, first, count, dst):
        copy = w_copy(z_src, x_src, first, count, dst, n_sends[1])
        n_sends[1] += 1
        sends.append(copy)
        copy.start()

    def w_wait(z_src, x_src, first, count):
        w_copy(z_src, x_src, first, count, {"tp": 0}, 0).wait_recv()

    def to_z(z_dst):
        return {"tp": NY * z_dst + my_y}

    def to_x(x_dst):
        return {"sp": 2 * x_dst + my_c}

    def share_copy(z_src, core, slot):
        ref = w_v.at[z_src, pl.ds(pl.multiple_of(core * d_half, 64), d_half)]
        return pltpu.make_async_remote_copy(src_ref=ref, dst_ref=ref, send_sem=share_send.at[slot], recv_sem=share_recv.at[z_src],
                                            device_id=partner, device_id_type=MESH)

    def blk_of(z_idx):
        return jnp.where(z_idx < NY // 2, sp, 2 * n_sp - 1 - sp)

    def kv_rows(z_idx):
        return pl.multiple_of(blk_of(z_idx) * chunk + (z_idx % 2) * part, part)

    def own_products(y_list):
        def body(idx, carry):
            y_idx = y_list[0]
            for other in range(1, len(y_list)):
                y_idx = jnp.where(idx == other, y_list[other], y_idx)
            prod = jnp.dot(xg[y_idx], w_v[my_z], preferred_element_type=jnp.float32).astype(jnp.bfloat16)
            q_v[pl.ds(pl.multiple_of(my_z * part + y_idx * rows, rows), rows), :] = prod[:, :2 * head]
            kv_v[pl.ds(pl.multiple_of(kv_rows(my_z) + y_idx * rows, rows), rows), :] = prod[:, 2 * head:]
            return carry

        lax.fori_loop(0, len(y_list), body, 0)

    def a_copy(kind, z_src, z_dst, slot):
        if kind:
            src, dst = o_st.at[pl.ds(slot * part, part)], q_v.at[pl.ds(pl.multiple_of(z_src * part, part), part)]
        else:
            src, dst = kv_st.at[slot], kv_v.at[pl.ds(kv_rows(z_src), part)]
        return pltpu.make_async_remote_copy(src_ref=src, dst_ref=dst, send_sem=a_send.at[kind, slot], recv_sem=a_recv.at[kind, z_src],
                                            device_id=to_z(z_dst), device_id_type=MESH)

    def products(z_dst, slot):
        def body(idx, carry):
            lhs = xg[pl.ds(2 * idx, 2)].reshape(2 * rows, xg.shape[2])
            prod = jnp.dot(lhs, w_v[z_dst], preferred_element_type=jnp.float32).astype(jnp.bfloat16)
            o_st[pl.ds(pl.multiple_of(slot * part + idx * 2 * rows, 2 * rows), 2 * rows), :] = prod[:, :2 * head]
            kv_st[slot, pl.ds(pl.multiple_of(idx * 2 * rows, 2 * rows), 2 * rows), :] = prod[:, 2 * head:]
            return carry

        lax.fori_loop(0, 2, body, 0)

    def a_start(kind, z_dst, slot):
        a_copy(kind, my_z, z_dst, slot).start()

    def a_wait(kind, z_src):
        a_copy(kind, z_src, 0, 0).wait_recv()

    half_rows = part // 2

    def far_copy(kind, half):
        src = o_st.at[pl.ds(2 * part + half * half_rows, half_rows)] if kind else kv_st.at[2, pl.ds(half * half_rows, half_rows)]
        return pltpu.make_async_remote_copy(src_ref=src, dst_ref=far_st.at[kind, half], send_sem=far_send.at[kind, half],
                                            recv_sem=far_recv.at[kind, half], device_id=to_z(zm if half else zp), device_id_type=MESH)

    def pass_copy(kind, half, z_src):
        at = (z_src * part if kind else kv_rows(z_src)) + half * half_rows
        dst = (q_v if kind else kv_v).at[pl.ds(pl.multiple_of(at, half_rows), half_rows)]
        return pltpu.make_async_remote_copy(src_ref=far_st.at[kind, half], dst_ref=dst, send_sem=pass_send.at[kind, half],
                                            recv_sem=pass_recv.at[kind, half], device_id=to_z(zm if half else zp), device_id_type=MESH)

    def far_pass(kind):
        for half in range(2):
            far_copy(kind, half).wait_recv()
            pass_copy(kind, half, zp if half else zm).start()

    def far_wait(kind):
        for half in range(2):
            pass_copy(kind, half, zo).wait_recv()

    def kv_part(pair, core, z_idx, kind, dst):
        blk = jnp.where(pair < NY, 2 * pair + core, 2 * pair + 1 - core)
        ref = kv_v.at[pl.ds(pl.multiple_of(blk * chunk + (z_idx % 2) * part, part), part)]
        return pltpu.make_async_remote_copy(src_ref=ref, dst_ref=ref, send_sem=kv_send.at[z_idx, kind], recv_sem=kv_recv.at[blk, z_idx % 2],
                                            device_id=dst, device_id_type=MESH)

    def own_pair(z_idx):
        return jnp.where(z_idx < NY // 2, my_x, 2 * NY - 1 - my_x)

    def own_next(z_idx):
        low = z_idx < NY // 2
        return jnp.where(low, jnp.where(my_x < NY - 1, my_x + 1, NY - 2), my_x - 1), low | (my_x >= 1)

    def direct_in(z_idx):
        low = z_idx < NY // 2
        return jnp.where(low, my_x - 1, 2 * NY - 2 - my_x), (low & (my_x >= 1)) | (jnp.logical_not(low) & (my_x < NY - 1))

    def direct_next(z_idx):
        return jnp.where(z_idx < NY // 2, my_x + 1, my_x - 1), (my_x >= 1) & (my_x < NY - 1)

    def relay_in(z_idx):
        low = z_idx < NY // 2
        return jnp.where(low, my_x - 2, 2 * NY - 3 - my_x), (low & (my_x >= 2)) | (jnp.logical_not(low) & (my_x < NY - 2))

    def turn_in(z_idx):
        return NY - 1, (z_idx < NY // 2) & (my_x == NY - 2)

    def kv_own(z_idx, act):
        dst, wanted = own_next(z_idx)

        @pl.when(wanted)
        def _():
            act(kv_part(own_pair(z_idx), my_c, z_idx, 1, to_x(dst)))

        act(kv_part(own_pair(z_idx), my_c, z_idx, 0, partner))

    def kv_direct(z_idx, act, arrive):
        pair, wanted = direct_in(z_idx)

        @pl.when(wanted)
        def _():
            if arrive:
                kv_part(pair, my_c, z_idx, 2, partner).wait_recv()
            dst, more = direct_next(z_idx)

            @pl.when(more)
            def _():
                act(kv_part(pair, my_c, z_idx, 3, to_x(dst)))

            act(kv_part(pair, my_c, z_idx, 2, partner))

    def kv_relay(z_idx, act, arrive):
        for kind, (pair, wanted) in ((4, relay_in(z_idx)), (5, turn_in(z_idx))):
            @pl.when(wanted)
            def _(kind=kind, pair=pair):
                copy = kv_part(pair, my_c, z_idx, kind, partner)
                if arrive:
                    copy.wait_recv()
                act(copy)

    def kv_from_partner(z_idx):
        kv_part(own_pair(z_idx), 1 - my_c, z_idx, 0, partner).wait_recv()
        for pair, wanted in (direct_in(z_idx), relay_in(z_idx), turn_in(z_idx)):
            @pl.when(wanted)
            def _(pair=pair):
                kv_part(pair, 1 - my_c, z_idx, 0, partner).wait_recv()

    def start(copy):
        copy.start()

    def done(copy):
        copy.wait_send()

    group = 2 * (my_x % 2) + my_c
    x_group = 2 - 2 * (my_x % 2) + my_c

    def wo_copy(step):
        dst = (my_z + step) % NY
        src_ref = wo_hbm.at[group, :, pl.ds(pl.multiple_of(dst * cols, 128), cols)]
        return pltpu.make_async_remote_copy(src_ref=src_ref, dst_ref=wo_v.at[NY * my_y + my_z, group], send_sem=wo_send.at[step],
                                            recv_sem=wo_recv.at[my_z], device_id=to_z(dst), device_id_type=MESH)

    wo_own = pltpu.make_async_copy(wo_hbm.at[group, :, pl.ds(pl.multiple_of(my_z * cols, 128), cols)], wo_v.at[NY * my_y + my_z, group], wo_sem)

    def wo_z_start():
        wo_own.start()
        for step in range(1, NY):
            wo_copy(step).start()

    def wy_copy(y_src, first, count, y_dst, slot):
        ref = wo_v.at[pl.ds(NY * y_src + 2 * first, 2 * count), group]
        return pltpu.make_async_remote_copy(src_ref=ref, dst_ref=ref, send_sem=wy_send.at[slot], recv_sem=wy_recv.at[y_src, first],
                                            device_id={"tp": NY * my_z + y_dst}, device_id_type=MESH)

    wy_sends = (wy_copy(my_y, 0, 2, yp, 0), wy_copy(my_y, 0, 2, ym, 1), wy_copy(ym, 0, 1, yp, 2), wy_copy(yp, 1, 1, ym, 3))

    def wo_y_start():
        wo_own.wait()
        for z_src in (zm, zp, zo):
            ref = wo_v.at[NY * my_y + z_src, group]
            pltpu.make_async_remote_copy(src_ref=ref, dst_ref=ref, send_sem=wo_send.at[1], recv_sem=wo_recv.at[z_src],
                                         device_id=to_z(z_src), device_id_type=MESH).wait_recv()
        for copy in wy_sends[:2]:
            copy.start()

    def wo_y_pass():
        for y_src, copy in ((ym, wy_sends[2]), (yp, wy_sends[3])):
            wy_copy(y_src, 0, 2, 0, 0).wait_recv()
            copy.start()

    def slab_copy(grp, first, count, dst, slot):
        ref = wo_v.at[pl.ds(first * (n_tp // 2), count * (n_tp // 2)), grp]
        return pltpu.make_async_remote_copy(src_ref=ref, dst_ref=ref, send_sem=sl_send.at[slot], recv_sem=sl_recv.at[grp, first],
                                            device_id=dst, device_id_type=MESH)

    slabs = (slab_copy(group, 0, 1, to_x(x_right), 0), slab_copy(group, 1, 1, to_x(x_left), 1), slab_copy(group, 0, 2, partner, 2),
             slab_copy(x_group, 0, 2, partner, 3))

    def wo_first():
        for first in range(2):
            wy_copy(yo, first, 1, 0, 0).wait_recv()
        for copy in slabs[:3]:
            copy.start()

    def wo_second():
        for first in range(2):
            slab_copy(x_group, first, 1, partner, 3).wait_recv()
        slabs[3].start()

    def wo_last():
        for grp in (2 * (my_x % 2), 2 - 2 * (my_x % 2)):
            slab_copy(grp + 1 - my_c, 0, 2, partner, 3).wait_recv()

    x_load.wait()
    x_put(my_y, 0, 2, yp)
    x_put(my_y, 0, 2, ym)
    for load in w_loads:
        load.wait()
    for z_dst in (zp, zm):
        w_put(my_z, my_x, 0, 2, to_z(z_dst))
    for z_src, first, z_dst in ((zm, 0, zp), (zp, 1, zm)):
        w_wait(z_src, my_x, 0, 2)
        w_put(z_src, my_x, first, 1, to_z(z_dst))
        for x_dst in (x_right, x_left):
            w_put(z_src, my_x, 0, 2, to_x(x_dst))
    for z_dst in (zp, zm):
        w_put(my_z, None, 0, 2, to_z(z_dst))
    wo_z_start()
    own_products([my_y])
    for z_src in (zm, zp):
        for x_src, first, x_dst in ((x_left, 0, x_right), (x_right, 1, x_left)):
            w_wait(z_src, x_src, 0, 2)
            w_put(z_src, x_src, first, 1, to_x(x_dst))
    for first in range(2):
        w_wait(zo, my_x, first, 1)
    for x_dst in (x_right, x_left):
        w_put(zo, my_x, 0, 2, to_x(x_dst))
    for y_src, first, y_dst in ((ym, 0, yp), (yp, 1, ym)):
        x_wait(y_src, 0, 2)
        x_put(y_src, first, 1, y_dst)
    for z_src, first, z_dst in ((zm, 0, zp), (zp, 1, zm)):
        w_wait(z_src, None, 0, 2)
        w_put(z_src, None, first, 1, to_z(z_dst))
    own_products([ym, yp])
    for slot, z_src in enumerate((zm, zp)):
        for first in range(2):
            w_wait(z_src, x_far, first, 1)
        share_copy(z_src, my_c, slot).start()
    for x_src, first, x_dst in ((x_left, 0, x_right), (x_right, 1, x_left)):
        w_wait(zo, x_src, 0, 2)
        w_put(zo, x_src, first, 1, to_x(x_dst))
    for first in range(2):
        x_wait(yo, first, 1)
    wo_y_start()
    own_products([yo])
    kv_own(my_z, start)
    for slot, z_dst in enumerate((zm, zp)):
        share_copy(z_dst, 1 - my_c, slot).wait_recv()
        products(z_dst, slot)
        a_start(0, z_dst, slot)
    for first in range(2):
        w_wait(zo, None, first, 1)
        w_wait(zo, x_far, first, 1)
    share_copy(zo, my_c, 2).start()
    share_copy(zo, 1 - my_c, 2).wait_recv()
    products(zo, 2)
    for half in range(2):
        far_copy(0, half).start()
    for slot, z_dst in enumerate((zm, zp)):
        a_start(1, z_dst, slot)
    kv_direct(my_z, start, True)
    for z_src in (zm, zp):
        a_wait(0, z_src)
        kv_own(z_src, start)
    far_pass(0)
    for half in range(2):
        far_copy(1, half).start()
    kv_relay(my_z, start, True)
    wo_y_pass()
    for z_src in (zm, zp):
        kv_direct(z_src, start, True)
    far_wait(0)
    kv_own(zo, start)
    far_pass(1)
    for z_src in (zm, zp):
        kv_relay(z_src, start, True)
    kv_direct(zo, start, True)
    kv_relay(zo, start, True)
    wo_first()
    for z_src in (zm, zp):
        a_wait(1, z_src)
    far_wait(1)
    for slot in range(2):
        a_copy(1, my_z, 0, slot).wait_send()
        far_copy(1, slot).wait_send()
    for z_idx in range(NY):
        kv_from_partner(z_idx)

    row_i = lax.broadcasted_iota(jnp.int32, (2 * TQ, TQ), 0) % TQ
    col_i = lax.broadcasted_iota(jnp.int32, (2 * TQ, TQ), 1)

    def lane_max(scores):
        best = scores[:, 0:head]
        for idx in range(1, scores.shape[1] // head):
            best = jnp.maximum(best, scores[:, idx * head:(idx + 1) * head])
        return best

    wide_o = NY * 2 * head

    def oy_copy(tile, src_tp):
        return pltpu.make_async_remote_copy(
            src_ref=o_st.at[pl.ds(pl.multiple_of(tile * rows, rows), rows)],
            dst_ref=og.at[tile // NY, :, pl.ds(pl.multiple_of(src_tp * 2 * head, 2 * head), 2 * head)],
            send_sem=oy_send.at[tile], recv_sem=oy_recv.at[tile // NY, src_tp % NY], device_id={"tp": NY * my_z + tile % NY}, device_id_type=MESH)

    def oz_copy(row, z_src, side):
        ref = og.at[row, :, pl.ds(pl.multiple_of(z_src * wide_o, wide_o), wide_o)]
        return pltpu.make_async_remote_copy(src_ref=ref, dst_ref=ref, send_sem=oz_send.at[row, side], recv_sem=oz_recv.at[row, z_src],
                                            device_id=to_z(zm if side else zp), device_id_type=MESH)

    def of_copy(row, z_src, side):
        ref = og.at[row, pl.ds(side * (rows // 2), rows // 2), pl.ds(pl.multiple_of(z_src * wide_o, wide_o), wide_o)]
        return pltpu.make_async_remote_copy(src_ref=ref, dst_ref=ref, send_sem=of_send.at[row, side], recv_sem=of_recv.at[row, side],
                                            device_id=to_z(zm if side else zp), device_id_type=MESH)

    def o_round(row):
        for y_src in (ym, yp, yo):
            oy_copy(NY * row + my_y, NY * my_z + y_src).wait_recv()
        for side in range(2):
            oz_copy(row, my_z, side).start()

    def o_pass(row):
        for side, z_src in ((0, zm), (1, zp)):
            oz_copy(row, z_src, side).wait_recv()
            of_copy(row, z_src, side).start()

    def o_far(row):
        for side in range(2):
            of_copy(row, zo, side).wait_recv()

    def attend(q_idx, gidx, wide, start_tile, n_steps, with_first):
        q_blk = q_v[pl.ds(pl.multiple_of(q_idx * TQ, TQ), TQ), :]
        q_two = jnp.concatenate([q_blk[:, :head], q_blk[:, head:]], axis=0)

        def keys(tile, width):
            return kv_v[pl.ds(pl.multiple_of(tile * TQ, TQ), width), 0:head]

        def values(tile, width):
            return kv_v[pl.ds(pl.multiple_of(tile * TQ, TQ), width), head:2 * head]

        per = wide // TQ
        scores = jnp.where(col_i <= row_i, dot_nt(q_two, keys(gidx, TQ)) * coef, NEG_BIG)
        s_v[:, 0:TQ] = scores
        best = lane_max(scores)
        if with_first:
            scores = jnp.where(col_i > row_i, dot_nt(q_two, keys(gidx - WINDOW // TQ, TQ)) * coef, NEG_BIG)
            s_v[:, TQ:2 * TQ] = scores
            best = jnp.maximum(best, lane_max(scores))
        mx_v[...] = best

        def score_step(idx, carry):
            part = dot_nt(q_two, keys(start_tile + per * idx, wide)) * coef
            s_v[:, pl.ds(pl.multiple_of(2 * TQ + idx * wide, TQ), wide)] = part
            mx_v[...] = jnp.maximum(mx_v[...], lane_max(part))
            return carry

        lax.fori_loop(0, n_steps, score_step, 0)
        row_best = jnp.max(mx_v[...], axis=1, keepdims=True)
        mb_v[...] = jnp.broadcast_to(row_best, mb_v.shape)

        def probs(col, width):
            base = mb_v[...]
            total = None
            parts = []
            for idx in range(width // head):
                part = jnp.exp2(s_v[:, pl.ds(pl.multiple_of(col + idx * head, head), head)] - base)
                total = part if total is None else total + part
                parts.append(part.astype(jnp.bfloat16))
            return jnp.concatenate(parts, axis=1), total

        prob, total = probs(0, TQ)
        acc = jnp.dot(prob, values(gidx, TQ), preferred_element_type=jnp.float32)
        if with_first:
            prob, total_b = probs(TQ, TQ)
            total = total + total_b
            acc = acc + jnp.dot(prob, values(gidx - WINDOW // TQ, TQ), preferred_element_type=jnp.float32)
        l_v[...] = total
        acc_v[...] = acc

        def value_step(idx, carry):
            prob, total = probs(2 * TQ + idx * wide, wide)
            l_v[...] += total
            acc_v[...] += jnp.dot(prob, values(start_tile + per * idx, wide), preferred_element_type=jnp.float32)
            return carry

        lax.fori_loop(0, n_steps, value_step, 0)
        denom = jnp.sum(l_v[...], axis=1, keepdims=True)
        out = (acc_v[...] / denom).astype(jnp.bfloat16)
        out = jnp.concatenate([out[:TQ], out[TQ:]], axis=1)
        o_st[pl.ds(pl.multiple_of(q_idx * TQ, TQ), TQ), :] = out

    def q_step(q_idx, carry):
        tiles = chunk // TQ
        blk = jnp.where(q_idx < tiles, sp, 2 * n_sp - 1 - sp)
        gidx = blk * tiles + q_idx % tiles

        @pl.when(gidx >= WINDOW // TQ)
        def _():
            attend(q_idx, gidx, WIDE, gidx - WINDOW // TQ + 1, N_WIDE, True)

        @pl.when(gidx < WINDOW // TQ)
        def _():
            attend(q_idx, gidx, TQ, 0, gidx, False)

        for sub in range(2):
            tile = 2 * q_idx + sub

            @pl.when(tile % NY != my_y)
            def _(tile=tile):
                oy_copy(tile, tp).start()

            @pl.when(tile % NY == my_y)
            def _(tile=tile):
                og[tile // NY, :, pl.ds(pl.multiple_of(tp * 2 * head, 2 * head), 2 * head)] = \
                    o_st[pl.ds(pl.multiple_of(tile * rows, rows), rows), :]

        @pl.when((q_idx >= 2) & (q_idx % 2 == 0))
        def _():
            o_round(q_idx // 2 - 1)

        @pl.when((q_idx >= 3) & (q_idx % 2 == 1))
        def _():
            o_pass((q_idx - 3) // 2)

        @pl.when(q_idx == 4)
        def _():
            wo_second()

        return carry

    lax.fori_loop(0, 2 * chunk // TQ, q_step, 0)

    def y_copy(z_dst, z_src):
        return pltpu.make_async_remote_copy(
            src_ref=yst.at[z_dst], dst_ref=yv.at[:, pl.ds(pl.multiple_of(z_src * cols, 128), cols)],
            send_sem=y_send.at[z_dst], recv_sem=y_recv.at[z_src], device_id={"tp": NY * z_dst + my_y}, device_id_type=MESH)

    def out_product(first, count):
        for row in range(first, first + count):
            o_far(row)
        lhs = og[first:first + count].reshape(count * rows, n_tp * 2 * head)
        for col in range(0, cols, 384):
            w_cols = jnp.concatenate([wo_v[NY * y_idx + z_idx, :, :, col:col + 384].reshape(2 * head, 384)
                                      for z_idx in range(NY) for y_idx in range(NY)], axis=0)
            res = jnp.dot(lhs, w_cols, preferred_element_type=jnp.float32).astype(jnp.bfloat16)
            yst[first:first + count, :, col:col + 384] = res.reshape(count, rows, 384)
        for z_dst in range(first, first + count):
            @pl.when(my_z != z_dst)
            def _(z_dst=z_dst):
                y_copy(z_dst, my_z).start()

            @pl.when(my_z == z_dst)
            def _(z_dst=z_dst):
                yv[:, pl.ds(pl.multiple_of(my_z * cols, 128), cols)] = yst[z_dst]

    o_round(NY - 1)
    wo_last()
    out_product(0, 2)
    o_pass(NY - 1)
    out_product(2, 1)
    out_product(3, 1)
    for z_src in range(NY):
        @pl.when(my_z != z_src)
        def _(z_src=z_src):
            y_copy(z_src, z_src).wait_recv()
    y_out = pltpu.make_async_copy(yv, y_hbm, y_sem)
    y_out.start()
    for tile in range(n_tp):
        @pl.when(tile % NY != my_y)
        def _(tile=tile):
            oy_copy(tile, tp).wait_send()
    for row in range(NY):
        for side, z_src in ((0, zm), (1, zp)):
            oz_copy(row, my_z, side).wait_send()
            of_copy(row, z_src, side).wait_send()
    for z_dst in range(NY):
        @pl.when(my_z != z_dst)
        def _(z_dst=z_dst):
            y_copy(z_dst, my_z).wait_send()
    for copy in sends + list(slabs):
        copy.wait_send()
    for step in range(1, NY):
        wo_copy(step).wait_send()
    for copy in wy_sends:
        copy.wait_send()
    for slot in range(3):
        share_copy(my_z, my_c, slot).wait_send()
    for slot in range(2):
        a_copy(0, my_z, 0, slot).wait_send()
        far_copy(0, slot).wait_send()
        for kind in range(2):
            pass_copy(kind, slot, my_z).wait_send()
    for z_idx in range(NY):
        kv_own(z_idx, done)
        kv_direct(z_idx, done, False)
        kv_relay(z_idx, done, False)
    y_out.wait()


def solution(mesh):
    n_sp, n_tp = mesh.shape["sp"], mesh.shape["tp"]

    def local_attn(x_part, w_query, w_key, w_value, w_out):
        rows, d_model = x_part.shape
        heads_loc, head = w_query.shape[1], w_query.shape[2]
        two_head = heads_loc * head
        seq_loc = rows * n_tp
        cols = d_model // NY
        any_spec = pl.BlockSpec(memory_space=pl.ANY)
        dma = pltpu.SemaphoreType.DMA
        bf16, f32 = jnp.bfloat16, jnp.float32
        wo_rows = w_out.shape[0] * w_out.shape[1] // NY
        return pl.pallas_call(
            layer_kernel,
            out_shape=jax.ShapeDtypeStruct((rows, d_model), bf16),
            in_specs=[any_spec] * 5,
            out_specs=any_spec,
            scratch_shapes=[
                pltpu.VMEM((NY, rows, d_model), bf16),
                pltpu.VMEM((NY, d_model, 2 * two_head), bf16),
                pltpu.VMEM((seq_loc, two_head), bf16),
                pltpu.VMEM((n_sp * seq_loc, two_head), bf16),
                pltpu.VMEM((NY - 1, seq_loc // NY, two_head), bf16),
                pltpu.VMEM((2, 2, seq_loc // (2 * NY), two_head), bf16),
                pltpu.VMEM((n_tp, NY, wo_rows, cols), bf16),
                pltpu.VMEM((2 * TQ, WINDOW + TQ), f32),
                pltpu.VMEM((2 * TQ, head), f32),
                pltpu.VMEM((2 * TQ, head), f32),
                pltpu.VMEM((2 * TQ, head), f32),
                pltpu.VMEM((2 * TQ, head), f32),
                pltpu.VMEM((seq_loc, two_head), bf16),
                pltpu.VMEM((NY, rows, n_tp * two_head), bf16),
                pltpu.VMEM((NY, rows, cols), bf16),
                pltpu.VMEM((rows, d_model), bf16),
                dma, dma((3,)), dma((4,)), dma((NY, 2)), dma((24,)), dma((NY, NY + 1, 2)), dma((3,)), dma((NY,)), dma((2, 2)), dma((2, NY)),
                dma((2, 2)), dma((2, 2)), dma((2, 2)), dma((2, 2)), dma((NY, 6)), dma((2 * n_sp, 2)), dma, dma((NY,)), dma((NY,)), dma((4,)),
                dma((NY, 2)), dma((16,)), dma((n_sp, 2)), dma((n_tp,)), dma((NY, NY)), dma((NY, 2)), dma((NY, NY)), dma((NY, 2)), dma((NY, 2)),
                dma((NY,)), dma((NY,)), dma,
            ],
            compiler_params=pltpu.CompilerParams(collective_id=1, has_side_effects=True, vmem_limit_bytes=67043328),
            name="layer",
        )(x_part, w_query.reshape(d_model, two_head), w_key.reshape(d_model, head), w_value.reshape(d_model, head),
          w_out.reshape(NY, wo_rows, d_model))

    return jax.shard_map(local_attn, mesh=mesh, in_specs=(P(("dp", "sp", "tp"), None), P(None, "tp", None), P(None, "tp", None), P(None, "tp", None), P("tp", None, None)), out_specs=P(("dp", "sp", "tp"), None), check_vma=False)
```

```python
import functools

import jax
import jax.numpy as jnp
from jax import lax
from jax.experimental import pallas as pl
from jax.experimental.pallas import tpu as pltpu
from jax.sharding import PartitionSpec as P

WINDOW = 4096
NEG_BIG = -1e30
LOG2E = 1.4426950408889634
MESH = pl.DeviceIdType.MESH
NY = 4
TQ = 256
WIDE = 768
N_WIDE = (WINDOW - TQ) // WIDE


def dot_nt(lhs, rhs):
    return lax.dot_general(lhs, rhs, (((1,), (1,)), ((), ())), preferred_element_type=jnp.float32)


def layer_kernel(x_hbm, wq_hbm, wk_hbm, wv_hbm, wo_hbm, y_hbm, xg, wq_v, wkv_v, q_v, kv_v, kv_st, far_st, wo_v, s_v, mx_v, mb_v, l_v, acc_v, o_st,
                 og, yst, yv, x_sem, wl_sem, x_send, x_recv, w_send, w_recv, share_send, share_recv, a_send, a_recv, far_send, far_recv,
                 pass_send, pass_recv, kv_send, kv_recv, wo_sem, wo_send, wo_recv, wy_send, wy_recv, sl_send, sl_recv, oy_send, oy_recv,
                 oz_send, oz_recv, of_send, of_recv, y_send, y_recv, y_sem):
    sp = lax.axis_index("sp")
    tp = lax.axis_index("tp")
    my_z, my_y = tp // NY, tp % NY
    my_x, my_c = sp // 2, sp % 2
    n_tp = NY * NY
    n_sp = 8
    chunk = kv_v.shape[0] // (2 * n_sp)
    head = kv_v.shape[1] // 2
    cols = yst.shape[2]
    rows = yst.shape[1]
    part = NY * rows
    coef = head ** -0.5 * LOG2E
    d_half = wq_v.shape[1] // 2
    s_rows = d_half // (6 * 32) * 32 - 32
    d_rows = d_half - NY * s_rows

    x_load = pltpu.make_async_copy(x_hbm, xg.at[my_y], x_sem)
    x_load.start()
    w_loads = (pltpu.make_async_copy(wk_hbm, wkv_v.at[my_z, :, 0:head], wl_sem.at[0]),
               pltpu.make_async_copy(wv_hbm, wkv_v.at[my_z, :, head:2 * head], wl_sem.at[1]),
               pltpu.make_async_copy(wq_hbm, wq_v.at[my_z], wl_sem.at[2]))
    for load in w_loads:
        load.start()

    barrier = pltpu.get_barrier_semaphore()
    for step in range(1, n_tp):
        pl.semaphore_signal(barrier, inc=1, device_id={"tp": (tp + step) % n_tp}, device_id_type=MESH)
    for step in range(1, n_sp):
        pl.semaphore_signal(barrier, inc=1, device_id={"sp": (sp + step) % n_sp}, device_id_type=MESH)
    pl.semaphore_wait(barrier, n_tp + n_sp - 2)

    zm, zp, zo = (my_z + 3) % NY, (my_z + 1) % NY, (my_z + 2) % NY
    ym, yp, yo = (my_y + 3) % NY, (my_y + 1) % NY, (my_y + 2) % NY
    x_left, x_right, x_far = (my_x + 3) % NY, (my_x + 1) % NY, (my_x + 2) % NY
    partner = {"sp": 2 * my_x + 1 - my_c}
    sends = []
    n_sends = [0, 0]

    def x_copy(y_src, first, count, y_dst, slot):
        ref = xg.at[y_src, pl.ds(first * (rows // 2), count * (rows // 2))]
        return pltpu.make_async_remote_copy(src_ref=ref, dst_ref=ref, send_sem=x_send.at[slot], recv_sem=x_recv.at[y_src, first],
                                            device_id={"tp": NY * my_z + y_dst}, device_id_type=MESH)

    def x_put(y_src, first, count, y_dst):
        copy = x_copy(y_src, first, count, y_dst, n_sends[0])
        n_sends[0] += 1
        sends.append(copy)
        copy.start()

    def x_wait(y_src, first, count):
        x_copy(y_src, first, count, 0, 0).wait_recv()

    def w_copy(kind, z_src, x_src, first, count, dst, slot):
        size = d_rows if x_src is None else s_rows
        base = my_c * d_half + (0 if x_src is None else d_rows + x_src * s_rows)
        ref = (wq_v if kind else wkv_v).at[z_src, pl.ds(pl.multiple_of(base + first * (size // 2), 16), count * (size // 2))]
        return pltpu.make_async_remote_copy(src_ref=ref, dst_ref=ref, send_sem=w_send.at[slot],
                                            recv_sem=w_recv.at[kind, z_src, NY if x_src is None else x_src, first], device_id=dst, device_id_type=MESH)

    def w_put(kind, z_src, x_src, first, count, dst):
        copy = w_copy(kind, z_src, x_src, first, count, dst, n_sends[1])
        n_sends[1] += 1
        sends.append(copy)
        copy.start()

    def w_wait(kind, z_src, x_src, first, count):
        w_copy(kind, z_src, x_src, first, count, {"tp": 0}, 0).wait_recv()

    def to_z(z_dst):
        return {"tp": NY * z_dst + my_y}

    def to_x(x_dst):
        return {"sp": 2 * x_dst + my_c}

    def share_copy(kind, z_src, core, slot):
        ref = (wq_v if kind else wkv_v).at[z_src, pl.ds(pl.multiple_of(core * d_half, 64), d_half)]
        return pltpu.make_async_remote_copy(src_ref=ref, dst_ref=ref, send_sem=share_send.at[kind, slot], recv_sem=share_recv.at[kind, z_src],
                                            device_id=partner, device_id_type=MESH)

    def blk_of(z_idx):
        return jnp.where(z_idx < NY // 2, sp, 2 * n_sp - 1 - sp)

    def kv_rows(z_idx):
        return pl.multiple_of(blk_of(z_idx) * chunk + (z_idx % 2) * part, part)

    def own_products(y_list):
        def body(idx, carry):
            y_idx = y_list[0]
            for other in range(1, len(y_list)):
                y_idx = jnp.where(idx == other, y_list[other], y_idx)
            prod = jnp.dot(xg[y_idx], wkv_v[my_z], preferred_element_type=jnp.float32).astype(jnp.bfloat16)
            kv_v[pl.ds(pl.multiple_of(kv_rows(my_z) + y_idx * rows, rows), rows), :] = prod
            prod = jnp.dot(xg[y_idx], wq_v[my_z], preferred_element_type=jnp.float32).astype(jnp.bfloat16)
            q_v[pl.ds(pl.multiple_of(my_z * part + y_idx * rows, rows), rows), :] = prod
            return carry

        lax.fori_loop(0, len(y_list), body, 0)

    def a_copy(kind, z_src, z_dst, slot):
        if kind:
            src, dst = o_st.at[pl.ds(slot * part, part)], q_v.at[pl.ds(pl.multiple_of(z_src * part, part), part)]
        else:
            src, dst = kv_st.at[slot], kv_v.at[pl.ds(kv_rows(z_src), part)]
        return pltpu.make_async_remote_copy(src_ref=src, dst_ref=dst, send_sem=a_send.at[kind, slot], recv_sem=a_recv.at[kind, z_src],
                                            device_id=to_z(z_dst), device_id_type=MESH)

    def products(kind, z_dst, slot):
        def body(idx, carry):
            lhs = xg[pl.ds(2 * idx, 2)].reshape(2 * rows, xg.shape[2])
            prod = jnp.dot(lhs, (wq_v if kind else wkv_v)[z_dst], preferred_element_type=jnp.float32).astype(jnp.bfloat16)
            if kind:
                o_st[pl.ds(pl.multiple_of(slot * part + idx * 2 * rows, 2 * rows), 2 * rows), :] = prod
            else:
                kv_st[slot, pl.ds(pl.multiple_of(idx * 2 * rows, 2 * rows), 2 * rows), :] = prod
            return carry

        lax.fori_loop(0, 2, body, 0)

    def a_start(kind, z_dst, slot):
        a_copy(kind, my_z, z_dst, slot).start()

    def a_wait(kind, z_src):
        a_copy(kind, z_src, 0, 0).wait_recv()

    half_rows = part // 2

    def far_copy(kind, half):
        src = o_st.at[pl.ds(2 * part + half * half_rows, half_rows)] if kind else kv_st.at[2, pl.ds(half * half_rows, half_rows)]
        return pltpu.make_async_remote_copy(src_ref=src, dst_ref=far_st.at[kind, half], send_sem=far_send.at[kind, half],
                                            recv_sem=far_recv.at[kind, half], device_id=to_z(zm if half else zp), device_id_type=MESH)

    def pass_copy(kind, half, z_src):
        at = (z_src * part if kind else kv_rows(z_src)) + half * half_rows
        dst = (q_v if kind else kv_v).at[pl.ds(pl.multiple_of(at, half_rows), half_rows)]
        return pltpu.make_async_remote_copy(src_ref=far_st.at[kind, half], dst_ref=dst, send_sem=pass_send.at[kind, half],
                                            recv_sem=pass_recv.at[kind, half], device_id=to_z(zm if half else zp), device_id_type=MESH)

    def far_pass(kind):
        for half in range(2):
            far_copy(kind, half).wait_recv()
            pass_copy(kind, half, zp if half else zm).start()

    def far_wait(kind):
        for half in range(2):
            pass_copy(kind, half, zo).wait_recv()

    def kv_part(pair, core, z_idx, kind, dst):
        blk = jnp.where(pair < NY, 2 * pair + core, 2 * pair + 1 - core)
        ref = kv_v.at[pl.ds(pl.multiple_of(blk * chunk + (z_idx % 2) * part, part), part)]
        return pltpu.make_async_remote_copy(src_ref=ref, dst_ref=ref, send_sem=kv_send.at[z_idx, kind], recv_sem=kv_recv.at[blk, z_idx % 2],
                                            device_id=dst, device_id_type=MESH)

    def own_pair(z_idx):
        return jnp.where(z_idx < NY // 2, my_x, 2 * NY - 1 - my_x)

    def own_next(z_idx):
        low = z_idx < NY // 2
        return jnp.where(low, jnp.where(my_x < NY - 1, my_x + 1, NY - 2), my_x - 1), low | (my_x >= 1)

    def direct_in(z_idx):
        low = z_idx < NY // 2
        return jnp.where(low, my_x - 1, 2 * NY - 2 - my_x), (low & (my_x >= 1)) | (jnp.logical_not(low) & (my_x < NY - 1))

    def direct_next(z_idx):
        return jnp.where(z_idx < NY // 2, my_x + 1, my_x - 1), (my_x >= 1) & (my_x < NY - 1)

    def relay_in(z_idx):
        low = z_idx < NY // 2
        return jnp.where(low, my_x - 2, 2 * NY - 3 - my_x), (low & (my_x >= 2)) | (jnp.logical_not(low) & (my_x < NY - 2))

    def turn_in(z_idx):
        return NY - 1, (z_idx < NY // 2) & (my_x == NY - 2)

    def kv_own(z_idx, act):
        dst, wanted = own_next(z_idx)

        @pl.when(wanted)
        def _():
            act(kv_part(own_pair(z_idx), my_c, z_idx, 1, to_x(dst)))

        act(kv_part(own_pair(z_idx), my_c, z_idx, 0, partner))

    def kv_direct(z_idx, act, arrive):
        pair, wanted = direct_in(z_idx)

        @pl.when(wanted)
        def _():
            if arrive:
                kv_part(pair, my_c, z_idx, 2, partner).wait_recv()
            dst, more = direct_next(z_idx)

            @pl.when(more)
            def _():
                act(kv_part(pair, my_c, z_idx, 3, to_x(dst)))

            act(kv_part(pair, my_c, z_idx, 2, partner))

    def kv_relay(z_idx, act, arrive):
        for kind, (pair, wanted) in ((4, relay_in(z_idx)), (5, turn_in(z_idx))):
            @pl.when(wanted)
            def _(kind=kind, pair=pair):
                copy = kv_part(pair, my_c, z_idx, kind, partner)
                if arrive:
                    copy.wait_recv()
                act(copy)

    def kv_from_partner(z_idx):
        kv_part(own_pair(z_idx), 1 - my_c, z_idx, 0, partner).wait_recv()
        for pair, wanted in (direct_in(z_idx), relay_in(z_idx), turn_in(z_idx)):
            @pl.when(wanted)
            def _(pair=pair):
                kv_part(pair, 1 - my_c, z_idx, 0, partner).wait_recv()

    def start(copy):
        copy.start()

    def done(copy):
        copy.wait_send()

    group = 2 * (my_x % 2) + my_c
    x_group = 2 - 2 * (my_x % 2) + my_c

    def wo_copy(step):
        dst = (my_z + step) % NY
        src_ref = wo_hbm.at[group, :, pl.ds(pl.multiple_of(dst * cols, 128), cols)]
        return pltpu.make_async_remote_copy(src_ref=src_ref, dst_ref=wo_v.at[NY * my_y + my_z, group], send_sem=wo_send.at[step],
                                            recv_sem=wo_recv.at[my_z], device_id=to_z(dst), device_id_type=MESH)

    wo_own = pltpu.make_async_copy(wo_hbm.at[group, :, pl.ds(pl.multiple_of(my_z * cols, 128), cols)], wo_v.at[NY * my_y + my_z, group], wo_sem)

    def wo_z_start():
        wo_own.start()
        for step in range(1, NY):
            wo_copy(step).start()

    def wy_copy(y_src, first, count, y_dst, slot):
        ref = wo_v.at[pl.ds(NY * y_src + 2 * first, 2 * count), group]
        return pltpu.make_async_remote_copy(src_ref=ref, dst_ref=ref, send_sem=wy_send.at[slot], recv_sem=wy_recv.at[y_src, first],
                                            device_id={"tp": NY * my_z + y_dst}, device_id_type=MESH)

    wy_sends = (wy_copy(my_y, 0, 2, yp, 0), wy_copy(my_y, 0, 2, ym, 1), wy_copy(ym, 0, 1, yp, 2), wy_copy(yp, 1, 1, ym, 3))

    def wo_y_start():
        wo_own.wait()
        for z_src in (zm, zp, zo):
            ref = wo_v.at[NY * my_y + z_src, group]
            pltpu.make_async_remote_copy(src_ref=ref, dst_ref=ref, send_sem=wo_send.at[1], recv_sem=wo_recv.at[z_src],
                                         device_id=to_z(z_src), device_id_type=MESH).wait_recv()
        for copy in wy_sends[:2]:
            copy.start()

    def wo_y_pass():
        for y_src, copy in ((ym, wy_sends[2]), (yp, wy_sends[3])):
            wy_copy(y_src, 0, 2, 0, 0).wait_recv()
            copy.start()

    def slab_copy(grp, first, count, dst, slot):
        ref = wo_v.at[pl.ds(first * (n_tp // 2), count * (n_tp // 2)), grp]
        return pltpu.make_async_remote_copy(src_ref=ref, dst_ref=ref, send_sem=sl_send.at[slot], recv_sem=sl_recv.at[grp, first],
                                            device_id=dst, device_id_type=MESH)

    slabs = (slab_copy(group, 0, 1, to_x(x_right), 0), slab_copy(group, 1, 1, to_x(x_left), 1), slab_copy(group, 0, 2, partner, 2),
             slab_copy(x_group, 0, 2, partner, 3))

    def wo_first():
        for first in range(2):
            wy_copy(yo, first, 1, 0, 0).wait_recv()
        for copy in slabs[:3]:
            copy.start()

    def wo_second():
        for first in range(2):
            slab_copy(x_group, first, 1, partner, 3).wait_recv()
        slabs[3].start()

    def wo_last():
        for grp in (2 * (my_x % 2), 2 - 2 * (my_x % 2)):
            slab_copy(grp + 1 - my_c, 0, 2, partner, 3).wait_recv()

    def w_own_slice(kind):
        for z_dst in (zp, zm):
            w_put(kind, my_z, my_x, 0, 2, to_z(z_dst))

    def w_slices(kind):
        for z_src, first, z_dst in ((zm, 0, zp), (zp, 1, zm)):
            w_wait(kind, z_src, my_x, 0, 2)
            w_put(kind, z_src, my_x, first, 1, to_z(z_dst))
            for x_dst in (x_right, x_left):
                w_put(kind, z_src, my_x, 0, 2, to_x(x_dst))

    def w_own_rest(kind):
        for z_dst in (zp, zm):
            w_put(kind, my_z, None, 0, 2, to_z(z_dst))

    def w_far_slice(kind):
        for first in range(2):
            w_wait(kind, zo, my_x, first, 1)
        for x_dst in (x_right, x_left):
            w_put(kind, zo, my_x, 0, 2, to_x(x_dst))

    def w_ring(kind, z_src):
        for x_src, first, x_dst in ((x_left, 0, x_right), (x_right, 1, x_left)):
            w_wait(kind, z_src, x_src, 0, 2)
            w_put(kind, z_src, x_src, first, 1, to_x(x_dst))

    def w_rest(kind):
        for z_src, first, z_dst in ((zm, 0, zp), (zp, 1, zm)):
            w_wait(kind, z_src, None, 0, 2)
            w_put(kind, z_src, None, first, 1, to_z(z_dst))

    def w_share(kind, z_src, slot):
        for first in range(2):
            w_wait(kind, z_src, x_far, first, 1)
            if slot == 2:
                w_wait(kind, z_src, None, first, 1)
        share_copy(kind, z_src, my_c, slot).start()

    def w_full(kind, z_src, slot):
        share_copy(kind, z_src, 1 - my_c, slot).wait_recv()

    x_load.wait()
    x_put(my_y, 0, 2, yp)
    x_put(my_y, 0, 2, ym)
    for load in w_loads[:2]:
        load.wait()
    w_own_slice(0)
    w_slices(0)
    w_own_rest(0)
    w_loads[2].wait()
    w_own_slice(1)
    w_far_slice(0)
    own_products([my_y])
    w_ring(0, zm)
    w_ring(0, zp)
    w_rest(0)
    w_ring(0, zo)
    w_slices(1)
    w_own_rest(1)
    w_share(0, zm, 0)
    w_share(0, zp, 1)
    for y_src, first, y_dst in ((ym, 0, yp), (yp, 1, ym)):
        x_wait(y_src, 0, 2)
        x_put(y_src, first, 1, y_dst)
    w_share(0, zo, 2)
    w_far_slice(1)
    own_products([ym, yp])
    w_ring(1, zm)
    w_ring(1, zp)
    w_rest(1)
    wo_z_start()
    w_ring(1, zo)
    for first in range(2):
        x_wait(yo, first, 1)
    own_products([yo])
    kv_own(my_z, start)
    for slot, z_dst in enumerate((zm, zp)):
        w_full(0, z_dst, slot)
        products(0, z_dst, slot)
        a_start(0, z_dst, slot)
    w_full(0, zo, 2)
    products(0, zo, 2)
    for half in range(2):
        far_copy(0, half).start()
    w_share(1, zm, 0)
    w_share(1, zp, 1)
    w_share(1, zo, 2)
    wo_y_start()
    kv_direct(my_z, start, True)
    for z_src in (zm, zp):
        a_wait(0, z_src)
        kv_own(z_src, start)
    w_full(1, zm, 0)
    products(1, zm, 0)
    far_pass(0)
    a_start(1, zm, 0)
    kv_relay(my_z, start, True)
    w_full(1, zp, 1)
    products(1, zp, 1)
    a_start(1, zp, 1)
    for z_src in (zm, zp):
        kv_direct(z_src, start, True)
    w_full(1, zo, 2)
    products(1, zo, 2)
    for half in range(2):
        far_copy(1, half).start()
    far_wait(0)
    kv_own(zo, start)
    wo_y_pass()
    for z_src in (zm, zp):
        kv_relay(z_src, start, True)
    far_pass(1)
    kv_direct(zo, start, True)
    kv_relay(zo, start, True)
    wo_first()
    for z_src in (zm, zp):
        a_wait(1, z_src)
    far_wait(1)
    for slot in range(2):
        a_copy(1, my_z, 0, slot).wait_send()
        far_copy(1, slot).wait_send()
    for z_idx in range(NY):
        kv_from_partner(z_idx)

    row_i = lax.broadcasted_iota(jnp.int32, (2 * TQ, TQ), 0) % TQ
    col_i = lax.broadcasted_iota(jnp.int32, (2 * TQ, TQ), 1)

    def lane_max(scores):
        best = scores[:, 0:head]
        for idx in range(1, scores.shape[1] // head):
            best = jnp.maximum(best, scores[:, idx * head:(idx + 1) * head])
        return best

    wide_o = NY * 2 * head

    def oy_copy(tile, src_tp):
        return pltpu.make_async_remote_copy(
            src_ref=o_st.at[pl.ds(pl.multiple_of(tile * rows, rows), rows)],
            dst_ref=og.at[tile // NY, :, pl.ds(pl.multiple_of(src_tp * 2 * head, 2 * head), 2 * head)],
            send_sem=oy_send.at[tile], recv_sem=oy_recv.at[tile // NY, src_tp % NY], device_id={"tp": NY * my_z + tile % NY}, device_id_type=MESH)

    def oz_copy(row, z_src, side):
        ref = og.at[row, :, pl.ds(pl.multiple_of(z_src * wide_o, wide_o), wide_o)]
        return pltpu.make_async_remote_copy(src_ref=ref, dst_ref=ref, send_sem=oz_send.at[row, side], recv_sem=oz_recv.at[row, z_src],
                                            device_id=to_z(zm if side else zp), device_id_type=MESH)

    def of_copy(row, z_src, side):
        ref = og.at[row, pl.ds(side * (rows // 2), rows // 2), pl.ds(pl.multiple_of(z_src * wide_o, wide_o), wide_o)]
        return pltpu.make_async_remote_copy(src_ref=ref, dst_ref=ref, send_sem=of_send.at[row, side], recv_sem=of_recv.at[row, side],
                                            device_id=to_z(zm if side else zp), device_id_type=MESH)

    def o_round(row):
        for y_src in (ym, yp, yo):
            oy_copy(NY * row + my_y, NY * my_z + y_src).wait_recv()
        for side in range(2):
            oz_copy(row, my_z, side).start()

    def o_pass(row):
        for side, z_src in ((0, zm), (1, zp)):
            oz_copy(row, z_src, side).wait_recv()
            of_copy(row, z_src, side).start()

    def o_far(row):
        for side in range(2):
            of_copy(row, zo, side).wait_recv()

    def attend(q_idx, gidx, wide, start_tile, n_steps, with_first):
        q_blk = q_v[pl.ds(pl.multiple_of(q_idx * TQ, TQ), TQ), :]
        q_two = jnp.concatenate([q_blk[:, :head], q_blk[:, head:]], axis=0)

        def keys(tile, width):
            return kv_v[pl.ds(pl.multiple_of(tile * TQ, TQ), width), 0:head]

        def values(tile, width):
            return kv_v[pl.ds(pl.multiple_of(tile * TQ, TQ), width), head:2 * head]

        per = wide // TQ
        scores = jnp.where(col_i <= row_i, dot_nt(q_two, keys(gidx, TQ)) * coef, NEG_BIG)
        s_v[:, 0:TQ] = scores
        best = lane_max(scores)
        if with_first:
            scores = jnp.where(col_i > row_i, dot_nt(q_two, keys(gidx - WINDOW // TQ, TQ)) * coef, NEG_BIG)
            s_v[:, TQ:2 * TQ] = scores
            best = jnp.maximum(best, lane_max(scores))
        mx_v[...] = best

        def score_step(idx, carry):
            part = dot_nt(q_two, keys(start_tile + per * idx, wide)) * coef
            s_v[:, pl.ds(pl.multiple_of(2 * TQ + idx * wide, TQ), wide)] = part
            mx_v[...] = jnp.maximum(mx_v[...], lane_max(part))
            return carry

        lax.fori_loop(0, n_steps, score_step, 0)
        row_best = jnp.max(mx_v[...], axis=1, keepdims=True)
        mb_v[...] = jnp.broadcast_to(row_best, mb_v.shape)

        def probs(col, width):
            base = mb_v[...]
            total = None
            parts = []
            for idx in range(width // head):
                part = jnp.exp2(s_v[:, pl.ds(pl.multiple_of(col + idx * head, head), head)] - base)
                total = part if total is None else total + part
                parts.append(part.astype(jnp.bfloat16))
            return jnp.concatenate(parts, axis=1), total

        prob, total = probs(0, TQ)
        acc = jnp.dot(prob, values(gidx, TQ), preferred_element_type=jnp.float32)
        if with_first:
            prob, total_b = probs(TQ, TQ)
            total = total + total_b
            acc = acc + jnp.dot(prob, values(gidx - WINDOW // TQ, TQ), preferred_element_type=jnp.float32)
        l_v[...] = total
        acc_v[...] = acc

        def value_step(idx, carry):
            prob, total = probs(2 * TQ + idx * wide, wide)
            l_v[...] += total
            acc_v[...] += jnp.dot(prob, values(start_tile + per * idx, wide), preferred_element_type=jnp.float32)
            return carry

        lax.fori_loop(0, n_steps, value_step, 0)
        denom = jnp.sum(l_v[...], axis=1, keepdims=True)
        out = (acc_v[...] / denom).astype(jnp.bfloat16)
        out = jnp.concatenate([out[:TQ], out[TQ:]], axis=1)
        o_st[pl.ds(pl.multiple_of(q_idx * TQ, TQ), TQ), :] = out

    def y_copy(z_dst, z_src):
        return pltpu.make_async_remote_copy(
            src_ref=yst.at[z_dst], dst_ref=yv.at[:, pl.ds(pl.multiple_of(z_src * cols, 128), cols)],
            send_sem=y_send.at[z_dst], recv_sem=y_recv.at[z_src], device_id={"tp": NY * z_dst + my_y}, device_id_type=MESH)

    def out_product(first, count):
        for row in range(first, first + count):
            o_far(row)
        lhs = og[first:first + count].reshape(count * rows, n_tp * 2 * head)
        for col in range(0, cols, 384):
            w_cols = jnp.concatenate([wo_v[NY * y_idx + z_idx, :, :, col:col + 384].reshape(2 * head, 384)
                                      for z_idx in range(NY) for y_idx in range(NY)], axis=0)
            res = jnp.dot(lhs, w_cols, preferred_element_type=jnp.float32).astype(jnp.bfloat16)
            yst[first:first + count, :, col:col + 384] = res.reshape(count, rows, 384)

    def y_put(first, count):
        for z_dst in range(first, first + count):
            @pl.when(my_z != z_dst)
            def _(z_dst=z_dst):
                y_copy(z_dst, my_z).start()

            @pl.when(my_z == z_dst)
            def _(z_dst=z_dst):
                yv[:, pl.ds(pl.multiple_of(my_z * cols, 128), cols)] = yst[z_dst]

    def q_step(q_idx, carry):
        tiles = chunk // TQ
        blk = jnp.where(q_idx < tiles, sp, 2 * n_sp - 1 - sp)
        gidx = blk * tiles + q_idx % tiles

        @pl.when(gidx >= WINDOW // TQ)
        def _():
            attend(q_idx, gidx, WIDE, gidx - WINDOW // TQ + 1, N_WIDE, True)

        @pl.when(gidx < WINDOW // TQ)
        def _():
            attend(q_idx, gidx, TQ, 0, gidx, False)

        for sub in range(2):
            tile = 2 * q_idx + sub

            @pl.when(tile % NY != my_y)
            def _(tile=tile):
                oy_copy(tile, tp).start()

            @pl.when(tile % NY == my_y)
            def _(tile=tile):
                og[tile // NY, :, pl.ds(pl.multiple_of(tp * 2 * head, 2 * head), 2 * head)] = \
                    o_st[pl.ds(pl.multiple_of(tile * rows, rows), rows), :]

        @pl.when((q_idx >= 2) & (q_idx % 2 == 0))
        def _():
            o_round(q_idx // 2 - 1)

        @pl.when((q_idx >= 3) & (q_idx % 2 == 1))
        def _():
            o_pass((q_idx - 3) // 2)

        @pl.when(q_idx == 4)
        def _():
            wo_second()

        @pl.when(q_idx == 6)
        def _():
            wo_last()
            out_product(0, 2)
            y_put(0, 2)

        return carry

    lax.fori_loop(0, 2 * chunk // TQ, q_step, 0)

    o_round(NY - 1)
    out_product(2, 1)
    o_pass(NY - 1)
    y_put(2, 1)
    out_product(3, 1)
    y_put(3, 1)
    for z_src in range(NY):
        @pl.when(my_z != z_src)
        def _(z_src=z_src):
            y_copy(z_src, z_src).wait_recv()
    y_out = pltpu.make_async_copy(yv, y_hbm, y_sem)
    y_out.start()
    for tile in range(n_tp):
        @pl.when(tile % NY != my_y)
        def _(tile=tile):
            oy_copy(tile, tp).wait_send()
    for row in range(NY):
        for side, z_src in ((0, zm), (1, zp)):
            oz_copy(row, my_z, side).wait_send()
            of_copy(row, z_src, side).wait_send()
    for z_dst in range(NY):
        @pl.when(my_z != z_dst)
        def _(z_dst=z_dst):
            y_copy(z_dst, my_z).wait_send()
    for copy in sends + list(slabs):
        copy.wait_send()
    for step in range(1, NY):
        wo_copy(step).wait_send()
    for copy in wy_sends:
        copy.wait_send()
    for slot in range(3):
        for kind in range(2):
            share_copy(kind, my_z, my_c, slot).wait_send()
    for slot in range(2):
        a_copy(0, my_z, 0, slot).wait_send()
        far_copy(0, slot).wait_send()
        for kind in range(2):
            pass_copy(kind, slot, my_z).wait_send()
    for z_idx in range(NY):
        kv_own(z_idx, done)
        kv_direct(z_idx, done, False)
        kv_relay(z_idx, done, False)
    y_out.wait()


def solution(mesh):
    n_sp, n_tp = mesh.shape["sp"], mesh.shape["tp"]

    def local_attn(x_part, w_query, w_key, w_value, w_out):
        rows, d_model = x_part.shape
        heads_loc, head = w_query.shape[1], w_query.shape[2]
        two_head = heads_loc * head
        seq_loc = rows * n_tp
        cols = d_model // NY
        any_spec = pl.BlockSpec(memory_space=pl.ANY)
        dma = pltpu.SemaphoreType.DMA
        bf16, f32 = jnp.bfloat16, jnp.float32
        wo_rows = w_out.shape[0] * w_out.shape[1] // NY
        return pl.pallas_call(
            layer_kernel,
            out_shape=jax.ShapeDtypeStruct((rows, d_model), bf16),
            in_specs=[any_spec] * 5,
            out_specs=any_spec,
            scratch_shapes=[
                pltpu.VMEM((NY, rows, d_model), bf16),
                pltpu.VMEM((NY, d_model, two_head), bf16),
                pltpu.VMEM((NY, d_model, two_head), bf16),
                pltpu.VMEM((seq_loc, two_head), bf16),
                pltpu.VMEM((n_sp * seq_loc, two_head), bf16),
                pltpu.VMEM((NY - 1, seq_loc // NY, two_head), bf16),
                pltpu.VMEM((2, 2, seq_loc // (2 * NY), two_head), bf16),
                pltpu.VMEM((n_tp, NY, wo_rows, cols), bf16),
                pltpu.VMEM((2 * TQ, WINDOW + TQ), f32),
                pltpu.VMEM((2 * TQ, head), f32),
                pltpu.VMEM((2 * TQ, head), f32),
                pltpu.VMEM((2 * TQ, head), f32),
                pltpu.VMEM((2 * TQ, head), f32),
                pltpu.VMEM((seq_loc, two_head), bf16),
                pltpu.VMEM((NY, rows, n_tp * two_head), bf16),
                pltpu.VMEM((NY, rows, cols), bf16),
                pltpu.VMEM((rows, d_model), bf16),
                dma, dma((3,)), dma((4,)), dma((NY, 2)), dma((40,)), dma((2, NY, NY + 1, 2)), dma((2, 3)), dma((2, NY)), dma((2, 2)), dma((2, NY)),
                dma((2, 2)), dma((2, 2)), dma((2, 2)), dma((2, 2)), dma((NY, 6)), dma((2 * n_sp, 2)), dma, dma((NY,)), dma((NY,)), dma((4,)),
                dma((NY, 2)), dma((16,)), dma((n_sp, 2)), dma((n_tp,)), dma((NY, NY)), dma((NY, 2)), dma((NY, NY)), dma((NY, 2)), dma((NY, 2)),
                dma((NY,)), dma((NY,)), dma,
            ],
            compiler_params=pltpu.CompilerParams(collective_id=1, has_side_effects=True, vmem_limit_bytes=67043328),
            name="layer",
        )(x_part, w_query.reshape(d_model, two_head), w_key.reshape(d_model, head), w_value.reshape(d_model, head),
          w_out.reshape(NY, wo_rows, d_model))

    return jax.shard_map(local_attn, mesh=mesh, in_specs=(P(("dp", "sp", "tp"), None), P(None, "tp", None), P(None, "tp", None), P(None, "tp", None), P("tp", None, None)), out_specs=P(("dp", "sp", "tp"), None), check_vma=False)
```

```python
import functools

import jax
import jax.numpy as jnp
from jax import lax
from jax.experimental import pallas as pl
from jax.experimental.pallas import tpu as pltpu
from jax.sharding import PartitionSpec as P

WINDOW = 4096
NEG_BIG = -1e30
LOG2E = 1.4426950408889634
MESH = pl.DeviceIdType.MESH
NY = 4
TQ = 256
WIDE = 768
N_WIDE = (WINDOW - TQ) // WIDE


def dot_nt(lhs, rhs):
    return lax.dot_general(lhs, rhs, (((1,), (1,)), ((), ())), preferred_element_type=jnp.float32)


def layer_kernel(x_hbm, wq_hbm, wk_hbm, wv_hbm, wo_hbm, y_hbm, xg, wq_v, wkv_v, q_v, kv_v, kv_st, wo_v, s_v, mx_v, mb_v, l_v, acc_v, o_st,
                 og, yst, yv, x_sem, wl_sem, x_send, x_recv, w_send, w_recv, share_send, share_recv, a_send, a_recv,
                 kv_send, kv_recv, wo_sem, wo_send, wo_recv, wy_send, wy_recv, sl_send, sl_recv, o_send, o_recv,
                 y_send, y_recv, y_sem):
    sp = lax.axis_index("sp")
    tp = lax.axis_index("tp")
    my_z, my_y = tp // NY, tp % NY
    my_x, my_c = sp // 2, sp % 2
    n_tp = NY * NY
    n_sp = 8
    chunk = kv_v.shape[0] // (2 * n_sp)
    head = kv_v.shape[1] // 2
    cols = yst.shape[2]
    rows = yst.shape[1]
    part = NY * rows
    coef = head ** -0.5 * LOG2E
    d_half = wq_v.shape[1] // 2
    s_rows = d_half // (6 * 32) * 32 - 32
    d_rows = d_half - NY * s_rows

    x_load = pltpu.make_async_copy(x_hbm, xg.at[my_y], x_sem)
    x_load.start()
    w_loads = (pltpu.make_async_copy(wk_hbm, wkv_v.at[my_z, :, 0:head], wl_sem.at[0]),
               pltpu.make_async_copy(wv_hbm, wkv_v.at[my_z, :, head:2 * head], wl_sem.at[1]),
               pltpu.make_async_copy(wq_hbm, wq_v.at[my_z], wl_sem.at[2]))
    for load in w_loads:
        load.start()

    barrier = pltpu.get_barrier_semaphore()
    for step in range(1, n_tp):
        pl.semaphore_signal(barrier, inc=1, device_id={"tp": (tp + step) % n_tp}, device_id_type=MESH)
    for step in range(1, n_sp):
        pl.semaphore_signal(barrier, inc=1, device_id={"sp": (sp + step) % n_sp}, device_id_type=MESH)
    pl.semaphore_wait(barrier, n_tp + n_sp - 2)

    zm, zp, zo = (my_z + 3) % NY, (my_z + 1) % NY, (my_z + 2) % NY
    ym, yp, yo = (my_y + 3) % NY, (my_y + 1) % NY, (my_y + 2) % NY
    x_left, x_right, x_far = (my_x + 3) % NY, (my_x + 1) % NY, (my_x + 2) % NY
    partner = {"sp": 2 * my_x + 1 - my_c}
    sends = []
    n_sends = [0, 0]

    def x_copy(y_src, first, count, y_dst, slot):
        ref = xg.at[y_src, pl.ds(first * (rows // 2), count * (rows // 2))]
        return pltpu.make_async_remote_copy(src_ref=ref, dst_ref=ref, send_sem=x_send.at[slot], recv_sem=x_recv.at[y_src, first],
                                            device_id={"tp": NY * my_z + y_dst}, device_id_type=MESH)

    def x_put(y_src, first, count, y_dst):
        copy = x_copy(y_src, first, count, y_dst, n_sends[0])
        n_sends[0] += 1
        sends.append(copy)
        copy.start()

    def x_wait(y_src, first, count):
        x_copy(y_src, first, count, 0, 0).wait_recv()

    def w_copy(kind, z_src, x_src, first, count, dst, slot):
        size = d_rows if x_src is None else s_rows
        base = my_c * d_half + (0 if x_src is None else d_rows + x_src * s_rows)
        ref = (wq_v if kind else wkv_v).at[z_src, pl.ds(pl.multiple_of(base + first * (size // 2), 16), count * (size // 2))]
        return pltpu.make_async_remote_copy(src_ref=ref, dst_ref=ref, send_sem=w_send.at[slot],
                                            recv_sem=w_recv.at[kind, z_src, NY if x_src is None else x_src, first], device_id=dst, device_id_type=MESH)

    def w_put(kind, z_src, x_src, first, count, dst):
        copy = w_copy(kind, z_src, x_src, first, count, dst, n_sends[1])
        n_sends[1] += 1
        sends.append(copy)
        copy.start()

    def w_wait(kind, z_src, x_src, first, count):
        w_copy(kind, z_src, x_src, first, count, {"tp": 0}, 0).wait_recv()

    def to_z(z_dst):
        return {"tp": NY * z_dst + my_y}

    def to_x(x_dst):
        return {"sp": 2 * x_dst + my_c}

    def share_copy(kind, z_src, core, slot):
        ref = (wq_v if kind else wkv_v).at[z_src, pl.ds(pl.multiple_of(core * d_half, 64), d_half)]
        return pltpu.make_async_remote_copy(src_ref=ref, dst_ref=ref, send_sem=share_send.at[kind, slot], recv_sem=share_recv.at[kind, z_src],
                                            device_id=partner, device_id_type=MESH)

    def blk_of(z_idx):
        return jnp.where(z_idx < NY // 2, sp, 2 * n_sp - 1 - sp)

    def kv_rows(z_idx):
        return pl.multiple_of(blk_of(z_idx) * chunk + (z_idx % 2) * part, part)

    def own_products(y_list):
        def body(idx, carry):
            y_idx = y_list[0]
            for other in range(1, len(y_list)):
                y_idx = jnp.where(idx == other, y_list[other], y_idx)
            prod = jnp.dot(xg[y_idx], wkv_v[my_z], preferred_element_type=jnp.float32).astype(jnp.bfloat16)
            kv_v[pl.ds(pl.multiple_of(kv_rows(my_z) + y_idx * rows, rows), rows), :] = prod
            prod = jnp.dot(xg[y_idx], wq_v[my_z], preferred_element_type=jnp.float32).astype(jnp.bfloat16)
            q_v[pl.ds(pl.multiple_of(my_z * part + y_idx * rows, rows), rows), :] = prod
            return carry

        lax.fori_loop(0, len(y_list), body, 0)

    def a_copy(kind, z_src, z_dst, slot):
        if kind:
            src, dst = o_st.at[pl.ds(slot * part, part)], q_v.at[pl.ds(pl.multiple_of(z_src * part, part), part)]
        else:
            src, dst = kv_st.at[slot], kv_v.at[pl.ds(kv_rows(z_src), part)]
        return pltpu.make_async_remote_copy(src_ref=src, dst_ref=dst, send_sem=a_send.at[kind, slot], recv_sem=a_recv.at[kind, z_src],
                                            device_id=to_z(z_dst), device_id_type=MESH)

    def products(kind, z_dst, slot):
        def body(idx, carry):
            lhs = xg[pl.ds(2 * idx, 2)].reshape(2 * rows, xg.shape[2])
            prod = jnp.dot(lhs, (wq_v if kind else wkv_v)[z_dst], preferred_element_type=jnp.float32).astype(jnp.bfloat16)
            if kind:
                o_st[pl.ds(pl.multiple_of(slot * part + idx * 2 * rows, 2 * rows), 2 * rows), :] = prod
            else:
                kv_st[slot, pl.ds(pl.multiple_of(idx * 2 * rows, 2 * rows), 2 * rows), :] = prod
            return carry

        lax.fori_loop(0, 2, body, 0)

    def a_start(kind, z_dst, slot):
        a_copy(kind, my_z, z_dst, slot).start()

    def a_wait(kind, z_src):
        a_copy(kind, z_src, 0, 0).wait_recv()

    def kv_part(pair, core, z_idx, kind, dst):
        blk = jnp.where(pair < NY, 2 * pair + core, 2 * pair + 1 - core)
        ref = kv_v.at[pl.ds(pl.multiple_of(blk * chunk + (z_idx % 2) * part, part), part)]
        return pltpu.make_async_remote_copy(src_ref=ref, dst_ref=ref, send_sem=kv_send.at[z_idx, kind], recv_sem=kv_recv.at[blk, z_idx % 2],
                                            device_id=dst, device_id_type=MESH)

    def own_pair(z_idx):
        return jnp.where(z_idx < NY // 2, my_x, 2 * NY - 1 - my_x)

    def own_next(z_idx):
        low = z_idx < NY // 2
        return jnp.where(low, jnp.where(my_x < NY - 1, my_x + 1, NY - 2), my_x - 1), low | (my_x >= 1)

    def direct_in(z_idx):
        low = z_idx < NY // 2
        return jnp.where(low, my_x - 1, 2 * NY - 2 - my_x), (low & (my_x >= 1)) | (jnp.logical_not(low) & (my_x < NY - 1))

    def direct_next(z_idx):
        return jnp.where(z_idx < NY // 2, my_x + 1, my_x - 1), (my_x >= 1) & (my_x < NY - 1)

    def relay_in(z_idx):
        low = z_idx < NY // 2
        return jnp.where(low, my_x - 2, 2 * NY - 3 - my_x), (low & (my_x >= 2)) | (jnp.logical_not(low) & (my_x < NY - 2))

    def turn_in(z_idx):
        return NY - 1, (z_idx < NY // 2) & (my_x == NY - 2)

    def kv_own(z_idx, act):
        dst, wanted = own_next(z_idx)

        @pl.when(wanted)
        def _():
            act(kv_part(own_pair(z_idx), my_c, z_idx, 1, to_x(dst)))

        act(kv_part(own_pair(z_idx), my_c, z_idx, 0, partner))

    def kv_direct(z_idx, act, arrive):
        pair, wanted = direct_in(z_idx)

        @pl.when(wanted)
        def _():
            if arrive:
                kv_part(pair, my_c, z_idx, 2, partner).wait_recv()
            dst, more = direct_next(z_idx)

            @pl.when(more)
            def _():
                act(kv_part(pair, my_c, z_idx, 3, to_x(dst)))

            act(kv_part(pair, my_c, z_idx, 2, partner))

    def kv_relay(z_idx, act, arrive):
        for kind, (pair, wanted) in ((4, relay_in(z_idx)), (5, turn_in(z_idx))):
            @pl.when(wanted)
            def _(kind=kind, pair=pair):
                copy = kv_part(pair, my_c, z_idx, kind, partner)
                if arrive:
                    copy.wait_recv()
                act(copy)

    def kv_from_partner(z_idx):
        kv_part(own_pair(z_idx), 1 - my_c, z_idx, 0, partner).wait_recv()
        for pair, wanted in (direct_in(z_idx), relay_in(z_idx), turn_in(z_idx)):
            @pl.when(wanted)
            def _(pair=pair):
                kv_part(pair, 1 - my_c, z_idx, 0, partner).wait_recv()

    def start(copy):
        copy.start()

    def done(copy):
        copy.wait_send()

    group = 2 * (my_x % 2) + my_c
    x_group = 2 - 2 * (my_x % 2) + my_c

    def wo_copy(step):
        dst = (my_z + step) % NY
        src_ref = wo_hbm.at[group, :, pl.ds(pl.multiple_of(dst * cols, 128), cols)]
        return pltpu.make_async_remote_copy(src_ref=src_ref, dst_ref=wo_v.at[NY * my_y + my_z, group], send_sem=wo_send.at[step],
                                            recv_sem=wo_recv.at[my_z], device_id=to_z(dst), device_id_type=MESH)

    wo_own = pltpu.make_async_copy(wo_hbm.at[group, :, pl.ds(pl.multiple_of(my_z * cols, 128), cols)], wo_v.at[NY * my_y + my_z, group], wo_sem)

    def wo_z_start():
        wo_own.start()
        for step in range(1, NY):
            wo_copy(step).start()

    def wy_copy(y_src, first, count, y_dst, slot):
        ref = wo_v.at[pl.ds(NY * y_src + 2 * first, 2 * count), group]
        return pltpu.make_async_remote_copy(src_ref=ref, dst_ref=ref, send_sem=wy_send.at[slot], recv_sem=wy_recv.at[y_src, first],
                                            device_id={"tp": NY * my_z + y_dst}, device_id_type=MESH)

    wy_sends = (wy_copy(my_y, 0, 2, yp, 0), wy_copy(my_y, 0, 2, ym, 1), wy_copy(ym, 0, 1, yp, 2), wy_copy(yp, 1, 1, ym, 3))

    def wo_y_start():
        wo_own.wait()
        for z_src in (zm, zp, zo):
            ref = wo_v.at[NY * my_y + z_src, group]
            pltpu.make_async_remote_copy(src_ref=ref, dst_ref=ref, send_sem=wo_send.at[1], recv_sem=wo_recv.at[z_src],
                                         device_id=to_z(z_src), device_id_type=MESH).wait_recv()
        for copy in wy_sends[:2]:
            copy.start()

    def wo_y_pass():
        for y_src, copy in ((ym, wy_sends[2]), (yp, wy_sends[3])):
            wy_copy(y_src, 0, 2, 0, 0).wait_recv()
            copy.start()

    def slab_copy(grp, first, count, dst, slot):
        ref = wo_v.at[pl.ds(first * (n_tp // 2), count * (n_tp // 2)), grp]
        return pltpu.make_async_remote_copy(src_ref=ref, dst_ref=ref, send_sem=sl_send.at[slot], recv_sem=sl_recv.at[grp, first],
                                            device_id=dst, device_id_type=MESH)

    slabs = (slab_copy(group, 0, 1, to_x(x_right), 0), slab_copy(group, 1, 1, to_x(x_left), 1), slab_copy(group, 0, 2, partner, 2),
             slab_copy(x_group, 0, 2, partner, 3))

    def wo_first():
        for first in range(2):
            wy_copy(yo, first, 1, 0, 0).wait_recv()
        for copy in slabs[:3]:
            copy.start()

    def wo_second():
        for first in range(2):
            slab_copy(x_group, first, 1, partner, 3).wait_recv()
        slabs[3].start()

    def wo_last():
        for grp in (2 * (my_x % 2), 2 - 2 * (my_x % 2)):
            slab_copy(grp + 1 - my_c, 0, 2, partner, 3).wait_recv()

    def w_own_slice(kind):
        for z_dst in (zp, zm):
            w_put(kind, my_z, my_x, 0, 2, to_z(z_dst))

    def w_slices(kind):
        for z_src, first, z_dst in ((zm, 0, zp), (zp, 1, zm)):
            w_wait(kind, z_src, my_x, 0, 2)
            w_put(kind, z_src, my_x, first, 1, to_z(z_dst))
            for x_dst in (x_right, x_left):
                w_put(kind, z_src, my_x, 0, 2, to_x(x_dst))

    def w_own_rest(kind):
        for z_dst in (zp, zm):
            w_put(kind, my_z, None, 0, 2, to_z(z_dst))

    def w_far_slice(kind):
        for first in range(2):
            w_wait(kind, zo, my_x, first, 1)
        for x_dst in (x_right, x_left):
            w_put(kind, zo, my_x, 0, 2, to_x(x_dst))

    def w_ring(kind, z_src):
        for x_src, first, x_dst in ((x_left, 0, x_right), (x_right, 1, x_left)):
            w_wait(kind, z_src, x_src, 0, 2)
            w_put(kind, z_src, x_src, first, 1, to_x(x_dst))

    def w_rest(kind):
        for z_src, first, z_dst in ((zm, 0, zp), (zp, 1, zm)):
            w_wait(kind, z_src, None, 0, 2)
            w_put(kind, z_src, None, first, 1, to_z(z_dst))

    def w_share(kind, z_src, slot):
        for first in range(2):
            w_wait(kind, z_src, x_far, first, 1)
            if slot == 2:
                w_wait(kind, z_src, None, first, 1)
        share_copy(kind, z_src, my_c, slot).start()

    def w_full(kind, z_src, slot):
        share_copy(kind, z_src, 1 - my_c, slot).wait_recv()

    x_load.wait()
    x_put(my_y, 0, 2, yp)
    x_put(my_y, 0, 2, ym)
    for load in w_loads[:2]:
        load.wait()
    w_own_slice(0)
    w_slices(0)
    w_own_rest(0)
    wo_z_start()
    w_loads[2].wait()
    w_own_slice(1)
    w_far_slice(0)
    own_products([my_y])
    w_ring(0, zm)
    w_ring(0, zp)
    w_rest(0)
    w_ring(0, zo)
    w_slices(1)
    w_own_rest(1)
    for y_src, first, y_dst in ((ym, 0, yp), (yp, 1, ym)):
        x_wait(y_src, 0, 2)
        x_put(y_src, first, 1, y_dst)
    w_share(0, zm, 0)
    w_share(0, zp, 1)
    w_far_slice(1)
    own_products([ym, yp])
    w_share(0, zo, 2)
    w_ring(1, zm)
    w_ring(1, zp)
    for first in range(2):
        x_wait(yo, first, 1)
    own_products([yo])
    kv_own(my_z, start)
    for slot, z_dst in enumerate((zo, zm, zp)):
        w_full(0, z_dst, slot)
        products(0, z_dst, slot)
        a_start(0, z_dst, slot)
    w_rest(1)
    w_ring(1, zo)
    wo_y_start()
    kv_direct(my_z, start, True)
    for z_src in (zo, zm, zp):
        a_wait(0, z_src)
        kv_own(z_src, start)
    for slot, z_src in enumerate((zm, zp, zo)):
        w_share(1, z_src, slot)
    kv_relay(my_z, start, True)
    for slot, z_dst in enumerate((zo, zm, zp)):
        w_full(1, z_dst, slot)
        products(1, z_dst, slot)
        a_start(1, z_dst, slot)
        kv_direct(z_dst, start, True)
        if slot == 0:
            wo_y_pass()
    for z_src in (zo, zm, zp):
        kv_relay(z_src, start, True)
    wo_first()
    for z_src in (zm, zp, zo):
        a_wait(1, z_src)
    for slot in range(3):
        a_copy(1, my_z, 0, slot).wait_send()
    for z_idx in range(NY):
        kv_from_partner(z_idx)

    row_i = lax.broadcasted_iota(jnp.int32, (2 * TQ, TQ), 0) % TQ
    col_i = lax.broadcasted_iota(jnp.int32, (2 * TQ, TQ), 1)

    def lane_max(scores):
        best = scores[:, 0:head]
        for idx in range(1, scores.shape[1] // head):
            best = jnp.maximum(best, scores[:, idx * head:(idx + 1) * head])
        return best

    def o_copy(tile, z_dst):
        y_dst, z_row = tile % NY, tile // NY
        src = o_st.at[pl.ds(pl.multiple_of(tile * rows, rows), rows)]
        dst = og.at[z_row, :, pl.ds(pl.multiple_of(tp * 2 * head, 2 * head), 2 * head)]
        return pltpu.make_async_remote_copy(src_ref=src, dst_ref=dst, send_sem=o_send.at[tile, z_dst], recv_sem=o_recv.at[z_row, tp],
                                            device_id={"tp": NY * z_dst + y_dst}, device_id_type=MESH)

    def o_arrival(z_row, src):
        dst = og.at[z_row, :, pl.ds(src * 2 * head, 2 * head)]
        return pltpu.make_async_remote_copy(src_ref=o_st.at[pl.ds(0, rows)], dst_ref=dst, send_sem=o_send.at[0, 0],
                                            recv_sem=o_recv.at[z_row, src], device_id={"tp": 0}, device_id_type=MESH)

    def attend(q_idx, gidx, wide, start_tile, n_steps, with_first):
        q_blk = q_v[pl.ds(pl.multiple_of(q_idx * TQ, TQ), TQ), :]
        q_two = jnp.concatenate([q_blk[:, :head], q_blk[:, head:]], axis=0)

        def keys(tile, width):
            return kv_v[pl.ds(pl.multiple_of(tile * TQ, TQ), width), 0:head]

        def values(tile, width):
            return kv_v[pl.ds(pl.multiple_of(tile * TQ, TQ), width), head:2 * head]

        per = wide // TQ
        scores = jnp.where(col_i <= row_i, dot_nt(q_two, keys(gidx, TQ)) * coef, NEG_BIG)
        s_v[:, 0:TQ] = scores
        best = lane_max(scores)
        if with_first:
            scores = jnp.where(col_i > row_i, dot_nt(q_two, keys(gidx - WINDOW // TQ, TQ)) * coef, NEG_BIG)
            s_v[:, TQ:2 * TQ] = scores
            best = jnp.maximum(best, lane_max(scores))
        mx_v[...] = best

        def score_step(idx, carry):
            part = dot_nt(q_two, keys(start_tile + per * idx, wide)) * coef
            s_v[:, pl.ds(pl.multiple_of(2 * TQ + idx * wide, TQ), wide)] = part
            mx_v[...] = jnp.maximum(mx_v[...], lane_max(part))
            return carry

        lax.fori_loop(0, n_steps, score_step, 0)
        row_best = jnp.max(mx_v[...], axis=1, keepdims=True)
        mb_v[...] = jnp.broadcast_to(row_best, mb_v.shape)

        def probs(col, width):
            base = mb_v[...]
            total = None
            parts = []
            for idx in range(width // head):
                part = jnp.exp2(s_v[:, pl.ds(pl.multiple_of(col + idx * head, head), head)] - base)
                total = part if total is None else total + part
                parts.append(part.astype(jnp.bfloat16))
            return jnp.concatenate(parts, axis=1), total

        prob, total = probs(0, TQ)
        acc = jnp.dot(prob, values(gidx, TQ), preferred_element_type=jnp.float32)
        if with_first:
            prob, total_b = probs(TQ, TQ)
            total = total + total_b
            acc = acc + jnp.dot(prob, values(gidx - WINDOW // TQ, TQ), preferred_element_type=jnp.float32)
        l_v[...] = total
        acc_v[...] = acc

        def value_step(idx, carry):
            prob, total = probs(2 * TQ + idx * wide, wide)
            l_v[...] += total
            acc_v[...] += jnp.dot(prob, values(start_tile + per * idx, wide), preferred_element_type=jnp.float32)
            return carry

        lax.fori_loop(0, n_steps, value_step, 0)
        denom = jnp.sum(l_v[...], axis=1, keepdims=True)
        out = (acc_v[...] / denom).astype(jnp.bfloat16)
        out = jnp.concatenate([out[:TQ], out[TQ:]], axis=1)
        o_st[pl.ds(pl.multiple_of(q_idx * TQ, TQ), TQ), :] = out

    def y_copy(z_dst, z_src):
        return pltpu.make_async_remote_copy(
            src_ref=yst.at[z_dst], dst_ref=yv.at[:, pl.ds(pl.multiple_of(z_src * cols, 128), cols)],
            send_sem=y_send.at[z_dst], recv_sem=y_recv.at[z_src], device_id={"tp": NY * z_dst + my_y}, device_id_type=MESH)

    def out_product(first, count):
        for row in range(first, first + count):
            for src in range(n_tp):
                @pl.when(tp != src)
                def _(row=row, src=src):
                    o_arrival(row, src).wait_recv()
        lhs = og[first:first + count].reshape(count * rows, n_tp * 2 * head)
        for col in range(0, cols, 384):
            w_cols = jnp.concatenate([wo_v[NY * y_idx + z_idx, :, :, col:col + 384].reshape(2 * head, 384)
                                      for z_idx in range(NY) for y_idx in range(NY)], axis=0)
            res = jnp.dot(lhs, w_cols, preferred_element_type=jnp.float32).astype(jnp.bfloat16)
            yst[first:first + count, :, col:col + 384] = res.reshape(count, rows, 384)

    def y_put(first, count):
        for z_dst in range(first, first + count):
            @pl.when(my_z != z_dst)
            def _(z_dst=z_dst):
                y_copy(z_dst, my_z).start()

            @pl.when(my_z == z_dst)
            def _(z_dst=z_dst):
                yv[:, pl.ds(pl.multiple_of(my_z * cols, 128), cols)] = yst[z_dst]

    def q_step(q_idx, carry):
        tiles = chunk // TQ
        blk = jnp.where(q_idx < tiles, sp, 2 * n_sp - 1 - sp)
        gidx = blk * tiles + q_idx % tiles

        @pl.when(gidx >= WINDOW // TQ)
        def _():
            attend(q_idx, gidx, WIDE, gidx - WINDOW // TQ + 1, N_WIDE, True)

        @pl.when(gidx < WINDOW // TQ)
        def _():
            attend(q_idx, gidx, TQ, 0, gidx, False)

        for sub in range(2):
            tile = 2 * q_idx + sub

            for z_dst in range(NY):
                mine = (tile % NY == my_y) & (my_z == z_dst)

                @pl.when(jnp.logical_not(mine))
                def _(tile=tile, z_dst=z_dst):
                    o_copy(tile, z_dst).start()

            @pl.when(tile % NY == my_y)
            def _(tile=tile):
                og[tile // NY, :, pl.ds(pl.multiple_of(tp * 2 * head, 2 * head), 2 * head)] = \
                    o_st[pl.ds(pl.multiple_of(tile * rows, rows), rows), :]

        @pl.when(q_idx == 5)
        def _():
            wo_second()

        @pl.when(q_idx == 6)
        def _():
            wo_last()
            out_product(0, 1)
            y_put(0, 1)

        @pl.when(q_idx == 7)
        def _():
            out_product(1, 1)
            y_put(1, 1)

        return carry

    lax.fori_loop(0, 2 * chunk // TQ, q_step, 0)

    out_product(2, 1)
    y_put(2, 1)
    out_product(3, 1)
    y_put(3, 1)
    for z_src in range(NY):
        @pl.when(my_z != z_src)
        def _(z_src=z_src):
            y_copy(z_src, z_src).wait_recv()
    y_out = pltpu.make_async_copy(yv, y_hbm, y_sem)
    y_out.start()
    for tile in range(n_tp):
        for z_dst in range(NY):
            mine = (tile % NY == my_y) & (my_z == z_dst)

            @pl.when(jnp.logical_not(mine))
            def _(tile=tile, z_dst=z_dst):
                o_copy(tile, z_dst).wait_send()
    for z_dst in range(NY):
        @pl.when(my_z != z_dst)
        def _(z_dst=z_dst):
            y_copy(z_dst, my_z).wait_send()
    for copy in sends + list(slabs):
        copy.wait_send()
    for step in range(1, NY):
        wo_copy(step).wait_send()
    for copy in wy_sends:
        copy.wait_send()
    for slot in range(3):
        for kind in range(2):
            share_copy(kind, my_z, my_c, slot).wait_send()
    for slot in range(3):
        a_copy(0, my_z, 0, slot).wait_send()
    for z_idx in range(NY):
        kv_own(z_idx, done)
        kv_direct(z_idx, done, False)
        kv_relay(z_idx, done, False)
    y_out.wait()


def solution(mesh):
    n_sp, n_tp = mesh.shape["sp"], mesh.shape["tp"]

    def local_attn(x_part, w_query, w_key, w_value, w_out):
        rows, d_model = x_part.shape
        heads_loc, head = w_query.shape[1], w_query.shape[2]
        two_head = heads_loc * head
        seq_loc = rows * n_tp
        cols = d_model // NY
        any_spec = pl.BlockSpec(memory_space=pl.ANY)
        dma = pltpu.SemaphoreType.DMA
        bf16, f32 = jnp.bfloat16, jnp.float32
        wo_rows = w_out.shape[0] * w_out.shape[1] // NY
        return pl.pallas_call(
            layer_kernel,
            out_shape=jax.ShapeDtypeStruct((rows, d_model), bf16),
            in_specs=[any_spec] * 5,
            out_specs=any_spec,
            scratch_shapes=[
                pltpu.VMEM((NY, rows, d_model), bf16),
                pltpu.VMEM((NY, d_model, two_head), bf16),
                pltpu.VMEM((NY, d_model, two_head), bf16),
                pltpu.VMEM((seq_loc, two_head), bf16),
                pltpu.VMEM((n_sp * seq_loc, two_head), bf16),
                pltpu.VMEM((NY - 1, seq_loc // NY, two_head), bf16),
                pltpu.VMEM((n_tp, NY, wo_rows, cols), bf16),
                pltpu.VMEM((2 * TQ, WINDOW + TQ), f32),
                pltpu.VMEM((2 * TQ, head), f32),
                pltpu.VMEM((2 * TQ, head), f32),
                pltpu.VMEM((2 * TQ, head), f32),
                pltpu.VMEM((2 * TQ, head), f32),
                pltpu.VMEM((seq_loc, two_head), bf16),
                pltpu.VMEM((NY, rows, n_tp * two_head), bf16),
                pltpu.VMEM((NY, rows, cols), bf16),
                pltpu.VMEM((rows, d_model), bf16),
                dma, dma((3,)), dma((4,)), dma((NY, 2)), dma((40,)), dma((2, NY, NY + 1, 2)), dma((2, 3)), dma((2, NY)), dma((2, 3)), dma((2, NY)),
                dma((NY, 6)), dma((2 * n_sp, 2)), dma, dma((NY,)), dma((NY,)), dma((4,)), dma((NY, 2)), dma((4,)), dma((NY, 2)),
                dma((n_tp, NY)), dma((NY, n_tp)), dma((NY,)), dma((NY,)), dma,
            ],
            compiler_params=pltpu.CompilerParams(collective_id=1, has_side_effects=True, vmem_limit_bytes=67043328),
            name="layer",
        )(x_part, w_query.reshape(d_model, two_head), w_key.reshape(d_model, head), w_value.reshape(d_model, head),
          w_out.reshape(NY, wo_rows, d_model))

    return jax.shard_map(local_attn, mesh=mesh, in_specs=(P(("dp", "sp", "tp"), None), P(None, "tp", None), P(None, "tp", None), P(None, "tp", None), P("tp", None, None)), out_specs=P(("dp", "sp", "tp"), None), check_vma=False)
```

```python
import functools

import jax
import jax.numpy as jnp
from jax import lax
from jax.experimental import pallas as pl
from jax.experimental.pallas import tpu as pltpu
from jax.sharding import PartitionSpec as P

WINDOW = 4096
NEG_BIG = -1e30
LOG2E = 1.4426950408889634
MESH = pl.DeviceIdType.MESH
NY = 4
TQ = 256
WIDE = 768
N_WIDE = (WINDOW - TQ) // WIDE


def dot_nt(lhs, rhs):
    return lax.dot_general(lhs, rhs, (((1,), (1,)), ((), ())), preferred_element_type=jnp.float32)


def layer_kernel(x_hbm, wq_hbm, wk_hbm, wv_hbm, wo_hbm, y_hbm, xg, wq_v, wkv_v, q_v, kv_v, kv_st, wo_v, s_v, mx_v, mb_v, l_v, acc_v, o_st,
                 og, yst, yv, x_sem, wl_sem, x_send, x_recv, w_send, w_recv, share_send, share_recv, a_send, a_recv,
                 kv_send, kv_recv, wo_sem, wo_send, wo_recv, wy_send, wy_recv, sl_send, sl_recv, o_send, o_recv,
                 y_send, y_recv, y_sem):
    sp = lax.axis_index("sp")
    tp = lax.axis_index("tp")
    my_z, my_y = tp // NY, tp % NY
    my_x, my_c = sp // 2, sp % 2
    n_tp = NY * NY
    n_sp = 8
    chunk = kv_v.shape[0] // (2 * n_sp)
    head = kv_v.shape[1] // 2
    cols = yst.shape[2]
    rows = yst.shape[1]
    part = NY * rows
    coef = head ** -0.5 * LOG2E
    d_half = wq_v.shape[1] // 2
    s_rows = d_half // (6 * 32) * 32 - 32
    d_rows = d_half - NY * s_rows

    x_load = pltpu.make_async_copy(x_hbm, xg.at[my_y], x_sem)
    x_load.start()
    w_loads = (pltpu.make_async_copy(wk_hbm, wkv_v.at[my_z, :, 0:head], wl_sem.at[0]),
               pltpu.make_async_copy(wv_hbm, wkv_v.at[my_z, :, head:2 * head], wl_sem.at[1]),
               pltpu.make_async_copy(wq_hbm, wq_v.at[my_z], wl_sem.at[2]))
    for load in w_loads:
        load.start()

    barrier = pltpu.get_barrier_semaphore()
    for step in range(1, n_tp):
        pl.semaphore_signal(barrier, inc=1, device_id={"tp": (tp + step) % n_tp}, device_id_type=MESH)
    for step in range(1, n_sp):
        pl.semaphore_signal(barrier, inc=1, device_id={"sp": (sp + step) % n_sp}, device_id_type=MESH)
    pl.semaphore_wait(barrier, n_tp + n_sp - 2)

    zm, zp, zo = (my_z + 3) % NY, (my_z + 1) % NY, (my_z + 2) % NY
    ym, yp, yo = (my_y + 3) % NY, (my_y + 1) % NY, (my_y + 2) % NY
    x_left, x_right, x_far = (my_x + 3) % NY, (my_x + 1) % NY, (my_x + 2) % NY
    partner = {"sp": 2 * my_x + 1 - my_c}
    sends = []
    n_sends = [0, 0]

    def x_copy(y_src, first, count, y_dst, slot):
        ref = xg.at[y_src, pl.ds(first * (rows // 2), count * (rows // 2))]
        return pltpu.make_async_remote_copy(src_ref=ref, dst_ref=ref, send_sem=x_send.at[slot], recv_sem=x_recv.at[y_src, first],
                                            device_id={"tp": NY * my_z + y_dst}, device_id_type=MESH)

    def x_put(y_src, first, count, y_dst):
        copy = x_copy(y_src, first, count, y_dst, n_sends[0])
        n_sends[0] += 1
        sends.append(copy)
        copy.start()

    def x_wait(y_src, first, count):
        x_copy(y_src, first, count, 0, 0).wait_recv()

    def w_copy(kind, z_src, x_src, first, count, dst, slot):
        size = d_rows if x_src is None else s_rows
        base = my_c * d_half + (0 if x_src is None else d_rows + x_src * s_rows)
        ref = (wq_v if kind else wkv_v).at[z_src, pl.ds(pl.multiple_of(base + first * (size // 2), 16), count * (size // 2))]
        return pltpu.make_async_remote_copy(src_ref=ref, dst_ref=ref, send_sem=w_send.at[slot],
                                            recv_sem=w_recv.at[kind, z_src, NY if x_src is None else x_src, first], device_id=dst, device_id_type=MESH)

    def w_put(kind, z_src, x_src, first, count, dst):
        copy = w_copy(kind, z_src, x_src, first, count, dst, n_sends[1])
        n_sends[1] += 1
        sends.append(copy)
        copy.start()

    def w_wait(kind, z_src, x_src, first, count):
        w_copy(kind, z_src, x_src, first, count, {"tp": 0}, 0).wait_recv()

    def to_z(z_dst):
        return {"tp": NY * z_dst + my_y}

    def to_x(x_dst):
        return {"sp": 2 * x_dst + my_c}

    def share_copy(kind, z_src, core, slot):
        ref = (wq_v if kind else wkv_v).at[z_src, pl.ds(pl.multiple_of(core * d_half, 64), d_half)]
        return pltpu.make_async_remote_copy(src_ref=ref, dst_ref=ref, send_sem=share_send.at[kind, slot], recv_sem=share_recv.at[kind, z_src],
                                            device_id=partner, device_id_type=MESH)

    def blk_of(z_idx):
        return jnp.where(z_idx < NY // 2, sp, 2 * n_sp - 1 - sp)

    def kv_rows(z_idx):
        return pl.multiple_of(blk_of(z_idx) * chunk + (z_idx % 2) * part, part)

    def own_products(y_list):
        def body(idx, carry):
            y_idx = y_list[0]
            for other in range(1, len(y_list)):
                y_idx = jnp.where(idx == other, y_list[other], y_idx)
            prod = jnp.dot(xg[y_idx], wkv_v[my_z], preferred_element_type=jnp.float32).astype(jnp.bfloat16)
            kv_v[pl.ds(pl.multiple_of(kv_rows(my_z) + y_idx * rows, rows), rows), :] = prod
            prod = jnp.dot(xg[y_idx], wq_v[my_z], preferred_element_type=jnp.float32).astype(jnp.bfloat16)
            q_v[pl.ds(pl.multiple_of(my_z * part + y_idx * rows, rows), rows), :] = prod
            return carry

        lax.fori_loop(0, len(y_list), body, 0)

    def a_copy(kind, z_src, z_dst, slot):
        if kind:
            src, dst = o_st.at[pl.ds(slot * part, part)], q_v.at[pl.ds(pl.multiple_of(z_src * part, part), part)]
        else:
            src, dst = kv_st.at[slot], kv_v.at[pl.ds(kv_rows(z_src), part)]
        return pltpu.make_async_remote_copy(src_ref=src, dst_ref=dst, send_sem=a_send.at[kind, slot], recv_sem=a_recv.at[kind, z_src],
                                            device_id=to_z(z_dst), device_id_type=MESH)

    def products(kind, z_dst, slot):
        def body(idx, carry):
            lhs = xg[pl.ds(2 * idx, 2)].reshape(2 * rows, xg.shape[2])
            prod = jnp.dot(lhs, (wq_v if kind else wkv_v)[z_dst], preferred_element_type=jnp.float32).astype(jnp.bfloat16)
            if kind:
                o_st[pl.ds(pl.multiple_of(slot * part + idx * 2 * rows, 2 * rows), 2 * rows), :] = prod
            else:
                kv_st[slot, pl.ds(pl.multiple_of(idx * 2 * rows, 2 * rows), 2 * rows), :] = prod
            return carry

        lax.fori_loop(0, 2, body, 0)

    def a_start(kind, z_dst, slot):
        a_copy(kind, my_z, z_dst, slot).start()

    def a_wait(kind, z_src):
        a_copy(kind, z_src, 0, 0).wait_recv()

    def kv_part(pair, core, z_idx, kind, dst):
        blk = jnp.where(pair < NY, 2 * pair + core, 2 * pair + 1 - core)
        ref = kv_v.at[pl.ds(pl.multiple_of(blk * chunk + (z_idx % 2) * part, part), part)]
        return pltpu.make_async_remote_copy(src_ref=ref, dst_ref=ref, send_sem=kv_send.at[z_idx, kind], recv_sem=kv_recv.at[blk, z_idx % 2],
                                            device_id=dst, device_id_type=MESH)

    def own_pair(z_idx):
        return jnp.where(z_idx < NY // 2, my_x, 2 * NY - 1 - my_x)

    def own_next(z_idx):
        low = z_idx < NY // 2
        return jnp.where(low, jnp.where(my_x < NY - 1, my_x + 1, NY - 2), my_x - 1), low | (my_x >= 1)

    def direct_in(z_idx):
        low = z_idx < NY // 2
        return jnp.where(low, my_x - 1, 2 * NY - 2 - my_x), (low & (my_x >= 1)) | (jnp.logical_not(low) & (my_x < NY - 1))

    def direct_next(z_idx):
        return jnp.where(z_idx < NY // 2, my_x + 1, my_x - 1), (my_x >= 1) & (my_x < NY - 1)

    def relay_in(z_idx):
        low = z_idx < NY // 2
        return jnp.where(low, my_x - 2, 2 * NY - 3 - my_x), (low & (my_x >= 2)) | (jnp.logical_not(low) & (my_x < NY - 2))

    def turn_in(z_idx):
        return NY - 1, (z_idx < NY // 2) & (my_x == NY - 2)

    def kv_own(z_idx, act):
        dst, wanted = own_next(z_idx)

        @pl.when(wanted)
        def _():
            act(kv_part(own_pair(z_idx), my_c, z_idx, 1, to_x(dst)))

        act(kv_part(own_pair(z_idx), my_c, z_idx, 0, partner))

    def kv_direct(z_idx, act, arrive):
        pair, wanted = direct_in(z_idx)

        @pl.when(wanted)
        def _():
            if arrive:
                kv_part(pair, my_c, z_idx, 2, partner).wait_recv()
            dst, more = direct_next(z_idx)

            @pl.when(more)
            def _():
                act(kv_part(pair, my_c, z_idx, 3, to_x(dst)))

            act(kv_part(pair, my_c, z_idx, 2, partner))

    def kv_relay(z_idx, act, arrive):
        for kind, (pair, wanted) in ((4, relay_in(z_idx)), (5, turn_in(z_idx))):
            @pl.when(wanted)
            def _(kind=kind, pair=pair):
                copy = kv_part(pair, my_c, z_idx, kind, partner)
                if arrive:
                    copy.wait_recv()
                act(copy)

    def kv_from_partner(z_idx):
        kv_part(own_pair(z_idx), 1 - my_c, z_idx, 0, partner).wait_recv()
        for pair, wanted in (direct_in(z_idx), relay_in(z_idx), turn_in(z_idx)):
            @pl.when(wanted)
            def _(pair=pair):
                kv_part(pair, 1 - my_c, z_idx, 0, partner).wait_recv()

    def start(copy):
        copy.start()

    def done(copy):
        copy.wait_send()

    group = 2 * (my_x % 2) + my_c
    x_group = 2 - 2 * (my_x % 2) + my_c

    def wo_copy(step):
        dst = (my_z + step) % NY
        src_ref = wo_hbm.at[group, :, pl.ds(pl.multiple_of(dst * cols, 128), cols)]
        return pltpu.make_async_remote_copy(src_ref=src_ref, dst_ref=wo_v.at[NY * my_y + my_z, group], send_sem=wo_send.at[step],
                                            recv_sem=wo_recv.at[my_z], device_id=to_z(dst), device_id_type=MESH)

    wo_own = pltpu.make_async_copy(wo_hbm.at[group, :, pl.ds(pl.multiple_of(my_z * cols, 128), cols)], wo_v.at[NY * my_y + my_z, group], wo_sem)

    def wo_z_start():
        wo_own.start()
        for step in range(1, NY):
            wo_copy(step).start()

    def wy_copy(y_src, first, count, y_dst, slot):
        ref = wo_v.at[pl.ds(NY * y_src + 2 * first, 2 * count), group]
        return pltpu.make_async_remote_copy(src_ref=ref, dst_ref=ref, send_sem=wy_send.at[slot], recv_sem=wy_recv.at[y_src, first],
                                            device_id={"tp": NY * my_z + y_dst}, device_id_type=MESH)

    wy_sends = (wy_copy(my_y, 0, 2, yp, 0), wy_copy(my_y, 0, 2, ym, 1), wy_copy(ym, 0, 1, yp, 2), wy_copy(yp, 1, 1, ym, 3))

    def wo_y_start():
        wo_own.wait()
        for z_src in (zm, zp, zo):
            ref = wo_v.at[NY * my_y + z_src, group]
            pltpu.make_async_remote_copy(src_ref=ref, dst_ref=ref, send_sem=wo_send.at[1], recv_sem=wo_recv.at[z_src],
                                         device_id=to_z(z_src), device_id_type=MESH).wait_recv()
        for copy in wy_sends[:2]:
            copy.start()

    def wo_y_pass():
        for y_src, copy in ((ym, wy_sends[2]), (yp, wy_sends[3])):
            wy_copy(y_src, 0, 2, 0, 0).wait_recv()
            copy.start()

    def slab_copy(grp, first, count, dst, slot):
        ref = wo_v.at[pl.ds(first * (n_tp // 2), count * (n_tp // 2)), grp]
        return pltpu.make_async_remote_copy(src_ref=ref, dst_ref=ref, send_sem=sl_send.at[slot], recv_sem=sl_recv.at[grp, first],
                                            device_id=dst, device_id_type=MESH)

    slabs = (slab_copy(group, 0, 1, to_x(x_right), 0), slab_copy(group, 1, 1, to_x(x_left), 1), slab_copy(group, 0, 2, partner, 2),
             slab_copy(x_group, 0, 2, partner, 3))

    def wo_first():
        for first in range(2):
            wy_copy(yo, first, 1, 0, 0).wait_recv()
        for copy in slabs[:3]:
            copy.start()

    def wo_second():
        for first in range(2):
            slab_copy(x_group, first, 1, partner, 3).wait_recv()
        slabs[3].start()

    def wo_last():
        for grp in (2 * (my_x % 2), 2 - 2 * (my_x % 2)):
            slab_copy(grp + 1 - my_c, 0, 2, partner, 3).wait_recv()

    def w_own_slice(kind):
        for z_dst in (zp, zm):
            w_put(kind, my_z, my_x, 0, 2, to_z(z_dst))

    def w_slices(kind):
        for z_src, first, z_dst in ((zm, 0, zp), (zp, 1, zm)):
            w_wait(kind, z_src, my_x, 0, 2)
            w_put(kind, z_src, my_x, first, 1, to_z(z_dst))
            for x_dst in (x_right, x_left):
                w_put(kind, z_src, my_x, 0, 2, to_x(x_dst))

    def w_own_rest(kind):
        for z_dst in (zp, zm):
            w_put(kind, my_z, None, 0, 2, to_z(z_dst))

    def w_far_slice(kind):
        for first in range(2):
            w_wait(kind, zo, my_x, first, 1)
        for x_dst in (x_right, x_left):
            w_put(kind, zo, my_x, 0, 2, to_x(x_dst))

    def w_ring(kind, z_src):
        for x_src, first, x_dst in ((x_left, 0, x_right), (x_right, 1, x_left)):
            w_wait(kind, z_src, x_src, 0, 2)
            w_put(kind, z_src, x_src, first, 1, to_x(x_dst))

    def w_rest(kind):
        for z_src, first, z_dst in ((zm, 0, zp), (zp, 1, zm)):
            w_wait(kind, z_src, None, 0, 2)
            w_put(kind, z_src, None, first, 1, to_z(z_dst))

    def w_share(kind, z_src, slot):
        for first in range(2):
            w_wait(kind, z_src, x_far, first, 1)
            if slot == 2:
                w_wait(kind, z_src, None, first, 1)
        share_copy(kind, z_src, my_c, slot).start()

    def w_full(kind, z_src, slot):
        share_copy(kind, z_src, 1 - my_c, slot).wait_recv()

    x_load.wait()
    x_put(my_y, 0, 2, yp)
    x_put(my_y, 0, 2, ym)
    for load in w_loads[:2]:
        load.wait()
    w_own_slice(0)
    w_slices(0)
    w_own_rest(0)
    wo_z_start()
    w_loads[2].wait()
    w_own_slice(1)
    w_far_slice(0)
    own_products([my_y])
    w_ring(0, zm)
    w_ring(0, zp)
    w_rest(0)
    w_ring(0, zo)
    w_slices(1)
    w_own_rest(1)
    for y_src, first, y_dst in ((ym, 0, yp), (yp, 1, ym)):
        x_wait(y_src, 0, 2)
        x_put(y_src, first, 1, y_dst)
    w_share(0, zm, 0)
    w_share(0, zp, 1)
    w_far_slice(1)
    own_products([ym, yp])
    w_share(0, zo, 2)
    w_ring(1, zm)
    w_ring(1, zp)
    for first in range(2):
        x_wait(yo, first, 1)
    own_products([yo])
    kv_own(my_z, start)
    for slot, z_dst in enumerate((zo, zm, zp)):
        w_full(0, z_dst, slot)
        products(0, z_dst, slot)
        a_start(0, z_dst, slot)
    w_rest(1)
    w_ring(1, zo)
    wo_y_start()
    kv_direct(my_z, start, True)
    for z_src in (zo, zm, zp):
        a_wait(0, z_src)
        kv_own(z_src, start)
    for slot, z_src in enumerate((zm, zp, zo)):
        w_share(1, z_src, slot)
    kv_relay(my_z, start, True)
    for slot, z_dst in enumerate((zo, zm, zp)):
        w_full(1, z_dst, slot)
        products(1, z_dst, slot)
        a_start(1, z_dst, slot)
        kv_direct(z_dst, start, True)
        if slot == 0:
            wo_y_pass()
    for z_src in (zo, zm, zp):
        kv_relay(z_src, start, True)
    wo_first()
    for z_src in (zm, zp, zo):
        a_wait(1, z_src)
    for slot in range(3):
        a_copy(1, my_z, 0, slot).wait_send()
    for z_idx in range(NY):
        kv_from_partner(z_idx)

    row_i = lax.broadcasted_iota(jnp.int32, (2 * TQ, TQ), 0) % TQ
    col_i = lax.broadcasted_iota(jnp.int32, (2 * TQ, TQ), 1)

    def lane_max(scores):
        best = scores[:, 0:head]
        for idx in range(1, scores.shape[1] // head):
            best = jnp.maximum(best, scores[:, idx * head:(idx + 1) * head])
        return best

    def o_copy(tile, z_dst):
        y_dst, z_row = tile % NY, tile // NY
        src = o_st.at[pl.ds(pl.multiple_of(tile * rows, rows), rows)]
        dst = og.at[z_row, tp]
        return pltpu.make_async_remote_copy(src_ref=src, dst_ref=dst, send_sem=o_send.at[tile, z_dst], recv_sem=o_recv.at[z_row, tp],
                                            device_id={"tp": NY * z_dst + y_dst}, device_id_type=MESH)

    def o_arrival(z_row, src):
        dst = og.at[z_row, src]
        return pltpu.make_async_remote_copy(src_ref=o_st.at[pl.ds(0, rows)], dst_ref=dst, send_sem=o_send.at[0, 0],
                                            recv_sem=o_recv.at[z_row, src], device_id={"tp": 0}, device_id_type=MESH)

    def attend(q_idx, gidx, start_tile, n_wide, n_narrow, with_first):
        q_blk = q_v[pl.ds(pl.multiple_of(q_idx * TQ, TQ), TQ), :]
        q_two = jnp.concatenate([q_blk[:, :head], q_blk[:, head:]], axis=0)

        def keys(tile, width):
            return kv_v[pl.ds(pl.multiple_of(tile * TQ, TQ), width), 0:head]

        def values(tile, width):
            return kv_v[pl.ds(pl.multiple_of(tile * TQ, TQ), width), head:2 * head]

        per = WIDE // TQ
        scores = jnp.where(col_i <= row_i, dot_nt(q_two, keys(gidx, TQ)) * coef, NEG_BIG)
        s_v[:, 0:TQ] = scores
        best = lane_max(scores)
        if with_first:
            scores = jnp.where(col_i > row_i, dot_nt(q_two, keys(gidx - WINDOW // TQ, TQ)) * coef, NEG_BIG)
            s_v[:, TQ:2 * TQ] = scores
            best = jnp.maximum(best, lane_max(scores))
        mx_v[...] = best

        def score_step(tile, width):
            part = dot_nt(q_two, keys(start_tile + tile, width)) * coef
            s_v[:, pl.ds(pl.multiple_of((2 + tile) * TQ, TQ), width)] = part
            mx_v[...] = jnp.maximum(mx_v[...], lane_max(part))

        def each_step(step):
            def wide_step(idx, carry):
                step(per * idx, WIDE)
                return carry

            def narrow_step(idx, carry):
                step(per * n_wide + idx, TQ)
                return carry

            lax.fori_loop(0, n_wide, wide_step, 0)
            if n_narrow is not None:
                lax.fori_loop(0, n_narrow, narrow_step, 0)

        each_step(score_step)
        row_best = jnp.max(mx_v[...], axis=1, keepdims=True)
        mb_v[...] = jnp.broadcast_to(row_best, mb_v.shape)

        def probs(col, width):
            base = mb_v[...]
            total = None
            parts = []
            for idx in range(width // head):
                part = jnp.exp2(s_v[:, pl.ds(pl.multiple_of(col + idx * head, head), head)] - base)
                total = part if total is None else total + part
                parts.append(part.astype(jnp.bfloat16))
            return jnp.concatenate(parts, axis=1), total

        prob, total = probs(0, TQ)
        acc = jnp.dot(prob, values(gidx, TQ), preferred_element_type=jnp.float32)
        if with_first:
            prob, total_b = probs(TQ, TQ)
            total = total + total_b
            acc = acc + jnp.dot(prob, values(gidx - WINDOW // TQ, TQ), preferred_element_type=jnp.float32)
        l_v[...] = total
        acc_v[...] = acc

        def value_step(tile, width):
            prob, total = probs((2 + tile) * TQ, width)
            l_v[...] += total
            acc_v[...] += jnp.dot(prob, values(start_tile + tile, width), preferred_element_type=jnp.float32)

        each_step(value_step)
        denom = jnp.sum(l_v[...], axis=1, keepdims=True)
        out = (acc_v[...] / denom).astype(jnp.bfloat16)
        out = jnp.concatenate([out[:TQ], out[TQ:]], axis=1)
        o_st[pl.ds(pl.multiple_of(q_idx * TQ, TQ), TQ), :] = out

    def y_copy(z_dst, z_src):
        return pltpu.make_async_remote_copy(
            src_ref=yst.at[z_dst], dst_ref=yv.at[:, pl.ds(pl.multiple_of(z_src * cols, 128), cols)],
            send_sem=y_send.at[z_dst], recv_sem=y_recv.at[z_src], device_id={"tp": NY * z_dst + my_y}, device_id_type=MESH)

    def out_product(first, count):
        for row in range(first, first + count):
            for src in range(n_tp):
                @pl.when(tp != src)
                def _(row=row, src=src):
                    o_arrival(row, src).wait_recv()
        lhs = jnp.concatenate([og[first:first + count, src].reshape(count * rows, 2 * head) for src in range(n_tp)], axis=1)
        for col in range(0, cols, 384):
            w_cols = jnp.concatenate([wo_v[NY * y_idx + z_idx, :, :, col:col + 384].reshape(2 * head, 384)
                                      for z_idx in range(NY) for y_idx in range(NY)], axis=0)
            res = jnp.dot(lhs, w_cols, preferred_element_type=jnp.float32).astype(jnp.bfloat16)
            yst[first:first + count, :, col:col + 384] = res.reshape(count, rows, 384)

    def y_put(first, count):
        for z_dst in range(first, first + count):
            @pl.when(my_z != z_dst)
            def _(z_dst=z_dst):
                y_copy(z_dst, my_z).start()

            @pl.when(my_z == z_dst)
            def _(z_dst=z_dst):
                yv[:, pl.ds(pl.multiple_of(my_z * cols, 128), cols)] = yst[z_dst]

    def q_step(q_idx, carry):
        tiles = chunk // TQ
        blk = jnp.where(q_idx < tiles, sp, 2 * n_sp - 1 - sp)
        gidx = blk * tiles + q_idx % tiles

        @pl.when(gidx >= WINDOW // TQ)
        def _():
            attend(q_idx, gidx, gidx - WINDOW // TQ + 1, N_WIDE, None, True)

        @pl.when(gidx < WINDOW // TQ)
        def _():
            attend(q_idx, gidx, 0, gidx // (WIDE // TQ), gidx % (WIDE // TQ), False)

        for sub in range(2):
            tile = 2 * q_idx + sub

            for z_dst in range(NY):
                mine = (tile % NY == my_y) & (my_z == z_dst)

                @pl.when(jnp.logical_not(mine))
                def _(tile=tile, z_dst=z_dst):
                    o_copy(tile, z_dst).start()

            @pl.when(tile % NY == my_y)
            def _(tile=tile):
                og[tile // NY, tp] = o_st[pl.ds(pl.multiple_of(tile * rows, rows), rows), :]

        @pl.when(q_idx == 5)
        def _():
            wo_second()

        return carry

    lax.fori_loop(0, 2 * chunk // TQ, q_step, 0)

    wo_last()
    out_product(0, 2)
    y_put(0, 2)
    out_product(2, 1)
    y_put(2, 1)
    out_product(3, 1)
    y_put(3, 1)
    for z_src in range(NY):
        @pl.when(my_z != z_src)
        def _(z_src=z_src):
            y_copy(z_src, z_src).wait_recv()
    y_out = pltpu.make_async_copy(yv, y_hbm, y_sem)
    y_out.start()
    for tile in range(n_tp):
        for z_dst in range(NY):
            mine = (tile % NY == my_y) & (my_z == z_dst)

            @pl.when(jnp.logical_not(mine))
            def _(tile=tile, z_dst=z_dst):
                o_copy(tile, z_dst).wait_send()
    for z_dst in range(NY):
        @pl.when(my_z != z_dst)
        def _(z_dst=z_dst):
            y_copy(z_dst, my_z).wait_send()
    for copy in sends + list(slabs):
        copy.wait_send()
    for step in range(1, NY):
        wo_copy(step).wait_send()
    for copy in wy_sends:
        copy.wait_send()
    for slot in range(3):
        for kind in range(2):
            share_copy(kind, my_z, my_c, slot).wait_send()
    for slot in range(3):
        a_copy(0, my_z, 0, slot).wait_send()
    for z_idx in range(NY):
        kv_own(z_idx, done)
        kv_direct(z_idx, done, False)
        kv_relay(z_idx, done, False)
    y_out.wait()


def solution(mesh):
    n_sp, n_tp = mesh.shape["sp"], mesh.shape["tp"]

    def local_attn(x_part, w_query, w_key, w_value, w_out):
        rows, d_model = x_part.shape
        heads_loc, head = w_query.shape[1], w_query.shape[2]
        two_head = heads_loc * head
        seq_loc = rows * n_tp
        cols = d_model // NY
        any_spec = pl.BlockSpec(memory_space=pl.ANY)
        dma = pltpu.SemaphoreType.DMA
        bf16, f32 = jnp.bfloat16, jnp.float32
        wo_rows = w_out.shape[0] * w_out.shape[1] // NY
        return pl.pallas_call(
            layer_kernel,
            out_shape=jax.ShapeDtypeStruct((rows, d_model), bf16),
            in_specs=[any_spec] * 5,
            out_specs=any_spec,
            scratch_shapes=[
                pltpu.VMEM((NY, rows, d_model), bf16),
                pltpu.VMEM((NY, d_model, two_head), bf16),
                pltpu.VMEM((NY, d_model, two_head), bf16),
                pltpu.VMEM((seq_loc, two_head), bf16),
                pltpu.VMEM((n_sp * seq_loc, two_head), bf16),
                pltpu.VMEM((NY - 1, seq_loc // NY, two_head), bf16),
                pltpu.VMEM((n_tp, NY, wo_rows, cols), bf16),
                pltpu.VMEM((2 * TQ, WINDOW + TQ), f32),
                pltpu.VMEM((2 * TQ, head), f32),
                pltpu.VMEM((2 * TQ, head), f32),
                pltpu.VMEM((2 * TQ, head), f32),
                pltpu.VMEM((2 * TQ, head), f32),
                pltpu.VMEM((seq_loc, two_head), bf16),
                pltpu.VMEM((NY, n_tp, rows, two_head), bf16),
                pltpu.VMEM((NY, rows, cols), bf16),
                pltpu.VMEM((rows, d_model), bf16),
                dma, dma((3,)), dma((4,)), dma((NY, 2)), dma((40,)), dma((2, NY, NY + 1, 2)), dma((2, 3)), dma((2, NY)), dma((2, 3)), dma((2, NY)),
                dma((NY, 6)), dma((2 * n_sp, 2)), dma, dma((NY,)), dma((NY,)), dma((4,)), dma((NY, 2)), dma((4,)), dma((NY, 2)),
                dma((n_tp, NY)), dma((NY, n_tp)), dma((NY,)), dma((NY,)), dma,
            ],
            compiler_params=pltpu.CompilerParams(collective_id=1, has_side_effects=True, vmem_limit_bytes=67043328),
            name="layer",
        )(x_part, w_query.reshape(d_model, two_head), w_key.reshape(d_model, head), w_value.reshape(d_model, head),
          w_out.reshape(NY, wo_rows, d_model))

    return jax.shard_map(local_attn, mesh=mesh, in_specs=(P(("dp", "sp", "tp"), None), P(None, "tp", None), P(None, "tp", None), P(None, "tp", None), P("tp", None, None)), out_specs=P(("dp", "sp", "tp"), None), check_vma=False)
```

```python
import functools

import jax
import jax.numpy as jnp
from jax import lax
from jax.experimental import pallas as pl
from jax.experimental.pallas import tpu as pltpu
from jax.sharding import PartitionSpec as P

WINDOW = 4096
NEG_BIG = -1e30
LOG2E = 1.4426950408889634
MESH = pl.DeviceIdType.MESH
NY = 4
TQ = 256
WIDE = 768
N_WIDE = (WINDOW - TQ) // WIDE


def dot_nt(lhs, rhs):
    return lax.dot_general(lhs, rhs, (((1,), (1,)), ((), ())), preferred_element_type=jnp.float32)


def layer_kernel(x_hbm, wq_hbm, wk_hbm, wv_hbm, wo_hbm, y_hbm, xg, wq_v, wkv_v, q_v, kv_v, kv_st, wo_v, s_v, mx_v, mb_v, l_v, acc_v, o_st,
                 og, yst, raw_v, x_sem, wl_sem, x_send, x_recv, w_send, w_recv, share_send, share_recv, a_send, a_recv,
                 kv_send, kv_recv, wo_sem, wo_send, wo_recv, wy_send, wy_recv, sl_send, sl_recv, o_send, o_recv,
                 y_send, y_recv, y_sem):
    sp = lax.axis_index("sp")
    tp = lax.axis_index("tp")
    my_z, my_y = tp // NY, tp % NY
    my_x, my_c = sp // 2, sp % 2
    n_tp = NY * NY
    n_sp = 8
    chunk = kv_v.shape[0] // (2 * n_sp)
    head = kv_v.shape[1] // 2
    cols = yst.shape[2]
    rows = yst.shape[1]
    part = NY * rows
    coef = head ** -0.5 * LOG2E
    d_half = wq_v.shape[1] // 2
    s_rows = d_half // (6 * 32) * 32 - 32
    d_rows = d_half - NY * s_rows

    x_load = pltpu.make_async_copy(x_hbm, xg.at[my_y], x_sem)
    x_load.start()
    w_loads = (pltpu.make_async_copy(wk_hbm, wkv_v.at[my_z, :, 0:head], wl_sem.at[0]),
               pltpu.make_async_copy(wv_hbm, wkv_v.at[my_z, :, head:2 * head], wl_sem.at[1]),
               pltpu.make_async_copy(wq_hbm.at[pl.ds(0, raw_v.shape[0])], raw_v, wl_sem.at[2]))
    for load in w_loads:
        load.start()

    barrier = pltpu.get_barrier_semaphore()
    for step in range(1, n_tp):
        pl.semaphore_signal(barrier, inc=1, device_id={"tp": (tp + step) % n_tp}, device_id_type=MESH)
    for step in range(1, n_sp):
        pl.semaphore_signal(barrier, inc=1, device_id={"sp": (sp + step) % n_sp}, device_id_type=MESH)
    pl.semaphore_wait(barrier, n_tp + n_sp - 2)

    zm, zp, zo = (my_z + 3) % NY, (my_z + 1) % NY, (my_z + 2) % NY
    ym, yp, yo = (my_y + 3) % NY, (my_y + 1) % NY, (my_y + 2) % NY
    x_left, x_right, x_far = (my_x + 3) % NY, (my_x + 1) % NY, (my_x + 2) % NY
    partner = {"sp": 2 * my_x + 1 - my_c}
    sends = []
    n_sends = [0, 0]

    def x_copy(y_src, first, count, y_dst, slot):
        ref = xg.at[y_src, pl.ds(first * (rows // 2), count * (rows // 2))]
        return pltpu.make_async_remote_copy(src_ref=ref, dst_ref=ref, send_sem=x_send.at[slot], recv_sem=x_recv.at[y_src, first],
                                            device_id={"tp": NY * my_z + y_dst}, device_id_type=MESH)

    def x_put(y_src, first, count, y_dst):
        copy = x_copy(y_src, first, count, y_dst, n_sends[0])
        n_sends[0] += 1
        sends.append(copy)
        copy.start()

    def x_wait(y_src, first, count):
        x_copy(y_src, first, count, 0, 0).wait_recv()

    def w_copy(kind, z_src, x_src, first, count, dst, slot):
        size = d_rows if x_src is None else s_rows
        base = my_c * d_half + (0 if x_src is None else d_rows + x_src * s_rows)
        ref = (wq_v if kind else wkv_v).at[z_src, pl.ds(pl.multiple_of(base + first * (size // 2), 16), count * (size // 2))]
        return pltpu.make_async_remote_copy(src_ref=ref, dst_ref=ref, send_sem=w_send.at[slot],
                                            recv_sem=w_recv.at[kind, z_src, NY if x_src is None else x_src, first], device_id=dst, device_id_type=MESH)

    def w_put(kind, z_src, x_src, first, count, dst):
        copy = w_copy(kind, z_src, x_src, first, count, dst, n_sends[1])
        n_sends[1] += 1
        sends.append(copy)
        copy.start()

    def w_wait(kind, z_src, x_src, first, count):
        w_copy(kind, z_src, x_src, first, count, {"tp": 0}, 0).wait_recv()

    def to_z(z_dst):
        return {"tp": NY * z_dst + my_y}

    def to_x(x_dst):
        return {"sp": 2 * x_dst + my_c}

    def share_copy(kind, z_src, core, slot):
        ref = (wq_v if kind else wkv_v).at[z_src, pl.ds(pl.multiple_of(core * d_half, 64), d_half)]
        return pltpu.make_async_remote_copy(src_ref=ref, dst_ref=ref, send_sem=share_send.at[kind, slot], recv_sem=share_recv.at[kind, z_src],
                                            device_id=partner, device_id_type=MESH)

    def blk_of(z_idx):
        return jnp.where(z_idx < NY // 2, sp, 2 * n_sp - 1 - sp)

    def kv_rows(z_idx):
        return pl.multiple_of(blk_of(z_idx) * chunk + (z_idx % 2) * part, part)

    def own_products(y_list):
        def body(idx, carry):
            y_idx = y_list[0]
            for other in range(1, len(y_list)):
                y_idx = jnp.where(idx == other, y_list[other], y_idx)
            prod = jnp.dot(xg[y_idx], wkv_v[my_z], preferred_element_type=jnp.float32).astype(jnp.bfloat16)
            kv_v[pl.ds(pl.multiple_of(kv_rows(my_z) + y_idx * rows, rows), rows), :] = prod
            prod = jnp.dot(xg[y_idx], wq_v[my_z], preferred_element_type=jnp.float32).astype(jnp.bfloat16)
            q_v[pl.ds(pl.multiple_of(my_z * part + y_idx * rows, rows), rows), :] = prod
            return carry

        lax.fori_loop(0, len(y_list), body, 0)

    def a_copy(kind, z_src, z_dst, slot):
        if kind:
            src, dst = o_st.at[pl.ds(slot * part, part)], q_v.at[pl.ds(pl.multiple_of(z_src * part, part), part)]
        else:
            src, dst = kv_st.at[slot], kv_v.at[pl.ds(kv_rows(z_src), part)]
        return pltpu.make_async_remote_copy(src_ref=src, dst_ref=dst, send_sem=a_send.at[kind, slot], recv_sem=a_recv.at[kind, z_src],
                                            device_id=to_z(z_dst), device_id_type=MESH)

    def products(kind, z_dst, slot):
        def body(idx, carry):
            lhs = xg[pl.ds(2 * idx, 2)].reshape(2 * rows, xg.shape[2])
            prod = jnp.dot(lhs, (wq_v if kind else wkv_v)[z_dst], preferred_element_type=jnp.float32).astype(jnp.bfloat16)
            if kind:
                o_st[pl.ds(pl.multiple_of(slot * part + idx * 2 * rows, 2 * rows), 2 * rows), :] = prod
            else:
                kv_st[slot, pl.ds(pl.multiple_of(idx * 2 * rows, 2 * rows), 2 * rows), :] = prod
            return carry

        lax.fori_loop(0, 2, body, 0)

    def a_start(kind, z_dst, slot):
        a_copy(kind, my_z, z_dst, slot).start()

    def a_wait(kind, z_src):
        a_copy(kind, z_src, 0, 0).wait_recv()

    def kv_part(pair, core, z_idx, kind, dst):
        blk = jnp.where(pair < NY, 2 * pair + core, 2 * pair + 1 - core)
        ref = kv_v.at[pl.ds(pl.multiple_of(blk * chunk + (z_idx % 2) * part, part), part)]
        return pltpu.make_async_remote_copy(src_ref=ref, dst_ref=ref, send_sem=kv_send.at[z_idx, kind], recv_sem=kv_recv.at[blk, z_idx % 2],
                                            device_id=dst, device_id_type=MESH)

    def own_pair(z_idx):
        return jnp.where(z_idx < NY // 2, my_x, 2 * NY - 1 - my_x)

    def own_next(z_idx):
        low = z_idx < NY // 2
        return jnp.where(low, jnp.where(my_x < NY - 1, my_x + 1, NY - 2), my_x - 1), low | (my_x >= 1)

    def direct_in(z_idx):
        low = z_idx < NY // 2
        return jnp.where(low, my_x - 1, 2 * NY - 2 - my_x), (low & (my_x >= 1)) | (jnp.logical_not(low) & (my_x < NY - 1))

    def direct_next(z_idx):
        return jnp.where(z_idx < NY // 2, my_x + 1, my_x - 1), (my_x >= 1) & (my_x < NY - 1)

    def relay_in(z_idx):
        low = z_idx < NY // 2
        return jnp.where(low, my_x - 2, 2 * NY - 3 - my_x), (low & (my_x >= 2)) | (jnp.logical_not(low) & (my_x < NY - 2))

    def turn_in(z_idx):
        return NY - 1, (z_idx < NY // 2) & (my_x == NY - 2)

    def kv_own(z_idx, act):
        dst, wanted = own_next(z_idx)

        @pl.when(wanted)
        def _():
            act(kv_part(own_pair(z_idx), my_c, z_idx, 1, to_x(dst)))

        act(kv_part(own_pair(z_idx), my_c, z_idx, 0, partner))

    def kv_direct(z_idx, act, arrive):
        pair, wanted = direct_in(z_idx)

        @pl.when(wanted)
        def _():
            if arrive:
                kv_part(pair, my_c, z_idx, 2, partner).wait_recv()
            dst, more = direct_next(z_idx)

            @pl.when(more)
            def _():
                act(kv_part(pair, my_c, z_idx, 3, to_x(dst)))

            act(kv_part(pair, my_c, z_idx, 2, partner))

    def kv_relay(z_idx, act, arrive):
        for kind, (pair, wanted) in ((4, relay_in(z_idx)), (5, turn_in(z_idx))):
            @pl.when(wanted)
            def _(kind=kind, pair=pair):
                copy = kv_part(pair, my_c, z_idx, kind, partner)
                if arrive:
                    copy.wait_recv()
                act(copy)

    def kv_from_partner(z_idx):
        kv_part(own_pair(z_idx), 1 - my_c, z_idx, 0, partner).wait_recv()
        for pair, wanted in (direct_in(z_idx), relay_in(z_idx), turn_in(z_idx)):
            @pl.when(wanted)
            def _(pair=pair):
                kv_part(pair, 1 - my_c, z_idx, 0, partner).wait_recv()

    def start(copy):
        copy.start()

    def done(copy):
        copy.wait_send()

    group = 2 * (my_x % 2) + my_c
    x_group = 2 - 2 * (my_x % 2) + my_c

    def wo_copy(step):
        dst = (my_z + step) % NY
        src_ref = wo_hbm.at[group, :, pl.ds(pl.multiple_of(dst * cols, 128), cols)]
        return pltpu.make_async_remote_copy(src_ref=src_ref, dst_ref=wo_v.at[NY * my_y + my_z, group], send_sem=wo_send.at[step],
                                            recv_sem=wo_recv.at[my_z], device_id=to_z(dst), device_id_type=MESH)

    wo_own = pltpu.make_async_copy(wo_hbm.at[group, :, pl.ds(pl.multiple_of(my_z * cols, 128), cols)], wo_v.at[NY * my_y + my_z, group], wo_sem)

    def wo_z_start():
        wo_own.start()
        for step in range(1, NY):
            wo_copy(step).start()

    def wy_copy(y_src, first, count, y_dst, slot):
        ref = wo_v.at[pl.ds(NY * y_src + 2 * first, 2 * count), group]
        return pltpu.make_async_remote_copy(src_ref=ref, dst_ref=ref, send_sem=wy_send.at[slot], recv_sem=wy_recv.at[y_src, first],
                                            device_id={"tp": NY * my_z + y_dst}, device_id_type=MESH)

    wy_sends = (wy_copy(my_y, 0, 2, yp, 0), wy_copy(my_y, 0, 2, ym, 1), wy_copy(ym, 0, 1, yp, 2), wy_copy(yp, 1, 1, ym, 3))

    def wo_y_start():
        wo_own.wait()
        for z_src in (zm, zp, zo):
            ref = wo_v.at[NY * my_y + z_src, group]
            pltpu.make_async_remote_copy(src_ref=ref, dst_ref=ref, send_sem=wo_send.at[1], recv_sem=wo_recv.at[z_src],
                                         device_id=to_z(z_src), device_id_type=MESH).wait_recv()
        for copy in wy_sends[:2]:
            copy.start()

    def wo_y_pass():
        for y_src, copy in ((ym, wy_sends[2]), (yp, wy_sends[3])):
            wy_copy(y_src, 0, 2, 0, 0).wait_recv()
            copy.start()

    def slab_copy(grp, first, count, dst, slot):
        ref = wo_v.at[pl.ds(first * (n_tp // 2), count * (n_tp // 2)), grp]
        return pltpu.make_async_remote_copy(src_ref=ref, dst_ref=ref, send_sem=sl_send.at[slot], recv_sem=sl_recv.at[grp, first],
                                            device_id=dst, device_id_type=MESH)

    slabs = (slab_copy(group, 0, 1, to_x(x_right), 0), slab_copy(group, 1, 1, to_x(x_left), 1), slab_copy(group, 0, 2, partner, 2),
             slab_copy(x_group, 0, 2, partner, 3))

    def wo_first():
        for first in range(2):
            wy_copy(yo, first, 1, 0, 0).wait_recv()
        for copy in slabs[:3]:
            copy.start()

    def wo_second():
        for first in range(2):
            slab_copy(x_group, first, 1, partner, 3).wait_recv()
        slabs[3].start()

    def wo_last():
        for grp in (2 * (my_x % 2), 2 - 2 * (my_x % 2)):
            slab_copy(grp + 1 - my_c, 0, 2, partner, 3).wait_recv()

    def w_own_slice(kind):
        for z_dst in (zp, zm):
            w_put(kind, my_z, my_x, 0, 2, to_z(z_dst))

    def w_slices(kind):
        for z_src, first, z_dst in ((zm, 0, zp), (zp, 1, zm)):
            w_wait(kind, z_src, my_x, 0, 2)
            w_put(kind, z_src, my_x, first, 1, to_z(z_dst))
            for x_dst in (x_right, x_left):
                w_put(kind, z_src, my_x, 0, 2, to_x(x_dst))

    def w_own_rest(kind):
        for z_dst in (zp, zm):
            w_put(kind, my_z, None, 0, 2, to_z(z_dst))

    def w_far_slice(kind):
        for first in range(2):
            w_wait(kind, zo, my_x, first, 1)
        for x_dst in (x_right, x_left):
            w_put(kind, zo, my_x, 0, 2, to_x(x_dst))

    def w_ring(kind, z_src):
        for x_src, first, x_dst in ((x_left, 0, x_right), (x_right, 1, x_left)):
            w_wait(kind, z_src, x_src, 0, 2)
            w_put(kind, z_src, x_src, first, 1, to_x(x_dst))

    def w_rest(kind):
        for z_src, first, z_dst in ((zm, 0, zp), (zp, 1, zm)):
            w_wait(kind, z_src, None, 0, 2)
            w_put(kind, z_src, None, first, 1, to_z(z_dst))

    def w_share(kind, z_src, slot):
        for first in range(2):
            w_wait(kind, z_src, x_far, first, 1)
            if slot == 2:
                w_wait(kind, z_src, None, first, 1)
        share_copy(kind, z_src, my_c, slot).start()

    def w_full(kind, z_src, slot):
        share_copy(kind, z_src, 1 - my_c, slot).wait_recv()

    def split_heads():
        size = mx_v.shape[0]
        count = raw_v.shape[0] // size
        for part_idx in range(2):
            load = pltpu.make_async_copy(wq_hbm.at[pl.ds(part_idx * raw_v.shape[0], raw_v.shape[0])], raw_v, wl_sem.at[2])
            if part_idx:
                load.start()
            load.wait()

            def body(idx, carry, part_idx=part_idx):
                mx_v[...] = raw_v[pl.ds(pl.multiple_of(idx * size, size), size), :].astype(jnp.float32)
                at = pl.ds(pl.multiple_of((part_idx * count + idx) * (size // 2), size // 2), size // 2)
                for sub in range(2):
                    wq_v[my_z, at, sub * head:(sub + 1) * head] = mx_v[pl.ds(sub, size // 2, stride=2), :].astype(jnp.bfloat16)
                return carry

            lax.fori_loop(0, count, body, 0)

    x_load.wait()
    x_put(my_y, 0, 2, yp)
    x_put(my_y, 0, 2, ym)
    for load in w_loads[:2]:
        load.wait()
    w_own_slice(0)
    w_slices(0)
    w_own_rest(0)
    wo_z_start()
    split_heads()
    w_own_slice(1)
    w_far_slice(0)
    own_products([my_y])
    w_ring(0, zm)
    w_ring(0, zp)
    w_rest(0)
    w_ring(0, zo)
    w_slices(1)
    w_own_rest(1)
    for y_src, first, y_dst in ((ym, 0, yp), (yp, 1, ym)):
        x_wait(y_src, 0, 2)
        x_put(y_src, first, 1, y_dst)
    w_share(0, zm, 0)
    w_share(0, zp, 1)
    w_far_slice(1)
    own_products([ym, yp])
    w_share(0, zo, 2)
    w_ring(1, zm)
    w_ring(1, zp)
    for first in range(2):
        x_wait(yo, first, 1)
    own_products([yo])
    kv_own(my_z, start)
    for slot, z_dst in enumerate((zm, zp, zo)):
        w_full(0, z_dst, slot)
        products(0, z_dst, slot)
        a_start(0, z_dst, slot)
    w_rest(1)
    w_ring(1, zo)
    wo_y_start()
    kv_direct(my_z, start, True)
    for z_src in (zm, zp, zo):
        a_wait(0, z_src)
        kv_own(z_src, start)
    for slot, z_src in enumerate((zm, zp, zo)):
        w_share(1, z_src, slot)
    kv_relay(my_z, start, True)
    for slot, z_dst in enumerate((zm, zp, zo)):
        w_full(1, z_dst, slot)
        products(1, z_dst, slot)
        a_start(1, z_dst, slot)
        kv_direct(z_dst, start, True)
        if slot == 0:
            wo_y_pass()
    for z_src in (zm, zp, zo):
        kv_relay(z_src, start, True)
    wo_first()
    for z_src in (zm, zp, zo):
        a_wait(1, z_src)
    for slot in range(3):
        a_copy(1, my_z, 0, slot).wait_send()
    for z_idx in range(NY):
        kv_from_partner(z_idx)

    row_i = lax.broadcasted_iota(jnp.int32, (2 * TQ, TQ), 0) % TQ
    col_i = lax.broadcasted_iota(jnp.int32, (2 * TQ, TQ), 1)

    def lane_max(scores):
        best = scores[:, 0:head]
        for idx in range(1, scores.shape[1] // head):
            best = jnp.maximum(best, scores[:, idx * head:(idx + 1) * head])
        return best

    def o_copy(tile, z_dst):
        y_dst, z_row = tile % NY, tile // NY
        src = o_st.at[pl.ds(pl.multiple_of(tile * rows, rows), rows)]
        dst = og.at[z_row, tp]
        return pltpu.make_async_remote_copy(src_ref=src, dst_ref=dst, send_sem=o_send.at[tile, z_dst], recv_sem=o_recv.at[z_row, tp],
                                            device_id={"tp": NY * z_dst + y_dst}, device_id_type=MESH)

    def o_arrival(z_row, src):
        dst = og.at[z_row, src]
        return pltpu.make_async_remote_copy(src_ref=o_st.at[pl.ds(0, rows)], dst_ref=dst, send_sem=o_send.at[0, 0],
                                            recv_sem=o_recv.at[z_row, src], device_id={"tp": 0}, device_id_type=MESH)

    def attend(q_idx, gidx, start_tile, n_wide, n_narrow, with_first):
        q_blk = q_v[pl.ds(pl.multiple_of(q_idx * TQ, TQ), TQ), :]
        q_two = jnp.concatenate([q_blk[:, :head], q_blk[:, head:]], axis=0)

        def keys(tile, width):
            return kv_v[pl.ds(pl.multiple_of(tile * TQ, TQ), width), 0:head]

        def values(tile, width):
            return kv_v[pl.ds(pl.multiple_of(tile * TQ, TQ), width), head:2 * head]

        per = WIDE // TQ
        scores = jnp.where(col_i <= row_i, dot_nt(q_two, keys(gidx, TQ)) * coef, NEG_BIG)
        s_v[:, 0:TQ] = scores
        best = lane_max(scores)
        if with_first:
            scores = jnp.where(col_i > row_i, dot_nt(q_two, keys(gidx - WINDOW // TQ, TQ)) * coef, NEG_BIG)
            s_v[:, TQ:2 * TQ] = scores
            best = jnp.maximum(best, lane_max(scores))
        mx_v[...] = best

        def score_step(tile, width):
            part = dot_nt(q_two, keys(start_tile + tile, width)) * coef
            s_v[:, pl.ds(pl.multiple_of((2 + tile) * TQ, TQ), width)] = part
            mx_v[...] = jnp.maximum(mx_v[...], lane_max(part))

        def each_step(step):
            def wide_step(idx, carry):
                step(per * idx, WIDE)
                return carry

            def narrow_step(idx, carry):
                step(per * n_wide + idx, TQ)
                return carry

            lax.fori_loop(0, n_wide, wide_step, 0)
            if n_narrow is not None:
                lax.fori_loop(0, n_narrow, narrow_step, 0)

        each_step(score_step)
        row_best = jnp.max(mx_v[...], axis=1, keepdims=True)
        mb_v[...] = jnp.broadcast_to(row_best, mb_v.shape)

        def probs(col, width):
            base = mb_v[...]
            total = None
            parts = []
            for idx in range(width // head):
                part = jnp.exp2(s_v[:, pl.ds(pl.multiple_of(col + idx * head, head), head)] - base)
                total = part if total is None else total + part
                parts.append(part.astype(jnp.bfloat16))
            return jnp.concatenate(parts, axis=1), total

        prob, total = probs(0, TQ)
        acc = jnp.dot(prob, values(gidx, TQ), preferred_element_type=jnp.float32)
        if with_first:
            prob, total_b = probs(TQ, TQ)
            total = total + total_b
            acc = acc + jnp.dot(prob, values(gidx - WINDOW // TQ, TQ), preferred_element_type=jnp.float32)
        l_v[...] = total
        acc_v[...] = acc

        def value_step(tile, width):
            prob, total = probs((2 + tile) * TQ, width)
            l_v[...] += total
            acc_v[...] += jnp.dot(prob, values(start_tile + tile, width), preferred_element_type=jnp.float32)

        each_step(value_step)
        denom = jnp.sum(l_v[...], axis=1, keepdims=True)
        out = (acc_v[...] / denom).astype(jnp.bfloat16)
        out = jnp.concatenate([out[:TQ], out[TQ:]], axis=1)
        o_st[pl.ds(pl.multiple_of(q_idx * TQ, TQ), TQ), :] = out

    def y_copy(z_dst, z_src):
        return pltpu.make_async_remote_copy(
            src_ref=yst.at[z_dst], dst_ref=y_hbm.at[:, pl.ds(pl.multiple_of(z_src * cols, 128), cols)],
            send_sem=y_send.at[z_dst], recv_sem=y_recv.at[z_src], device_id={"tp": NY * z_dst + my_y}, device_id_type=MESH)

    y_own = pltpu.make_async_copy(yst.at[my_z], y_hbm.at[:, pl.ds(pl.multiple_of(my_z * cols, 128), cols)], y_sem)

    def out_product(first, count):
        for row in range(first, first + count):
            for src in range(n_tp):
                @pl.when(tp != src)
                def _(row=row, src=src):
                    o_arrival(row, src).wait_recv()
        lhs = jnp.concatenate([og[first:first + count, src].reshape(count * rows, 2 * head) for src in range(n_tp)], axis=1)
        for col in range(0, cols, 384):
            w_cols = jnp.concatenate([wo_v[NY * y_idx + z_idx, :, :, col:col + 384].reshape(2 * head, 384)
                                      for z_idx in range(NY) for y_idx in range(NY)], axis=0)
            res = jnp.dot(lhs, w_cols, preferred_element_type=jnp.float32).astype(jnp.bfloat16)
            yst[first:first + count, :, col:col + 384] = res.reshape(count, rows, 384)

    def y_put(first, count):
        for z_dst in range(first, first + count):
            @pl.when(my_z != z_dst)
            def _(z_dst=z_dst):
                y_copy(z_dst, my_z).start()

            @pl.when(my_z == z_dst)
            def _(z_dst=z_dst):
                y_own.start()

    def q_step(q_idx, carry):
        tiles = chunk // TQ
        blk = jnp.where(q_idx < tiles, sp, 2 * n_sp - 1 - sp)
        gidx = blk * tiles + q_idx % tiles

        @pl.when(gidx >= WINDOW // TQ)
        def _():
            attend(q_idx, gidx, gidx - WINDOW // TQ + 1, N_WIDE, None, True)

        @pl.when(gidx < WINDOW // TQ)
        def _():
            attend(q_idx, gidx, 0, gidx // (WIDE // TQ), gidx % (WIDE // TQ), False)

        for sub in range(2):
            tile = 2 * q_idx + sub

            for z_dst in range(NY):
                mine = (tile % NY == my_y) & (my_z == z_dst)

                @pl.when(jnp.logical_not(mine))
                def _(tile=tile, z_dst=z_dst):
                    o_copy(tile, z_dst).start()

            @pl.when(tile % NY == my_y)
            def _(tile=tile):
                og[tile // NY, tp] = o_st[pl.ds(pl.multiple_of(tile * rows, rows), rows), :]

        @pl.when(q_idx == 5)
        def _():
            wo_second()

        return carry

    lax.fori_loop(0, 2 * chunk // TQ, q_step, 0)

    wo_last()
    out_product(0, 2)
    y_put(0, 2)
    out_product(2, 1)
    y_put(2, 1)
    out_product(3, 1)
    y_put(3, 1)
    for z_src in range(NY):
        @pl.when(my_z != z_src)
        def _(z_src=z_src):
            y_copy(z_src, z_src).wait_recv()
    for tile in range(n_tp):
        for z_dst in range(NY):
            mine = (tile % NY == my_y) & (my_z == z_dst)

            @pl.when(jnp.logical_not(mine))
            def _(tile=tile, z_dst=z_dst):
                o_copy(tile, z_dst).wait_send()
    for z_dst in range(NY):
        @pl.when(my_z != z_dst)
        def _(z_dst=z_dst):
            y_copy(z_dst, my_z).wait_send()
    for copy in sends + list(slabs):
        copy.wait_send()
    for step in range(1, NY):
        wo_copy(step).wait_send()
    for copy in wy_sends:
        copy.wait_send()
    for slot in range(3):
        for kind in range(2):
            share_copy(kind, my_z, my_c, slot).wait_send()
    for slot in range(3):
        a_copy(0, my_z, 0, slot).wait_send()
    for z_idx in range(NY):
        kv_own(z_idx, done)
        kv_direct(z_idx, done, False)
        kv_relay(z_idx, done, False)
    y_own.wait()


def solution(mesh):
    n_sp, n_tp = mesh.shape["sp"], mesh.shape["tp"]

    def local_attn(x_part, w_query, w_key, w_value, w_out):
        rows, d_model = x_part.shape
        heads_loc, head = w_query.shape[1], w_query.shape[2]
        two_head = heads_loc * head
        seq_loc = rows * n_tp
        cols = d_model // NY
        any_spec = pl.BlockSpec(memory_space=pl.ANY)
        dma = pltpu.SemaphoreType.DMA
        bf16, f32 = jnp.bfloat16, jnp.float32
        wo_rows = w_out.shape[0] * w_out.shape[1] // NY
        return pl.pallas_call(
            layer_kernel,
            out_shape=jax.ShapeDtypeStruct((rows, d_model), bf16),
            in_specs=[any_spec] * 5,
            out_specs=any_spec,
            scratch_shapes=[
                pltpu.VMEM((NY, rows, d_model), bf16),
                pltpu.VMEM((NY, d_model, two_head), bf16),
                pltpu.VMEM((NY, d_model, two_head), bf16),
                pltpu.VMEM((seq_loc, two_head), bf16),
                pltpu.VMEM((n_sp * seq_loc, two_head), bf16),
                pltpu.VMEM((NY - 1, seq_loc // NY, two_head), bf16),
                pltpu.VMEM((n_tp, NY, wo_rows, cols), bf16),
                pltpu.VMEM((2 * TQ, WINDOW + TQ), f32),
                pltpu.VMEM((2 * TQ, head), f32),
                pltpu.VMEM((2 * TQ, head), f32),
                pltpu.VMEM((2 * TQ, head), f32),
                pltpu.VMEM((2 * TQ, head), f32),
                pltpu.VMEM((seq_loc, two_head), bf16),
                pltpu.VMEM((NY, n_tp, rows, two_head), bf16),
                pltpu.VMEM((NY, rows, cols), bf16),
                pltpu.VMEM((d_model, head), bf16),
                dma, dma((3,)), dma((4,)), dma((NY, 2)), dma((40,)), dma((2, NY, NY + 1, 2)), dma((2, 3)), dma((2, NY)), dma((2, 3)), dma((2, NY)),
                dma((NY, 6)), dma((2 * n_sp, 2)), dma, dma((NY,)), dma((NY,)), dma((4,)), dma((NY, 2)), dma((4,)), dma((NY, 2)),
                dma((n_tp, NY)), dma((NY, n_tp)), dma((NY,)), dma((NY,)), dma,
            ],
            compiler_params=pltpu.CompilerParams(collective_id=1, has_side_effects=True, vmem_limit_bytes=67043328),
            name="layer",
        )(x_part, w_query.reshape(heads_loc * d_model, head), w_key.reshape(d_model, head), w_value.reshape(d_model, head),
          w_out.reshape(NY, wo_rows, d_model))

    return jax.shard_map(local_attn, mesh=mesh, in_specs=(P(("dp", "sp", "tp"), None), P(None, "tp", None), P(None, "tp", None), P(None, "tp", None), P("tp", None, None)), out_specs=P(("dp", "sp", "tp"), None), check_vma=False)
```

```python
import functools

import jax
import jax.numpy as jnp
from jax import lax
from jax.experimental import pallas as pl
from jax.experimental.pallas import tpu as pltpu
from jax.sharding import PartitionSpec as P

WINDOW = 4096
NEG_BIG = -1e30
LOG2E = 1.4426950408889634
MESH = pl.DeviceIdType.MESH
NY = 4
TQ = 256
WIDE = 1280
N_WIDE = (WINDOW - TQ) // WIDE


def dot_nt(lhs, rhs):
    return lax.dot_general(lhs, rhs, (((1,), (1,)), ((), ())), preferred_element_type=jnp.float32)


def layer_kernel(x_hbm, wq_hbm, wk_hbm, wv_hbm, wo_hbm, y_hbm, xg, wq_v, wkv_v, q_v, kv_v, kv_st, wo_v, s_v, mx_v, mb_v, l_v, acc_v, o_st,
                 og, yst, raw_v, x_sem, wl_sem, x_send, x_recv, w_send, w_recv, share_send, share_recv, a_send, a_recv,
                 kv_send, kv_recv, wo_sem, wo_send, wo_recv, wy_send, wy_recv, sl_send, sl_recv, o_send, o_recv,
                 y_send, y_recv, y_sem):
    sp = lax.axis_index("sp")
    tp = lax.axis_index("tp")
    my_z, my_y = tp // NY, tp % NY
    my_x, my_c = sp // 2, sp % 2
    n_tp = NY * NY
    n_sp = 8
    chunk = kv_v.shape[0] // (2 * n_sp)
    head = kv_v.shape[1] // 2
    cols = yst.shape[2]
    rows = yst.shape[1]
    part = NY * rows
    coef = head ** -0.5 * LOG2E
    d_half = wq_v.shape[1] // 2
    s_rows = d_half // (6 * 32) * 32 - 32
    d_rows = d_half - NY * s_rows

    x_load = pltpu.make_async_copy(x_hbm, xg.at[my_y], x_sem)
    x_load.start()
    w_loads = (pltpu.make_async_copy(wk_hbm, wkv_v.at[my_z, :, 0:head], wl_sem.at[0]),
               pltpu.make_async_copy(wv_hbm, wkv_v.at[my_z, :, head:2 * head], wl_sem.at[1]),
               pltpu.make_async_copy(wq_hbm.at[pl.ds(0, raw_v.shape[0])], raw_v, wl_sem.at[2]))
    for load in w_loads:
        load.start()

    barrier = pltpu.get_barrier_semaphore()
    for step in range(1, n_tp):
        pl.semaphore_signal(barrier, inc=1, device_id={"tp": (tp + step) % n_tp}, device_id_type=MESH)
    for step in range(1, n_sp):
        pl.semaphore_signal(barrier, inc=1, device_id={"sp": (sp + step) % n_sp}, device_id_type=MESH)
    pl.semaphore_wait(barrier, n_tp + n_sp - 2)

    zm, zp, zo = (my_z + 3) % NY, (my_z + 1) % NY, (my_z + 2) % NY
    ym, yp, yo = (my_y + 3) % NY, (my_y + 1) % NY, (my_y + 2) % NY
    x_left, x_right, x_far = (my_x + 3) % NY, (my_x + 1) % NY, (my_x + 2) % NY
    partner = {"sp": 2 * my_x + 1 - my_c}
    sends = []
    n_sends = [0, 0]

    def x_copy(y_src, first, count, y_dst, slot):
        ref = xg.at[y_src, pl.ds(first * (rows // 2), count * (rows // 2))]
        return pltpu.make_async_remote_copy(src_ref=ref, dst_ref=ref, send_sem=x_send.at[slot], recv_sem=x_recv.at[y_src, first],
                                            device_id={"tp": NY * my_z + y_dst}, device_id_type=MESH)

    def x_put(y_src, first, count, y_dst):
        copy = x_copy(y_src, first, count, y_dst, n_sends[0])
        n_sends[0] += 1
        sends.append(copy)
        copy.start()

    def x_wait(y_src, first, count):
        x_copy(y_src, first, count, 0, 0).wait_recv()

    def w_copy(kind, z_src, x_src, first, count, dst, slot):
        size = d_rows if x_src is None else s_rows
        base = my_c * d_half + (0 if x_src is None else d_rows + x_src * s_rows)
        ref = (wq_v if kind else wkv_v).at[z_src, pl.ds(pl.multiple_of(base + first * (size // 2), 16), count * (size // 2))]
        return pltpu.make_async_remote_copy(src_ref=ref, dst_ref=ref, send_sem=w_send.at[slot],
                                            recv_sem=w_recv.at[kind, z_src, NY if x_src is None else x_src, first], device_id=dst, device_id_type=MESH)

    def w_put(kind, z_src, x_src, first, count, dst):
        copy = w_copy(kind, z_src, x_src, first, count, dst, n_sends[1])
        n_sends[1] += 1
        sends.append(copy)
        copy.start()

    def w_wait(kind, z_src, x_src, first, count):
        w_copy(kind, z_src, x_src, first, count, {"tp": 0}, 0).wait_recv()

    def to_z(z_dst):
        return {"tp": NY * z_dst + my_y}

    def to_x(x_dst):
        return {"sp": 2 * x_dst + my_c}

    def share_copy(kind, z_src, core, slot):
        ref = (wq_v if kind else wkv_v).at[z_src, pl.ds(pl.multiple_of(core * d_half, 64), d_half)]
        return pltpu.make_async_remote_copy(src_ref=ref, dst_ref=ref, send_sem=share_send.at[kind, slot], recv_sem=share_recv.at[kind, z_src],
                                            device_id=partner, device_id_type=MESH)

    def blk_of(z_idx):
        return jnp.where(z_idx < NY // 2, sp, 2 * n_sp - 1 - sp)

    def kv_rows(z_idx):
        return pl.multiple_of(blk_of(z_idx) * chunk + (z_idx % 2) * part, part)

    def own_products(y_list):
        def body(idx, carry):
            y_idx = y_list[0]
            for other in range(1, len(y_list)):
                y_idx = jnp.where(idx == other, y_list[other], y_idx)
            prod = jnp.dot(xg[y_idx], wkv_v[my_z], preferred_element_type=jnp.float32).astype(jnp.bfloat16)
            kv_v[pl.ds(pl.multiple_of(kv_rows(my_z) + y_idx * rows, rows), rows), :] = prod
            prod = jnp.dot(xg[y_idx], wq_v[my_z], preferred_element_type=jnp.float32).astype(jnp.bfloat16)
            q_v[pl.ds(pl.multiple_of(my_z * part + y_idx * rows, rows), rows), :] = prod
            return carry

        lax.fori_loop(0, len(y_list), body, 0)

    def a_copy(kind, z_src, z_dst, slot):
        if kind:
            src, dst = o_st.at[pl.ds(slot * part, part)], q_v.at[pl.ds(pl.multiple_of(z_src * part, part), part)]
        else:
            src, dst = kv_st.at[slot], kv_v.at[pl.ds(kv_rows(z_src), part)]
        return pltpu.make_async_remote_copy(src_ref=src, dst_ref=dst, send_sem=a_send.at[kind, slot], recv_sem=a_recv.at[kind, z_src],
                                            device_id=to_z(z_dst), device_id_type=MESH)

    def products(kind, z_dst, slot):
        def body(idx, carry):
            lhs = xg[pl.ds(2 * idx, 2)].reshape(2 * rows, xg.shape[2])
            prod = jnp.dot(lhs, (wq_v if kind else wkv_v)[z_dst], preferred_element_type=jnp.float32).astype(jnp.bfloat16)
            if kind:
                o_st[pl.ds(pl.multiple_of(slot * part + idx * 2 * rows, 2 * rows), 2 * rows), :] = prod
            else:
                kv_st[slot, pl.ds(pl.multiple_of(idx * 2 * rows, 2 * rows), 2 * rows), :] = prod
            return carry

        lax.fori_loop(0, 2, body, 0)

    def a_start(kind, z_dst, slot):
        a_copy(kind, my_z, z_dst, slot).start()

    def a_wait(kind, z_src):
        a_copy(kind, z_src, 0, 0).wait_recv()

    def kv_part(pair, core, z_idx, kind, dst):
        blk = jnp.where(pair < NY, 2 * pair + core, 2 * pair + 1 - core)
        ref = kv_v.at[pl.ds(pl.multiple_of(blk * chunk + (z_idx % 2) * part, part), part)]
        return pltpu.make_async_remote_copy(src_ref=ref, dst_ref=ref, send_sem=kv_send.at[z_idx, kind], recv_sem=kv_recv.at[blk, z_idx % 2],
                                            device_id=dst, device_id_type=MESH)

    def own_pair(z_idx):
        return jnp.where(z_idx < NY // 2, my_x, 2 * NY - 1 - my_x)

    def own_next(z_idx):
        low = z_idx < NY // 2
        return jnp.where(low, jnp.where(my_x < NY - 1, my_x + 1, NY - 2), my_x - 1), low | (my_x >= 1)

    def direct_in(z_idx):
        low = z_idx < NY // 2
        return jnp.where(low, my_x - 1, 2 * NY - 2 - my_x), (low & (my_x >= 1)) | (jnp.logical_not(low) & (my_x < NY - 1))

    def direct_next(z_idx):
        return jnp.where(z_idx < NY // 2, my_x + 1, my_x - 1), (my_x >= 1) & (my_x < NY - 1)

    def relay_in(z_idx):
        low = z_idx < NY // 2
        return jnp.where(low, my_x - 2, 2 * NY - 3 - my_x), (low & (my_x >= 2)) | (jnp.logical_not(low) & (my_x < NY - 2))

    def turn_in(z_idx):
        return NY - 1, (z_idx < NY // 2) & (my_x == NY - 2)

    def kv_own(z_idx, act):
        dst, wanted = own_next(z_idx)

        @pl.when(wanted)
        def _():
            act(kv_part(own_pair(z_idx), my_c, z_idx, 1, to_x(dst)))

        act(kv_part(own_pair(z_idx), my_c, z_idx, 0, partner))

    def kv_direct(z_idx, act, arrive):
        pair, wanted = direct_in(z_idx)

        @pl.when(wanted)
        def _():
            if arrive:
                kv_part(pair, my_c, z_idx, 2, partner).wait_recv()
            dst, more = direct_next(z_idx)

            @pl.when(more)
            def _():
                act(kv_part(pair, my_c, z_idx, 3, to_x(dst)))

            act(kv_part(pair, my_c, z_idx, 2, partner))

    def kv_relay(z_idx, act, arrive):
        for kind, (pair, wanted) in ((4, relay_in(z_idx)), (5, turn_in(z_idx))):
            @pl.when(wanted)
            def _(kind=kind, pair=pair):
                copy = kv_part(pair, my_c, z_idx, kind, partner)
                if arrive:
                    copy.wait_recv()
                act(copy)

    def kv_from_partner(z_idx):
        kv_part(own_pair(z_idx), 1 - my_c, z_idx, 0, partner).wait_recv()
        for pair, wanted in (direct_in(z_idx), relay_in(z_idx), turn_in(z_idx)):
            @pl.when(wanted)
            def _(pair=pair):
                kv_part(pair, 1 - my_c, z_idx, 0, partner).wait_recv()

    def start(copy):
        copy.start()

    def done(copy):
        copy.wait_send()

    group = 2 * (my_x % 2) + my_c
    x_group = 2 - 2 * (my_x % 2) + my_c

    def wo_copy(step):
        dst = (my_z + step) % NY
        src_ref = wo_hbm.at[group, :, pl.ds(pl.multiple_of(dst * cols, 128), cols)]
        return pltpu.make_async_remote_copy(src_ref=src_ref, dst_ref=wo_v.at[NY * my_y + my_z, group], send_sem=wo_send.at[step],
                                            recv_sem=wo_recv.at[my_z], device_id=to_z(dst), device_id_type=MESH)

    wo_own = pltpu.make_async_copy(wo_hbm.at[group, :, pl.ds(pl.multiple_of(my_z * cols, 128), cols)], wo_v.at[NY * my_y + my_z, group], wo_sem)

    def wo_z_start():
        wo_own.start()
        for step in range(1, NY):
            wo_copy(step).start()

    def wy_copy(y_src, first, count, y_dst, slot):
        ref = wo_v.at[pl.ds(NY * y_src + 2 * first, 2 * count), group]
        return pltpu.make_async_remote_copy(src_ref=ref, dst_ref=ref, send_sem=wy_send.at[slot], recv_sem=wy_recv.at[y_src, first],
                                            device_id={"tp": NY * my_z + y_dst}, device_id_type=MESH)

    wy_sends = (wy_copy(my_y, 0, 2, yp, 0), wy_copy(my_y, 0, 2, ym, 1), wy_copy(ym, 0, 1, yp, 2), wy_copy(yp, 1, 1, ym, 3))

    def wo_y_start():
        wo_own.wait()
        for z_src in (zm, zp, zo):
            ref = wo_v.at[NY * my_y + z_src, group]
            pltpu.make_async_remote_copy(src_ref=ref, dst_ref=ref, send_sem=wo_send.at[1], recv_sem=wo_recv.at[z_src],
                                         device_id=to_z(z_src), device_id_type=MESH).wait_recv()
        for copy in wy_sends[:2]:
            copy.start()

    def wo_y_pass():
        for y_src, copy in ((ym, wy_sends[2]), (yp, wy_sends[3])):
            wy_copy(y_src, 0, 2, 0, 0).wait_recv()
            copy.start()

    def slab_copy(grp, first, count, dst, slot):
        ref = wo_v.at[pl.ds(first * (n_tp // 2), count * (n_tp // 2)), grp]
        return pltpu.make_async_remote_copy(src_ref=ref, dst_ref=ref, send_sem=sl_send.at[slot], recv_sem=sl_recv.at[grp, first],
                                            device_id=dst, device_id_type=MESH)

    slabs = (slab_copy(group, 0, 1, to_x(x_right), 0), slab_copy(group, 1, 1, to_x(x_left), 1), slab_copy(group, 0, 2, partner, 2),
             slab_copy(x_group, 0, 2, partner, 3))

    def wo_first():
        for first in range(2):
            wy_copy(yo, first, 1, 0, 0).wait_recv()
        for copy in slabs[:3]:
            copy.start()

    def wo_second():
        for first in range(2):
            slab_copy(x_group, first, 1, partner, 3).wait_recv()
        slabs[3].start()

    def wo_last():
        for grp in (2 * (my_x % 2), 2 - 2 * (my_x % 2)):
            slab_copy(grp + 1 - my_c, 0, 2, partner, 3).wait_recv()

    def w_own_slice(kind):
        for z_dst in (zp, zm):
            w_put(kind, my_z, my_x, 0, 2, to_z(z_dst))

    def w_slices(kind):
        for z_src, first, z_dst in ((zm, 0, zp), (zp, 1, zm)):
            w_wait(kind, z_src, my_x, 0, 2)
            w_put(kind, z_src, my_x, first, 1, to_z(z_dst))
            for x_dst in (x_right, x_left):
                w_put(kind, z_src, my_x, 0, 2, to_x(x_dst))

    def w_own_rest(kind):
        for z_dst in (zp, zm):
            w_put(kind, my_z, None, 0, 2, to_z(z_dst))

    def w_far_slice(kind):
        for first in range(2):
            w_wait(kind, zo, my_x, first, 1)
        for x_dst in (x_right, x_left):
            w_put(kind, zo, my_x, 0, 2, to_x(x_dst))

    def w_ring(kind, z_src):
        for x_src, first, x_dst in ((x_left, 0, x_right), (x_right, 1, x_left)):
            w_wait(kind, z_src, x_src, 0, 2)
            w_put(kind, z_src, x_src, first, 1, to_x(x_dst))

    def w_rest(kind):
        for z_src, first, z_dst in ((zm, 0, zp), (zp, 1, zm)):
            w_wait(kind, z_src, None, 0, 2)
            w_put(kind, z_src, None, first, 1, to_z(z_dst))

    def w_share(kind, z_src, slot):
        for first in range(2):
            w_wait(kind, z_src, x_far, first, 1)
            if slot == 2:
                w_wait(kind, z_src, None, first, 1)
        share_copy(kind, z_src, my_c, slot).start()

    def w_full(kind, z_src, slot):
        share_copy(kind, z_src, 1 - my_c, slot).wait_recv()

    def split_heads():
        size = mx_v.shape[0]
        count = raw_v.shape[0] // size
        for part_idx in range(2):
            load = pltpu.make_async_copy(wq_hbm.at[pl.ds(part_idx * raw_v.shape[0], raw_v.shape[0])], raw_v, wl_sem.at[2])
            if part_idx:
                load.start()
            load.wait()

            def body(idx, carry, part_idx=part_idx):
                mx_v[...] = raw_v[pl.ds(pl.multiple_of(idx * size, size), size), :].astype(jnp.float32)
                at = pl.ds(pl.multiple_of((part_idx * count + idx) * (size // 2), size // 2), size // 2)
                for sub in range(2):
                    wq_v[my_z, at, sub * head:(sub + 1) * head] = mx_v[pl.ds(sub, size // 2, stride=2), :].astype(jnp.bfloat16)
                return carry

            lax.fori_loop(0, count, body, 0)

    x_load.wait()
    x_put(my_y, 0, 2, yp)
    x_put(my_y, 0, 2, ym)
    for load in w_loads[:2]:
        load.wait()
    w_own_slice(0)
    w_slices(0)
    w_own_rest(0)
    wo_z_start()
    split_heads()
    w_own_slice(1)
    w_far_slice(0)
    own_products([my_y])
    w_ring(0, zm)
    w_ring(0, zp)
    w_rest(0)
    w_ring(0, zo)
    w_slices(1)
    w_own_rest(1)
    for y_src, first, y_dst in ((ym, 0, yp), (yp, 1, ym)):
        x_wait(y_src, 0, 2)
        x_put(y_src, first, 1, y_dst)
    w_share(0, zm, 0)
    w_share(0, zp, 1)
    w_far_slice(1)
    own_products([ym, yp])
    w_share(0, zo, 2)
    w_ring(1, zm)
    w_ring(1, zp)
    for first in range(2):
        x_wait(yo, first, 1)
    own_products([yo])
    kv_own(my_z, start)
    for slot, z_dst in enumerate((zm, zp, zo)):
        w_full(0, z_dst, slot)
        products(0, z_dst, slot)
        a_start(0, z_dst, slot)
    w_rest(1)
    w_ring(1, zo)
    wo_y_start()
    kv_direct(my_z, start, True)
    for z_src in (zm, zp, zo):
        a_wait(0, z_src)
        kv_own(z_src, start)
    for slot, z_src in enumerate((zm, zp, zo)):
        w_share(1, z_src, slot)
    kv_relay(my_z, start, True)
    for slot, z_dst in enumerate((zm, zp, zo)):
        w_full(1, z_dst, slot)
        products(1, z_dst, slot)
        a_start(1, z_dst, slot)
        kv_direct(z_dst, start, True)
        if slot == 0:
            wo_y_pass()
    for z_src in (zm, zp, zo):
        kv_relay(z_src, start, True)
    wo_first()
    for z_src in (zm, zp, zo):
        a_wait(1, z_src)
    for slot in range(3):
        a_copy(1, my_z, 0, slot).wait_send()
    for z_idx in range(NY):
        kv_from_partner(z_idx)

    row_i = lax.broadcasted_iota(jnp.int32, (2 * TQ, TQ), 0) % TQ
    col_i = lax.broadcasted_iota(jnp.int32, (2 * TQ, TQ), 1)

    def lane_max(scores):
        best = scores[:, 0:head]
        for idx in range(1, scores.shape[1] // head):
            best = jnp.maximum(best, scores[:, idx * head:(idx + 1) * head])
        return best

    def o_copy(tile, z_dst):
        y_dst, z_row = tile % NY, tile // NY
        src = o_st.at[pl.ds(pl.multiple_of(tile * rows, rows), rows)]
        dst = og.at[z_row, tp]
        return pltpu.make_async_remote_copy(src_ref=src, dst_ref=dst, send_sem=o_send.at[tile, z_dst], recv_sem=o_recv.at[z_row, tp],
                                            device_id={"tp": NY * z_dst + y_dst}, device_id_type=MESH)

    def o_arrival(z_row, src):
        dst = og.at[z_row, src]
        return pltpu.make_async_remote_copy(src_ref=o_st.at[pl.ds(0, rows)], dst_ref=dst, send_sem=o_send.at[0, 0],
                                            recv_sem=o_recv.at[z_row, src], device_id={"tp": 0}, device_id_type=MESH)

    def attend(q_idx, gidx, start_tile, n_wide, n_narrow, with_first):
        q_blk = q_v[pl.ds(pl.multiple_of(q_idx * TQ, TQ), TQ), :]
        q_two = jnp.concatenate([q_blk[:, :head], q_blk[:, head:]], axis=0)

        def keys(tile, width):
            return kv_v[pl.ds(pl.multiple_of(tile * TQ, TQ), width), 0:head]

        def values(tile, width):
            return kv_v[pl.ds(pl.multiple_of(tile * TQ, TQ), width), head:2 * head]

        per = WIDE // TQ
        scores = jnp.where(col_i <= row_i, dot_nt(q_two, keys(gidx, TQ)) * coef, NEG_BIG)
        s_v[:, 0:TQ] = scores
        best = lane_max(scores)
        if with_first:
            scores = jnp.where(col_i > row_i, dot_nt(q_two, keys(gidx - WINDOW // TQ, TQ)) * coef, NEG_BIG)
            s_v[:, TQ:2 * TQ] = scores
            best = jnp.maximum(best, lane_max(scores))
        mx_v[...] = best

        def score_step(tile, width):
            part = dot_nt(q_two, keys(start_tile + tile, width)) * coef
            s_v[:, pl.ds(pl.multiple_of((2 + tile) * TQ, TQ), width)] = part
            mx_v[...] = jnp.maximum(mx_v[...], lane_max(part))

        def each_step(step):
            def wide_step(idx, carry):
                step(per * idx, WIDE)
                return carry

            def narrow_step(idx, carry):
                step(per * n_wide + idx, TQ)
                return carry

            lax.fori_loop(0, n_wide, wide_step, 0)
            if n_narrow is not None:
                lax.fori_loop(0, n_narrow, narrow_step, 0)

        each_step(score_step)
        row_best = jnp.max(mx_v[...], axis=1, keepdims=True)
        mb_v[...] = jnp.broadcast_to(row_best, mb_v.shape)

        def probs(col, width):
            base = mb_v[...]
            total = None
            parts = []
            for idx in range(width // head):
                part = jnp.exp2(s_v[:, pl.ds(pl.multiple_of(col + idx * head, head), head)] - base)
                total = part if total is None else total + part
                parts.append(part.astype(jnp.bfloat16))
            return jnp.concatenate(parts, axis=1), total

        prob, total = probs(0, TQ)
        acc = jnp.dot(prob, values(gidx, TQ), preferred_element_type=jnp.float32)
        if with_first:
            prob, total_b = probs(TQ, TQ)
            total = total + total_b
            acc = acc + jnp.dot(prob, values(gidx - WINDOW // TQ, TQ), preferred_element_type=jnp.float32)
        l_v[...] = total
        acc_v[...] = acc

        def value_step(tile, width):
            prob, total = probs((2 + tile) * TQ, width)
            l_v[...] += total
            acc_v[...] += jnp.dot(prob, values(start_tile + tile, width), preferred_element_type=jnp.float32)

        each_step(value_step)
        denom = jnp.sum(l_v[...], axis=1, keepdims=True)
        out = (acc_v[...] / denom).astype(jnp.bfloat16)
        out = jnp.concatenate([out[:TQ], out[TQ:]], axis=1)
        o_st[pl.ds(pl.multiple_of(q_idx * TQ, TQ), TQ), :] = out

    def y_copy(z_dst, z_src):
        return pltpu.make_async_remote_copy(
            src_ref=yst.at[z_dst], dst_ref=y_hbm.at[:, pl.ds(pl.multiple_of(z_src * cols, 128), cols)],
            send_sem=y_send.at[z_dst], recv_sem=y_recv.at[z_src], device_id={"tp": NY * z_dst + my_y}, device_id_type=MESH)

    y_own = pltpu.make_async_copy(yst.at[my_z], y_hbm.at[:, pl.ds(pl.multiple_of(my_z * cols, 128), cols)], y_sem)

    def out_product(first, count):
        for row in range(first, first + count):
            for src in range(n_tp):
                @pl.when(tp != src)
                def _(row=row, src=src):
                    o_arrival(row, src).wait_recv()
        lhs = jnp.concatenate([og[first:first + count, src].reshape(count * rows, 2 * head) for src in range(n_tp)], axis=1)
        for col in range(0, cols, 384):
            w_cols = jnp.concatenate([wo_v[NY * y_idx + z_idx, :, :, col:col + 384].reshape(2 * head, 384)
                                      for z_idx in range(NY) for y_idx in range(NY)], axis=0)
            res = jnp.dot(lhs, w_cols, preferred_element_type=jnp.float32).astype(jnp.bfloat16)
            yst[first:first + count, :, col:col + 384] = res.reshape(count, rows, 384)

    def y_put(first, count):
        for z_dst in range(first, first + count):
            @pl.when(my_z != z_dst)
            def _(z_dst=z_dst):
                y_copy(z_dst, my_z).start()

            @pl.when(my_z == z_dst)
            def _(z_dst=z_dst):
                y_own.start()

    def q_step(q_idx, carry):
        tiles = chunk // TQ
        blk = jnp.where(q_idx < tiles, sp, 2 * n_sp - 1 - sp)
        gidx = blk * tiles + q_idx % tiles

        @pl.when(gidx >= WINDOW // TQ)
        def _():
            attend(q_idx, gidx, gidx - WINDOW // TQ + 1, N_WIDE, None, True)

        @pl.when(gidx < WINDOW // TQ)
        def _():
            attend(q_idx, gidx, 0, gidx // (WIDE // TQ), gidx % (WIDE // TQ), False)

        for sub in range(2):
            tile = 2 * q_idx + sub

            for z_dst in range(NY):
                mine = (tile % NY == my_y) & (my_z == z_dst)

                @pl.when(jnp.logical_not(mine))
                def _(tile=tile, z_dst=z_dst):
                    o_copy(tile, z_dst).start()

            @pl.when(tile % NY == my_y)
            def _(tile=tile):
                og[tile // NY, tp] = o_st[pl.ds(pl.multiple_of(tile * rows, rows), rows), :]

        @pl.when(q_idx == 5)
        def _():
            wo_second()

        return carry

    lax.fori_loop(0, 2 * chunk // TQ, q_step, 0)

    wo_last()
    out_product(0, 2)
    y_put(0, 2)
    out_product(2, 1)
    y_put(2, 1)
    out_product(3, 1)
    y_put(3, 1)
    for z_src in range(NY):
        @pl.when(my_z != z_src)
        def _(z_src=z_src):
            y_copy(z_src, z_src).wait_recv()
    for tile in range(n_tp):
        for z_dst in range(NY):
            mine = (tile % NY == my_y) & (my_z == z_dst)

            @pl.when(jnp.logical_not(mine))
            def _(tile=tile, z_dst=z_dst):
                o_copy(tile, z_dst).wait_send()
    for z_dst in range(NY):
        @pl.when(my_z != z_dst)
        def _(z_dst=z_dst):
            y_copy(z_dst, my_z).wait_send()
    for copy in sends + list(slabs):
        copy.wait_send()
    for step in range(1, NY):
        wo_copy(step).wait_send()
    for copy in wy_sends:
        copy.wait_send()
    for slot in range(3):
        for kind in range(2):
            share_copy(kind, my_z, my_c, slot).wait_send()
    for slot in range(3):
        a_copy(0, my_z, 0, slot).wait_send()
    for z_idx in range(NY):
        kv_own(z_idx, done)
        kv_direct(z_idx, done, False)
        kv_relay(z_idx, done, False)
    y_own.wait()


def solution(mesh):
    n_sp, n_tp = mesh.shape["sp"], mesh.shape["tp"]

    def local_attn(x_part, w_query, w_key, w_value, w_out):
        rows, d_model = x_part.shape
        heads_loc, head = w_query.shape[1], w_query.shape[2]
        two_head = heads_loc * head
        seq_loc = rows * n_tp
        cols = d_model // NY
        any_spec = pl.BlockSpec(memory_space=pl.ANY)
        dma = pltpu.SemaphoreType.DMA
        bf16, f32 = jnp.bfloat16, jnp.float32
        wo_rows = w_out.shape[0] * w_out.shape[1] // NY
        return pl.pallas_call(
            layer_kernel,
            out_shape=jax.ShapeDtypeStruct((rows, d_model), bf16),
            in_specs=[any_spec] * 5,
            out_specs=any_spec,
            scratch_shapes=[
                pltpu.VMEM((NY, rows, d_model), bf16),
                pltpu.VMEM((NY, d_model, two_head), bf16),
                pltpu.VMEM((NY, d_model, two_head), bf16),
                pltpu.VMEM((seq_loc, two_head), bf16),
                pltpu.VMEM((n_sp * seq_loc, two_head), bf16),
                pltpu.VMEM((NY - 1, seq_loc // NY, two_head), bf16),
                pltpu.VMEM((n_tp, NY, wo_rows, cols), bf16),
                pltpu.VMEM((2 * TQ, WINDOW + TQ), f32),
                pltpu.VMEM((2 * TQ, head), f32),
                pltpu.VMEM((2 * TQ, head), f32),
                pltpu.VMEM((2 * TQ, head), f32),
                pltpu.VMEM((2 * TQ, head), f32),
                pltpu.VMEM((seq_loc, two_head), bf16),
                pltpu.VMEM((NY, n_tp, rows, two_head), bf16),
                pltpu.VMEM((NY, rows, cols), bf16),
                pltpu.VMEM((d_model, head), bf16),
                dma, dma((3,)), dma((4,)), dma((NY, 2)), dma((40,)), dma((2, NY, NY + 1, 2)), dma((2, 3)), dma((2, NY)), dma((2, 3)), dma((2, NY)),
                dma((NY, 6)), dma((2 * n_sp, 2)), dma, dma((NY,)), dma((NY,)), dma((4,)), dma((NY, 2)), dma((4,)), dma((NY, 2)),
                dma((n_tp, NY)), dma((NY, n_tp)), dma((NY,)), dma((NY,)), dma,
            ],
            compiler_params=pltpu.CompilerParams(collective_id=1, has_side_effects=True, vmem_limit_bytes=67043328),
            name="layer",
        )(x_part, w_query.reshape(heads_loc * d_model, head), w_key.reshape(d_model, head), w_value.reshape(d_model, head),
          w_out.reshape(NY, wo_rows, d_model))

    return jax.shard_map(local_attn, mesh=mesh, in_specs=(P(("dp", "sp", "tp"), None), P(None, "tp", None), P(None, "tp", None), P(None, "tp", None), P("tp", None, None)), out_specs=P(("dp", "sp", "tp"), None), check_vma=False)
```

```python
import functools

import jax
import jax.numpy as jnp
from jax import lax
from jax.experimental import pallas as pl
from jax.experimental.pallas import tpu as pltpu
from jax.sharding import PartitionSpec as P

WINDOW = 4096
NEG_BIG = -1e30
LOG2E = 1.4426950408889634
MESH = pl.DeviceIdType.MESH
NY = 4
TQ = 256
WIDE = 1280
N_WIDE = (WINDOW - TQ) // WIDE


def dot_nt(lhs, rhs):
    return lax.dot_general(lhs, rhs, (((1,), (1,)), ((), ())), preferred_element_type=jnp.float32)


def layer_kernel(x_hbm, wq_hbm, wk_hbm, wv_hbm, wo_hbm, y_hbm, xg, wq_v, wkv_v, q_v, kv_v, kv_st, wo_v, s_v, mx_v, mb_v, l_v, acc_v, o_st,
                 og, yst, raw_v, x_sem, wl_sem, x_send, x_recv, w_send, w_recv, share_send, share_recv, a_send, a_recv,
                 kv_send, kv_recv, wo_sem, wo_send, wo_recv, wy_send, wy_recv, sl_send, sl_recv, o_send, o_recv,
                 y_send, y_recv, y_sem):
    sp = lax.axis_index("sp")
    tp = lax.axis_index("tp")
    my_z, my_y = tp // NY, tp % NY
    my_x, my_c = sp // 2, sp % 2
    n_tp = NY * NY
    n_sp = 8
    chunk = kv_v.shape[0] // (2 * n_sp)
    head = kv_v.shape[1] // 2
    cols = yst.shape[2]
    rows = yst.shape[1]
    part = NY * rows
    coef = head ** -0.5 * LOG2E
    d_half = wq_v.shape[1] // 2
    s_rows = d_half // (6 * 32) * 32 - 32
    d_rows = d_half - NY * s_rows

    x_load = pltpu.make_async_copy(x_hbm, xg.at[my_y], x_sem)
    x_load.start()
    w_loads = (pltpu.make_async_copy(wk_hbm, wkv_v.at[my_z, :, 0:head], wl_sem.at[0]),
               pltpu.make_async_copy(wv_hbm, wkv_v.at[my_z, :, head:2 * head], wl_sem.at[1]),
               pltpu.make_async_copy(wq_hbm.at[pl.ds(0, raw_v.shape[0])], raw_v, wl_sem.at[2]))
    for load in w_loads:
        load.start()

    barrier = pltpu.get_barrier_semaphore()
    for step in range(1, n_tp):
        pl.semaphore_signal(barrier, inc=1, device_id={"tp": (tp + step) % n_tp}, device_id_type=MESH)
    for step in range(1, n_sp):
        pl.semaphore_signal(barrier, inc=1, device_id={"sp": (sp + step) % n_sp}, device_id_type=MESH)
    pl.semaphore_wait(barrier, n_tp + n_sp - 2)

    zm, zp, zo = (my_z + 3) % NY, (my_z + 1) % NY, (my_z + 2) % NY
    ym, yp, yo = (my_y + 3) % NY, (my_y + 1) % NY, (my_y + 2) % NY
    x_left, x_right, x_far = (my_x + 3) % NY, (my_x + 1) % NY, (my_x + 2) % NY
    partner = {"sp": 2 * my_x + 1 - my_c}
    sends = []
    n_sends = [0, 0]

    def x_copy(y_src, first, count, y_dst, slot):
        ref = xg.at[y_src, pl.ds(first * (rows // 2), count * (rows // 2))]
        return pltpu.make_async_remote_copy(src_ref=ref, dst_ref=ref, send_sem=x_send.at[slot], recv_sem=x_recv.at[y_src, first],
                                            device_id={"tp": NY * my_z + y_dst}, device_id_type=MESH)

    def x_put(y_src, first, count, y_dst):
        copy = x_copy(y_src, first, count, y_dst, n_sends[0])
        n_sends[0] += 1
        sends.append(copy)
        copy.start()

    def x_wait(y_src, first, count):
        x_copy(y_src, first, count, 0, 0).wait_recv()

    def w_copy(kind, z_src, x_src, first, count, dst, slot):
        size = d_rows if x_src is None else s_rows
        base = my_c * d_half + (0 if x_src is None else d_rows + x_src * s_rows)
        ref = (wq_v if kind else wkv_v).at[z_src, pl.ds(pl.multiple_of(base + first * (size // 2), 16), count * (size // 2))]
        return pltpu.make_async_remote_copy(src_ref=ref, dst_ref=ref, send_sem=w_send.at[slot],
                                            recv_sem=w_recv.at[kind, z_src, NY if x_src is None else x_src, first], device_id=dst, device_id_type=MESH)

    def w_put(kind, z_src, x_src, first, count, dst):
        copy = w_copy(kind, z_src, x_src, first, count, dst, n_sends[1])
        n_sends[1] += 1
        sends.append(copy)
        copy.start()

    def w_wait(kind, z_src, x_src, first, count):
        w_copy(kind, z_src, x_src, first, count, {"tp": 0}, 0).wait_recv()

    def to_z(z_dst):
        return {"tp": NY * z_dst + my_y}

    def to_x(x_dst):
        return {"sp": 2 * x_dst + my_c}

    def share_copy(kind, z_src, core, slot):
        ref = (wq_v if kind else wkv_v).at[z_src, pl.ds(pl.multiple_of(core * d_half, 64), d_half)]
        return pltpu.make_async_remote_copy(src_ref=ref, dst_ref=ref, send_sem=share_send.at[kind, slot], recv_sem=share_recv.at[kind, z_src],
                                            device_id=partner, device_id_type=MESH)

    def blk_of(z_idx):
        return jnp.where(z_idx < NY // 2, sp, 2 * n_sp - 1 - sp)

    def kv_rows(z_idx):
        return pl.multiple_of(blk_of(z_idx) * chunk + (z_idx % 2) * part, part)

    def own_products(y_list):
        def body(idx, carry):
            y_idx = y_list[0]
            for other in range(1, len(y_list)):
                y_idx = jnp.where(idx == other, y_list[other], y_idx)
            prod = jnp.dot(xg[y_idx], wkv_v[my_z], preferred_element_type=jnp.float32).astype(jnp.bfloat16)
            kv_v[pl.ds(pl.multiple_of(kv_rows(my_z) + y_idx * rows, rows), rows), :] = prod
            prod = jnp.dot(xg[y_idx], wq_v[my_z], preferred_element_type=jnp.float32).astype(jnp.bfloat16)
            q_v[pl.ds(pl.multiple_of(my_z * part + y_idx * rows, rows), rows), :] = prod
            return carry

        lax.fori_loop(0, len(y_list), body, 0)

    def a_copy(kind, z_src, z_dst, slot):
        if kind:
            src, dst = o_st.at[pl.ds(slot * part, part)], q_v.at[pl.ds(pl.multiple_of(z_src * part, part), part)]
        else:
            src, dst = kv_st.at[slot], kv_v.at[pl.ds(kv_rows(z_src), part)]
        return pltpu.make_async_remote_copy(src_ref=src, dst_ref=dst, send_sem=a_send.at[kind, slot], recv_sem=a_recv.at[kind, z_src],
                                            device_id=to_z(z_dst), device_id_type=MESH)

    def products(kind, z_dst, slot):
        def body(idx, carry):
            lhs = xg[pl.ds(2 * idx, 2)].reshape(2 * rows, xg.shape[2])
            prod = jnp.dot(lhs, (wq_v if kind else wkv_v)[z_dst], preferred_element_type=jnp.float32).astype(jnp.bfloat16)
            if kind:
                o_st[pl.ds(pl.multiple_of(slot * part + idx * 2 * rows, 2 * rows), 2 * rows), :] = prod
            else:
                kv_st[slot, pl.ds(pl.multiple_of(idx * 2 * rows, 2 * rows), 2 * rows), :] = prod
            return carry

        lax.fori_loop(0, 2, body, 0)

    def a_start(kind, z_dst, slot):
        a_copy(kind, my_z, z_dst, slot).start()

    def a_wait(kind, z_src):
        a_copy(kind, z_src, 0, 0).wait_recv()

    def kv_part(pair, core, z_idx, kind, dst):
        blk = jnp.where(pair < NY, 2 * pair + core, 2 * pair + 1 - core)
        ref = kv_v.at[pl.ds(pl.multiple_of(blk * chunk + (z_idx % 2) * part, part), part)]
        return pltpu.make_async_remote_copy(src_ref=ref, dst_ref=ref, send_sem=kv_send.at[z_idx, kind], recv_sem=kv_recv.at[blk, z_idx % 2],
                                            device_id=dst, device_id_type=MESH)

    def own_pair(z_idx):
        return jnp.where(z_idx < NY // 2, my_x, 2 * NY - 1 - my_x)

    def own_next(z_idx):
        low = z_idx < NY // 2
        return jnp.where(low, jnp.where(my_x < NY - 1, my_x + 1, NY - 2), my_x - 1), low | (my_x >= 1)

    def direct_in(z_idx):
        low = z_idx < NY // 2
        return jnp.where(low, my_x - 1, 2 * NY - 2 - my_x), (low & (my_x >= 1)) | (jnp.logical_not(low) & (my_x < NY - 1))

    def direct_next(z_idx):
        return jnp.where(z_idx < NY // 2, my_x + 1, my_x - 1), (my_x >= 1) & (my_x < NY - 1)

    def relay_in(z_idx):
        low = z_idx < NY // 2
        return jnp.where(low, my_x - 2, 2 * NY - 3 - my_x), (low & (my_x >= 2)) | (jnp.logical_not(low) & (my_x < NY - 2))

    def turn_in(z_idx):
        return NY - 1, (z_idx < NY // 2) & (my_x == NY - 2)

    def kv_own(z_idx, act):
        dst, wanted = own_next(z_idx)

        @pl.when(wanted)
        def _():
            act(kv_part(own_pair(z_idx), my_c, z_idx, 1, to_x(dst)))

        act(kv_part(own_pair(z_idx), my_c, z_idx, 0, partner))

    def kv_direct(z_idx, act, arrive):
        pair, wanted = direct_in(z_idx)

        @pl.when(wanted)
        def _():
            if arrive:
                kv_part(pair, my_c, z_idx, 2, partner).wait_recv()
            dst, more = direct_next(z_idx)

            @pl.when(more)
            def _():
                act(kv_part(pair, my_c, z_idx, 3, to_x(dst)))

            act(kv_part(pair, my_c, z_idx, 2, partner))

    def kv_relay(z_idx, act, arrive):
        for kind, (pair, wanted) in ((4, relay_in(z_idx)), (5, turn_in(z_idx))):
            @pl.when(wanted)
            def _(kind=kind, pair=pair):
                copy = kv_part(pair, my_c, z_idx, kind, partner)
                if arrive:
                    copy.wait_recv()
                act(copy)

    def kv_from_partner(z_idx):
        kv_part(own_pair(z_idx), 1 - my_c, z_idx, 0, partner).wait_recv()
        for pair, wanted in (direct_in(z_idx), relay_in(z_idx), turn_in(z_idx)):
            @pl.when(wanted)
            def _(pair=pair):
                kv_part(pair, 1 - my_c, z_idx, 0, partner).wait_recv()

    def start(copy):
        copy.start()

    def done(copy):
        copy.wait_send()

    group = 2 * (my_x % 2) + my_c
    x_group = 2 - 2 * (my_x % 2) + my_c

    def wo_copy(step):
        dst = (my_z + step) % NY
        src_ref = wo_hbm.at[group, :, pl.ds(pl.multiple_of(dst * cols, 128), cols)]
        return pltpu.make_async_remote_copy(src_ref=src_ref, dst_ref=wo_v.at[NY * my_y + my_z, group], send_sem=wo_send.at[step],
                                            recv_sem=wo_recv.at[my_z], device_id=to_z(dst), device_id_type=MESH)

    wo_own = pltpu.make_async_copy(wo_hbm.at[group, :, pl.ds(pl.multiple_of(my_z * cols, 128), cols)], wo_v.at[NY * my_y + my_z, group], wo_sem)

    def wo_z_start():
        wo_own.start()
        for step in range(1, NY):
            wo_copy(step).start()

    def wy_copy(y_src, first, count, y_dst, slot):
        ref = wo_v.at[pl.ds(NY * y_src + 2 * first, 2 * count), group]
        return pltpu.make_async_remote_copy(src_ref=ref, dst_ref=ref, send_sem=wy_send.at[slot], recv_sem=wy_recv.at[y_src, first],
                                            device_id={"tp": NY * my_z + y_dst}, device_id_type=MESH)

    wy_sends = (wy_copy(my_y, 0, 2, yp, 0), wy_copy(my_y, 0, 2, ym, 1), wy_copy(ym, 0, 1, yp, 2), wy_copy(yp, 1, 1, ym, 3))

    def wo_y_start():
        wo_own.wait()
        for z_src in (zm, zp, zo):
            ref = wo_v.at[NY * my_y + z_src, group]
            pltpu.make_async_remote_copy(src_ref=ref, dst_ref=ref, send_sem=wo_send.at[1], recv_sem=wo_recv.at[z_src],
                                         device_id=to_z(z_src), device_id_type=MESH).wait_recv()
        for copy in wy_sends[:2]:
            copy.start()

    def wo_y_pass():
        for y_src, copy in ((ym, wy_sends[2]), (yp, wy_sends[3])):
            wy_copy(y_src, 0, 2, 0, 0).wait_recv()
            copy.start()

    def slab_copy(grp, first, count, dst, slot):
        ref = wo_v.at[pl.ds(first * (n_tp // 2), count * (n_tp // 2)), grp]
        return pltpu.make_async_remote_copy(src_ref=ref, dst_ref=ref, send_sem=sl_send.at[slot], recv_sem=sl_recv.at[grp, first],
                                            device_id=dst, device_id_type=MESH)

    slabs = (slab_copy(group, 0, 1, to_x(x_right), 0), slab_copy(group, 1, 1, to_x(x_left), 1), slab_copy(group, 0, 2, partner, 2),
             slab_copy(x_group, 0, 2, partner, 3))

    def wo_first():
        for first in range(2):
            wy_copy(yo, first, 1, 0, 0).wait_recv()
        for copy in slabs[:3]:
            copy.start()

    def wo_second():
        for first in range(2):
            slab_copy(x_group, first, 1, partner, 3).wait_recv()
        slabs[3].start()

    def wo_last():
        for grp in (2 * (my_x % 2), 2 - 2 * (my_x % 2)):
            slab_copy(grp + 1 - my_c, 0, 2, partner, 3).wait_recv()

    def w_own_slice(kind):
        for z_dst in (zp, zm):
            w_put(kind, my_z, my_x, 0, 2, to_z(z_dst))

    def w_slices(kind):
        for z_src, first, z_dst in ((zm, 0, zp), (zp, 1, zm)):
            w_wait(kind, z_src, my_x, 0, 2)
            w_put(kind, z_src, my_x, first, 1, to_z(z_dst))
            for x_dst in (x_right, x_left):
                w_put(kind, z_src, my_x, 0, 2, to_x(x_dst))

    def w_own_rest(kind):
        for z_dst in (zp, zm):
            w_put(kind, my_z, None, 0, 2, to_z(z_dst))

    def w_far_slice(kind):
        for first in range(2):
            w_wait(kind, zo, my_x, first, 1)
        for x_dst in (x_right, x_left):
            w_put(kind, zo, my_x, 0, 2, to_x(x_dst))

    def w_ring(kind, z_src):
        for x_src, first, x_dst in ((x_left, 0, x_right), (x_right, 1, x_left)):
            w_wait(kind, z_src, x_src, 0, 2)
            w_put(kind, z_src, x_src, first, 1, to_x(x_dst))

    def w_rest(kind):
        for z_src, first, z_dst in ((zm, 0, zp), (zp, 1, zm)):
            w_wait(kind, z_src, None, 0, 2)
            w_put(kind, z_src, None, first, 1, to_z(z_dst))

    def w_share(kind, z_src, slot):
        for first in range(2):
            w_wait(kind, z_src, x_far, first, 1)
            if slot == 2:
                w_wait(kind, z_src, None, first, 1)
        share_copy(kind, z_src, my_c, slot).start()

    def w_full(kind, z_src, slot):
        share_copy(kind, z_src, 1 - my_c, slot).wait_recv()

    def split_heads():
        size = mx_v.shape[0]
        count = raw_v.shape[0] // size
        for part_idx in range(2):
            load = pltpu.make_async_copy(wq_hbm.at[pl.ds(part_idx * raw_v.shape[0], raw_v.shape[0])], raw_v, wl_sem.at[2])
            if part_idx:
                load.start()
            load.wait()

            def body(idx, carry, part_idx=part_idx):
                mx_v[...] = raw_v[pl.ds(pl.multiple_of(idx * size, size), size), :].astype(jnp.float32)
                at = pl.ds(pl.multiple_of((part_idx * count + idx) * (size // 2), size // 2), size // 2)
                for sub in range(2):
                    wq_v[my_z, at, sub * head:(sub + 1) * head] = mx_v[pl.ds(sub, size // 2, stride=2), :].astype(jnp.bfloat16)
                return carry

            lax.fori_loop(0, count, body, 0)

    x_load.wait()
    x_put(my_y, 0, 2, yp)
    x_put(my_y, 0, 2, ym)
    for load in w_loads[:2]:
        load.wait()
    w_own_slice(0)
    w_slices(0)
    w_own_rest(0)
    wo_z_start()
    split_heads()
    w_own_slice(1)
    w_far_slice(0)
    own_products([my_y])
    w_ring(0, zm)
    w_ring(0, zp)
    w_rest(0)
    w_ring(0, zo)
    w_slices(1)
    w_own_rest(1)
    for y_src, first, y_dst in ((ym, 0, yp), (yp, 1, ym)):
        x_wait(y_src, 0, 2)
        x_put(y_src, first, 1, y_dst)
    w_share(0, zm, 0)
    w_share(0, zp, 1)
    w_far_slice(1)
    own_products([ym, yp])
    w_share(0, zo, 2)
    w_ring(1, zm)
    w_ring(1, zp)
    for first in range(2):
        x_wait(yo, first, 1)
    own_products([yo])
    kv_own(my_z, start)
    for slot, z_dst in enumerate((zm, zp, zo)):
        w_full(0, z_dst, slot)
        products(0, z_dst, slot)
        a_start(0, z_dst, slot)
    w_rest(1)
    w_ring(1, zo)
    wo_y_start()
    kv_direct(my_z, start, True)
    for z_src in (zm, zp, zo):
        a_wait(0, z_src)
        kv_own(z_src, start)
    for slot, z_src in enumerate((zm, zp, zo)):
        w_share(1, z_src, slot)
    kv_relay(my_z, start, True)
    for slot, z_dst in enumerate((zm, zp, zo)):
        w_full(1, z_dst, slot)
        products(1, z_dst, slot)
        a_start(1, z_dst, slot)
        kv_direct(z_dst, start, True)
        if slot == 0:
            wo_y_pass()
    for z_src in (zm, zp, zo):
        kv_relay(z_src, start, True)
    wo_first()
    for z_src in (zm, zp, zo):
        a_wait(1, z_src)
    for slot in range(3):
        a_copy(1, my_z, 0, slot).wait_send()
    for z_idx in range(NY):
        kv_from_partner(z_idx)

    row_i = lax.broadcasted_iota(jnp.int32, (2 * TQ, TQ), 0) % TQ
    col_i = lax.broadcasted_iota(jnp.int32, (2 * TQ, TQ), 1)

    def lane_max(scores):
        best = scores[:, 0:head]
        for idx in range(1, scores.shape[1] // head):
            best = jnp.maximum(best, scores[:, idx * head:(idx + 1) * head])
        return best

    def o_copy(tile, z_dst):
        y_dst, z_row = tile % NY, tile // NY
        src = o_st.at[pl.ds(pl.multiple_of(tile * rows, rows), rows)]
        dst = og.at[z_row, tp]
        return pltpu.make_async_remote_copy(src_ref=src, dst_ref=dst, send_sem=o_send.at[tile, z_dst], recv_sem=o_recv.at[z_row, tp],
                                            device_id={"tp": NY * z_dst + y_dst}, device_id_type=MESH)

    def o_arrival(z_row, src):
        dst = og.at[z_row, src]
        return pltpu.make_async_remote_copy(src_ref=o_st.at[pl.ds(0, rows)], dst_ref=dst, send_sem=o_send.at[0, 0],
                                            recv_sem=o_recv.at[z_row, src], device_id={"tp": 0}, device_id_type=MESH)

    def attend(q_idx, gidx, start_tile, n_wide, n_narrow, with_first):
        q_blk = q_v[pl.ds(pl.multiple_of(q_idx * TQ, TQ), TQ), :]
        q_two = jnp.concatenate([q_blk[:, :head], q_blk[:, head:]], axis=0)

        def keys(tile, width):
            return kv_v[pl.ds(pl.multiple_of(tile * TQ, TQ), width), 0:head]

        def values(tile, width):
            return kv_v[pl.ds(pl.multiple_of(tile * TQ, TQ), width), head:2 * head]

        per = WIDE // TQ
        scores = jnp.where(col_i <= row_i, dot_nt(q_two, keys(gidx, TQ)) * coef, NEG_BIG)
        s_v[:, 0:TQ] = scores
        best = lane_max(scores)
        if with_first:
            scores = jnp.where(col_i > row_i, dot_nt(q_two, keys(gidx - WINDOW // TQ, TQ)) * coef, NEG_BIG)
            s_v[:, TQ:2 * TQ] = scores
            best = jnp.maximum(best, lane_max(scores))
        mx_v[...] = best

        def score_step(tile, width):
            part = dot_nt(q_two, keys(start_tile + tile, width)) * coef
            s_v[:, pl.ds(pl.multiple_of((2 + tile) * TQ, TQ), width)] = part
            mx_v[...] = jnp.maximum(mx_v[...], lane_max(part))

        def each_step(step):
            def wide_step(idx, carry):
                step(per * idx, WIDE)
                return carry

            def narrow_step(idx, carry):
                step(per * n_wide + idx, TQ)
                return carry

            lax.fori_loop(0, n_wide, wide_step, 0)
            if n_narrow is not None:
                lax.fori_loop(0, n_narrow, narrow_step, 0)

        each_step(score_step)
        row_best = jnp.max(mx_v[...], axis=1, keepdims=True)
        mb_v[...] = jnp.broadcast_to(row_best, mb_v.shape)

        def probs(col, width):
            base = mb_v[...]
            total = None
            parts = []
            for idx in range(width // head):
                part = jnp.exp2(s_v[:, pl.ds(pl.multiple_of(col + idx * head, head), head)] - base)
                total = part if total is None else total + part
                parts.append(part.astype(jnp.bfloat16))
            return jnp.concatenate(parts, axis=1), total

        prob, total = probs(0, TQ)
        acc = jnp.dot(prob, values(gidx, TQ), preferred_element_type=jnp.float32)
        if with_first:
            prob, total_b = probs(TQ, TQ)
            total = total + total_b
            acc = acc + jnp.dot(prob, values(gidx - WINDOW // TQ, TQ), preferred_element_type=jnp.float32)
        l_v[...] = total
        acc_v[...] = acc

        def value_step(tile, width):
            prob, total = probs((2 + tile) * TQ, width)
            l_v[...] += total
            acc_v[...] += jnp.dot(prob, values(start_tile + tile, width), preferred_element_type=jnp.float32)

        each_step(value_step)
        denom = jnp.sum(l_v[...], axis=1, keepdims=True)
        out = (acc_v[...] / denom).astype(jnp.bfloat16)
        out = jnp.concatenate([out[:TQ], out[TQ:]], axis=1)
        o_st[pl.ds(pl.multiple_of(q_idx * TQ, TQ), TQ), :] = out

    def y_copy(z_dst, z_src):
        return pltpu.make_async_remote_copy(
            src_ref=yst.at[z_dst], dst_ref=y_hbm.at[:, pl.ds(pl.multiple_of(z_src * cols, 128), cols)],
            send_sem=y_send.at[z_dst], recv_sem=y_recv.at[z_src], device_id={"tp": NY * z_dst + my_y}, device_id_type=MESH)

    y_own = pltpu.make_async_copy(yst.at[my_z], y_hbm.at[:, pl.ds(pl.multiple_of(my_z * cols, 128), cols)], y_sem)

    def out_product(first, count):
        for row in range(first, first + count):
            for src in range(n_tp):
                @pl.when(tp != src)
                def _(row=row, src=src):
                    o_arrival(row, src).wait_recv()
        lhs = jnp.concatenate([og[first:first + count, src].reshape(count * rows, 2 * head) for src in range(n_tp)], axis=1)
        for col in range(0, cols, 384):
            w_cols = jnp.concatenate([wo_v[NY * y_idx + z_idx, :, :, col:col + 384].reshape(2 * head, 384)
                                      for z_idx in range(NY) for y_idx in range(NY)], axis=0)
            res = jnp.dot(lhs, w_cols, preferred_element_type=jnp.float32).astype(jnp.bfloat16)
            yst[first:first + count, :, col:col + 384] = res.reshape(count, rows, 384)

    def y_put(first, count):
        for z_dst in range(first, first + count):
            @pl.when(my_z != z_dst)
            def _(z_dst=z_dst):
                y_copy(z_dst, my_z).start()

            @pl.when(my_z == z_dst)
            def _(z_dst=z_dst):
                y_own.start()

    def q_step(q_idx, carry):
        tiles = chunk // TQ
        blk = jnp.where(q_idx < tiles, sp, 2 * n_sp - 1 - sp)
        gidx = blk * tiles + q_idx % tiles

        @pl.when(gidx >= WINDOW // TQ)
        def _():
            attend(q_idx, gidx, gidx - WINDOW // TQ + 1, N_WIDE, None, True)

        @pl.when(gidx < WINDOW // TQ)
        def _():
            attend(q_idx, gidx, 0, gidx // (WIDE // TQ), gidx % (WIDE // TQ), False)

        for sub in range(2):
            tile = 2 * q_idx + sub

            for z_dst in range(NY):
                mine = (tile % NY == my_y) & (my_z == z_dst)

                @pl.when(jnp.logical_not(mine))
                def _(tile=tile, z_dst=z_dst):
                    o_copy(tile, z_dst).start()

            @pl.when(tile % NY == my_y)
            def _(tile=tile):
                og[tile // NY, tp] = o_st[pl.ds(pl.multiple_of(tile * rows, rows), rows), :]

        @pl.when(q_idx == 6)
        def _():
            wo_second()

        return carry

    lax.fori_loop(0, 2 * chunk // TQ, q_step, 0)

    wo_last()
    out_product(0, 2)
    y_put(0, 2)
    out_product(2, 1)
    y_put(2, 1)
    out_product(3, 1)
    y_put(3, 1)
    for z_src in range(NY):
        @pl.when(my_z != z_src)
        def _(z_src=z_src):
            y_copy(z_src, z_src).wait_recv()
    for tile in range(n_tp):
        for z_dst in range(NY):
            mine = (tile % NY == my_y) & (my_z == z_dst)

            @pl.when(jnp.logical_not(mine))
            def _(tile=tile, z_dst=z_dst):
                o_copy(tile, z_dst).wait_send()
    for z_dst in range(NY):
        @pl.when(my_z != z_dst)
        def _(z_dst=z_dst):
            y_copy(z_dst, my_z).wait_send()
    for copy in sends + list(slabs):
        copy.wait_send()
    for step in range(1, NY):
        wo_copy(step).wait_send()
    for copy in wy_sends:
        copy.wait_send()
    for slot in range(3):
        for kind in range(2):
            share_copy(kind, my_z, my_c, slot).wait_send()
    for slot in range(3):
        a_copy(0, my_z, 0, slot).wait_send()
    for z_idx in range(NY):
        kv_own(z_idx, done)
        kv_direct(z_idx, done, False)
        kv_relay(z_idx, done, False)
    y_own.wait()


def solution(mesh):
    n_sp, n_tp = mesh.shape["sp"], mesh.shape["tp"]

    def local_attn(x_part, w_query, w_key, w_value, w_out):
        rows, d_model = x_part.shape
        heads_loc, head = w_query.shape[1], w_query.shape[2]
        two_head = heads_loc * head
        seq_loc = rows * n_tp
        cols = d_model // NY
        any_spec = pl.BlockSpec(memory_space=pl.ANY)
        dma = pltpu.SemaphoreType.DMA
        bf16, f32 = jnp.bfloat16, jnp.float32
        wo_rows = w_out.shape[0] * w_out.shape[1] // NY
        return pl.pallas_call(
            layer_kernel,
            out_shape=jax.ShapeDtypeStruct((rows, d_model), bf16),
            in_specs=[any_spec] * 5,
            out_specs=any_spec,
            scratch_shapes=[
                pltpu.VMEM((NY, rows, d_model), bf16),
                pltpu.VMEM((NY, d_model, two_head), bf16),
                pltpu.VMEM((NY, d_model, two_head), bf16),
                pltpu.VMEM((seq_loc, two_head), bf16),
                pltpu.VMEM((n_sp * seq_loc, two_head), bf16),
                pltpu.VMEM((NY - 1, seq_loc // NY, two_head), bf16),
                pltpu.VMEM((n_tp, NY, wo_rows, cols), bf16),
                pltpu.VMEM((2 * TQ, WINDOW + TQ), f32),
                pltpu.VMEM((2 * TQ, head), f32),
                pltpu.VMEM((2 * TQ, head), f32),
                pltpu.VMEM((2 * TQ, head), f32),
                pltpu.VMEM((2 * TQ, head), f32),
                pltpu.VMEM((seq_loc, two_head), bf16),
                pltpu.VMEM((NY, n_tp, rows, two_head), bf16),
                pltpu.VMEM((NY, rows, cols), bf16),
                pltpu.VMEM((d_model, head), bf16),
                dma, dma((3,)), dma((4,)), dma((NY, 2)), dma((40,)), dma((2, NY, NY + 1, 2)), dma((2, 3)), dma((2, NY)), dma((2, 3)), dma((2, NY)),
                dma((NY, 6)), dma((2 * n_sp, 2)), dma, dma((NY,)), dma((NY,)), dma((4,)), dma((NY, 2)), dma((4,)), dma((NY, 2)),
                dma((n_tp, NY)), dma((NY, n_tp)), dma((NY,)), dma((NY,)), dma,
            ],
            compiler_params=pltpu.CompilerParams(collective_id=1, has_side_effects=True, vmem_limit_bytes=67043328),
            name="layer",
        )(x_part, w_query.reshape(heads_loc * d_model, head), w_key.reshape(d_model, head), w_value.reshape(d_model, head),
          w_out.reshape(NY, wo_rows, d_model))

    return jax.shard_map(local_attn, mesh=mesh, in_specs=(P(("dp", "sp", "tp"), None), P(None, "tp", None), P(None, "tp", None), P(None, "tp", None), P("tp", None, None)), out_specs=P(("dp", "sp", "tp"), None), check_vma=False)
```
